32 devices in a mesh: dp: 8 (over y, x, core), tensor: 4 (over z).
Axes of the slice: x: 2, y: 2, z: 4, core: 2. Of those that a mesh axis runs over, the one named last changes fastest.
Arguments:
- tokens: bfloat16 [8192, 1024], P(('dp', 'tensor')), may hold values from -6 to 6
- segment_ids: int32 [8, 1024], P('dp'), may hold values from 0 to 7, never falling along the last dimension, each value on 1 to 512 neighbouring positions
- out_grad: bfloat16 [8192, 1024], P(('dp', 'tensor')), may hold values from -6 to 6
- w_qkv: bfloat16 [1024, 3, 1024], P('dp', None, 'tensor'), may hold values from -0.1875 to 0.1875
- b_qv: bfloat16 [2, 1024], P(None, 'tensor'), may hold values from -3 to 3
- w_out: bfloat16 [1024, 1024], P('tensor', 'dp'), may hold values from -1.5 to 1.5
- b_out: bfloat16 [1024], replicated, may hold values from -3 to 3
- norm1_gain: bfloat16 [1024], replicated, may hold values from 0.099609375 to 1.8984375
- norm1_bias: bfloat16 [1024], replicated, may hold values from -3 to 3
- w_up: bfloat16 [1024, 4096], P('dp', 'tensor'), may hold values from -0.1875 to 0.1875
- b_up: bfloat16 [4096], P('tensor'), may hold values from -3 to 3
- w_down: bfloat16 [4096, 1024], P('tensor', 'dp'), may hold values from -0.09375 to 0.09375
- b_down: bfloat16 [1024], replicated, may hold values from -3 to 3
- norm2_gain: bfloat16 [1024], replicated, may hold values from 0.099609375 to 1.8984375
- norm2_bias: bfloat16 [1024], replicated, may hold values from -3 to 3
Outputs:
- output: bfloat16 [8192, 1024], P(('dp', 'tensor'))
- grad_tokens: bfloat16 [8192, 1024], P(('dp', 'tensor'))
- grad_w_qkv: float32 [1024, 3, 1024], P('dp', None, 'tensor')
- grad_b_qv: float32 [2, 1024], P(None, 'tensor')
- grad_w_out: float32 [1024, 1024], P('tensor', 'dp')
- grad_b_out: float32 [1024], replicated
- grad_norm1_gain: float32 [1024], replicated
- grad_norm1_bias: float32 [1024], replicated
- grad_w_up: float32 [1024, 4096], P('dp', 'tensor')
- grad_b_up: float32 [4096], P('tensor')
- grad_w_down: float32 [4096, 1024], P('tensor', 'dp')
- grad_b_down: float32 [1024], replicated
- grad_norm2_gain: float32 [1024], replicated
- grad_norm2_bias: float32 [1024], replicated
The draws below stay inside these ranges and needn't reach their ends.
Inputs may be any that keep to these rules, and one draw needn't show every extreme that they name: `segment_ids`: along each packed row the ids never fall; each id covers one run of 1 to 512 positions, and some run in each row has exactly 512.
All inputs are finite; a program needn't handle non-finite values.
Results may differ from the reference program's by a relative error of at most 0.02.
Values may be sent and summed in bfloat16 or wider, within the bound.
A program may use at most 128 MiB of HBM per device.

```python
import math
import jax
import jax.numpy as jnp
import numpy as np
from jax import lax

D = 1024
H = 16
HD = 64
FF = 4096
SEG_MOST = 512
ROWS = 1024
SEGS = 8
TOKENS = 8192
N_DP = 8


def steps_of(stream_key, shape, cuts, least, top_value):
    loudness, own = 1.0, jax.random.fold_in(stream_key, 6)
    for dim, blocks in cuts:
        draws = jnp.exp(jax.random.uniform(jax.random.fold_in(own, dim), (blocks,), jnp.float32, least / len(cuts), top_value / len(cuts)))
        loudness = loudness * jnp.repeat(draws, shape[dim] // blocks).reshape([-1 if axis == dim else 1 for axis in range(len(shape))])
    return loudness


def split_up(count, total, bound, skew):
    loads = [(1 << 20) // math.isqrt(rank ** skew) + 1 for rank in range(2, count + 1)]
    rest, holding = total - bound - (count - 1), [1] * (count - 1)
    while rest > 0:
        movable = [i for i in range(count - 1) if holding[i] < bound]
        pool, left = sum([loads[i] for i in movable]), rest
        for i in movable:
            addition = min(bound - holding[i], max(1, left * loads[i] // pool), rest)
            holding[i] = holding[i] + addition
            rest = rest - addition
    return np.array([bound] + holding)


def ragged(stream_key, number_of, total, reach, lean):
    if number_of == 2:
        one = jax.random.randint(stream_key, (), max(1, total - reach), min(reach, total - 1) + 1)
        return jnp.stack([one, total - one])
    lengths = jnp.asarray(split_up(number_of, total, reach, lean), jnp.int32)
    couples = (number_of - 1) // 2
    donor, taker = lengths[1:1 + 2 * couples:2], lengths[2:2 + 2 * couples:2]
    room = jnp.minimum(donor - 1, reach - taker)
    passed = jax.random.randint(jax.random.fold_in(stream_key, 1), (couples,), 0, 1 << 20) % (room + 1)
    lengths = lengths.at[1:1 + 2 * couples:2].set(donor - passed).at[2:2 + 2 * couples:2].set(taker + passed)
    return lengths[jax.random.permutation(jax.random.fold_in(stream_key, 2), number_of)]


def bell_draw(stream_key, shape, deviation, reach, split=(), kind=jnp.bfloat16):
    array = deviation * jax.random.normal(stream_key, shape, jnp.float32)
    if split:
        array = array * steps_of(stream_key, shape, split, -0.22, 0.18)
    return jnp.clip(array, -reach, reach).astype(kind)


def setup_inputs(seed: int = 0) -> dict:
    streams_of = jax.random.split(jax.random.key(seed), 16)
    tokens = bell_draw(streams_of[0], (TOKENS, D), 1.0, 6.0, ((0, 32),))
    segment_ids = jax.vmap(lambda own: jnp.searchsorted(jnp.cumsum(ragged(own, SEGS, ROWS, SEG_MOST, 2)), jnp.arange(ROWS), side="right"))(jax.random.split(streams_of[1], N_DP)).reshape((N_DP, ROWS)).astype(jnp.int32)
    out_grad = bell_draw(streams_of[2], (TOKENS, D), 1.0, 6.0, ((0, 32),))
    w_qkv = bell_draw(streams_of[3], (D, 3, D), D ** -0.5, 0.1875, ((0, 8), (2, 4)))
    b_qv = bell_draw(streams_of[4], (2, D), 0.5, 3.0, ((1, 4),))
    w_out = bell_draw(streams_of[5], (D, D), (D // 64) ** -0.5, 1.5, ((0, 4), (1, 8)))
    b_out = bell_draw(streams_of[6], (D,), 0.5, 3.0)
    norm1_gain = jnp.clip(1.0 + 0.18 * jax.random.normal(streams_of[7], (D,), jnp.float32), 0.099609375, 1.8984375).astype(jnp.bfloat16)
    norm1_bias = bell_draw(streams_of[8], (D,), 0.5, 3.0)
    w_up = bell_draw(streams_of[9], (D, FF), D ** -0.5, 0.1875, ((0, 8), (1, 4)))
    b_up = bell_draw(streams_of[10], (FF,), 0.5, 3.0, ((0, 4),))
    w_down = bell_draw(streams_of[11], (FF, D), FF ** -0.5, 0.09375, ((0, 4), (1, 8)))
    b_down = bell_draw(streams_of[12], (D,), 0.5, 3.0)
    norm2_gain = jnp.clip(1.0 + 0.18 * jax.random.normal(streams_of[13], (D,), jnp.float32), 0.099609375, 1.8984375).astype(jnp.bfloat16)
    norm2_bias = bell_draw(streams_of[14], (D,), 0.5, 3.0)
    return dict(tokens=tokens, segment_ids=segment_ids, out_grad=out_grad, w_qkv=w_qkv, b_qv=b_qv, w_out=w_out, b_out=b_out, norm1_gain=norm1_gain, norm1_bias=norm1_bias, w_up=w_up, b_up=b_up, w_down=w_down, b_down=b_down, norm2_gain=norm2_gain, norm2_bias=norm2_bias)


@jax.custom_vjp
def low(v):
    return lax.optimization_barrier(v.astype(jnp.bfloat16)).astype(jnp.float32)

@jax.custom_vjp
def low_back(v):
    return v

def low_keep(v):
    return (low(v), None)

def low_pass(kept, grad):
    return (grad,)

def back_keep(v):
    return (v, None)

def back_low(kept, grad):
    return (low(grad),)
low.defvjp(low_keep, low_pass)
low_back.defvjp(back_keep, back_low)

def product(left_side, right_side):
    return jnp.dot(left_side, right_side, precision=lax.Precision.HIGHEST)

def layer_norm(summed, norm_gain, norm_bias):
    row_mean = lax.optimization_barrier(jnp.mean(summed, axis=-1, keepdims=True))
    centred = summed - row_mean
    variance = lax.optimization_barrier(jnp.mean(centred * centred, axis=-1, keepdims=True))
    return centred * lax.rsqrt(variance + 1e-05) * norm_gain + norm_bias

def attend_row(query_heads, key_heads, value_heads, segments):
    scores = jnp.einsum('qhd,khd->hqk', query_heads, key_heads, precision=lax.Precision.HIGHEST) * HD ** (-0.5)
    scores = low_back(scores)
    same_doc = segments[:, None] == segments[None, :]
    scores = jnp.where(same_doc[None], scores, -1e+30)
    attn_probs = low(jax.nn.softmax(scores, axis=-1))
    return jnp.einsum('hqk,khd->qhd', attn_probs, value_heads, precision=lax.Precision.HIGHEST)

def reference(tokens, segment_ids, out_grad, w_qkv, b_qv, w_out, b_out, norm1_gain, norm1_bias, w_up, b_up, w_down, b_down, norm2_gain, norm2_bias):

    def forward(inputs, wq, bq, wo, bo, gain1, shift1, wu, bu, wd, bd, gain2, shift2):
        projected = product(inputs, wq.reshape(D, 3 * D)).reshape(TOKENS, 3, D)
        query_all = low_back(low(projected[:, 0] + bq[0]))
        key_all = low_back(low(projected[:, 1]))
        value_all = low_back(low(projected[:, 2] + bq[1]))
        row_shape = (N_DP, ROWS, H, HD)

        def row_step(state_in, row_item):
            return (state_in, jax.checkpoint(attend_row)(row_item[0], row_item[1], row_item[2], row_item[3]))
        unused, context = lax.scan(row_step, jnp.zeros((), jnp.float32), (query_all.reshape(row_shape), key_all.reshape(row_shape), value_all.reshape(row_shape), segment_ids))
        context = low_back(low(context.reshape(TOKENS, D)))
        attention = low_back(product(context, wo) + bo)
        hidden1 = layer_norm(inputs + attention, gain1, shift1)
        hidden_pre = low_back(product(low(hidden1), wu) + bu)
        activated = low(jax.nn.gelu(hidden_pre, approximate=False))
        feed_out = low_back(product(activated, wd) + bd)
        return layer_norm(hidden1 + feed_out, gain2, shift2)
    params = [p.astype(jnp.float32) for p in (w_qkv, b_qv, w_out, b_out, norm1_gain, norm1_bias, w_up, b_up, w_down, b_down, norm2_gain, norm2_bias)]
    output, pullback = jax.vjp(forward, tokens.astype(jnp.float32), params[0], params[1], params[2], params[3], params[4], params[5], params[6], params[7], params[8], params[9], params[10], params[11])
    grads = pullback(out_grad.astype(jnp.float32))
    return (output.astype(jnp.bfloat16), grads[0].astype(jnp.bfloat16), grads[1], grads[2], grads[3], grads[4], grads[5], grads[6], grads[7], grads[8], grads[9], grads[10], grads[11], grads[12])
```

```python
import functools
import math
from types import SimpleNamespace

import jax
import jax.numpy as jnp
from jax import lax
from jax.experimental import pallas as pl
from jax.experimental.pallas import tpu as pltpu
from jax.sharding import PartitionSpec as P

HD = 64
MESH = pl.DeviceIdType.MESH
BF = jnp.bfloat16
F32 = jnp.float32
NEG = -1e30
VMEM_LIMIT = 67043328
MID, GF, FSND, FRCV = 0, 2, 4, 5


def nn(a, b):
    return jnp.dot(a, b, preferred_element_type=F32)


def nt(a, b):
    return lax.dot_general(a, b, (((1,), (1,)), ((), ())), preferred_element_type=F32)


def merge(x):
    return x.reshape(-1, x.shape[-1])


def spin(lo, hi, body):
    def step(i, carry):
        body(i)
        return carry

    lax.fori_loop(lo, hi, step, 0)


def order_table(T):
    return [sorted(range(T), key=lambda b: (abs(b - a), b if a < T / 2 else -b)) for a in range(T)]


def layer_kernel(cf, names, *refs):
    r = SimpleNamespace(**dict(zip(names, refs)))
    T, NQ, TB, D, R, C, HC, DP = cf.T, cf.NQ, cf.TB, cf.D, cf.R, cf.C, cf.HC, cf.DP
    S = NQ // 2
    RW = T * TB
    RC = 32
    heads = C // HD
    table = order_table(T)

    d = lax.axis_index("dp")
    t = lax.axis_index("tensor")
    q = lax.div(d, 2)
    c = d - 2 * q
    oc = 1 - c
    partner = (2 * q + oc, t)

    def perm(x):
        if NQ % 4:
            return x
        m = lax.rem(x, 4)
        return x + lax.div(m, 2) * (1 - 2 * lax.rem(m, 2))

    pos = perm(q)

    def chip_at(x):
        return perm(lax.rem(x + 4 * NQ, NQ))

    nxt = (2 * chip_at(pos + 1) + c, t)
    prv = (2 * chip_at(pos - 1) + c, t)

    def ind(a, b, n):
        x = lax.rem(a - b + n, n)
        return 1 - lax.div(x + n - 1, n)

    def tp(j):
        if isinstance(j, int):
            return sum(table[a][j] * ind(t, a, T) for a in range(T))
        js = [ind(j, b, T) for b in range(T)]
        total = 0
        for a in range(T):
            total = total + ind(t, a, T) * sum(table[a][b] * js[b] for b in range(T))
        return total

    def copy(src, dst, ss, rs, dev):
        return pltpu.make_async_remote_copy(
            src_ref=src, dst_ref=dst, send_sem=ss, recv_sem=rs, device_id=dev, device_id_type=MESH
        )

    def go(cp, op):
        if op == "start":
            cp.start()
        else:
            cp.wait_send()

    def half(kd, ref, h):
        if kd.split:
            return ref.at[h]
        n = kd.rows // 2
        return ref.at[pl.ds(h * n, n)]

    kt = SimpleNamespace(piece=lambda tt, qq: r.X.at[tt], zs=r.t_zs, zr=r.t_zr)
    kq = SimpleNamespace(
        piece=lambda tt, qq: r.Wq.at[2 * qq + c], split=False, rows=R, rs=r.q_rs, rr=r.q_rr,
        gs=r.q_gs, gr=r.q_gr, HB=r.q_HB, FB=r.q_FB,
    )
    ko = SimpleNamespace(
        piece=lambda tt, qq: r.Wo.at[tt, 2 * qq + c], split=False, rows=R, zs=r.o_zs, zr=r.o_zr,
        rs=r.o_rs, rr=r.o_rr, gs=r.o_gs, gr=r.o_gr, HB=r.o_HB, FB=r.o_FB,
        cs=r.o_cs, cr=r.o_cr, ZB=r.o_ZB,
    )
    ku = SimpleNamespace(
        piece=lambda tt, qq: r.Wu.at[tt, qq], split=True, rows=2 * R, zs=r.u_zs, zr=r.u_zr,
        rs=r.u_rs, rr=r.u_rr, gs=r.u_gs, gr=r.u_gr, HB=r.u_HB, FB=r.u_FB,
        cs=r.u_cs, cr=r.u_cr, ZB=r.u_ZB,
    )
    kd_ = SimpleNamespace(
        piece=lambda tt, qq: r.Wd.at[tt, qq], split=True, rows=2 * R, zs=r.d_zs, zr=r.d_zr,
        rs=r.d_rs, rr=r.d_rr, gs=r.d_gs, gr=r.d_gr, HB=r.d_HB, FB=r.d_FB,
        cs=r.d_cs, cr=r.d_cr, ZB=r.d_ZB,
    )
    kg = SimpleNamespace(piece=lambda tt, qq: r.POOL.at[tt], cs=r.g_cs, cr=r.g_cr, ZB=r.g_ZB)

    def z_right(k, tt, op):
        @pl.when((tt <= t) & (t < T - 1))
        def _():
            ref = k.piece(tt, q)
            go(copy(ref, ref, k.zs.at[tt, 0], k.zr.at[tt], (d, t + 1)), op)

    def z_left(k, tt, op):
        @pl.when((tt >= t) & (t > 0))
        def _():
            ref = k.piece(tt, q)
            go(copy(ref, ref, k.zs.at[tt, 1], k.zr.at[tt], (d, t - 1)), op)

    def z_send(k, tt, op="start"):
        z_right(k, tt, op)
        z_left(k, tt, op)

    def z_wait(k, tt):
        ref = k.piece(tt, q)
        copy(ref, ref, k.zs.at[tt, 0], k.zr.at[tt], partner).wait_recv()

    def ring_send(k, tt, s, op="start"):
        a = k.piece(tt, chip_at(pos - s))
        b = k.piece(tt, chip_at(pos + s))
        if s == S - 1:
            a, b = half(k, a, 0), half(k, b, 1)
        go(copy(a, a, k.rs.at[tt, 0, s], k.rr.at[tt, 0, s], nxt), op)
        go(copy(b, b, k.rs.at[tt, 1, s], k.rr.at[tt, 1, s], prv), op)

    def ring_wait(k, tt, s):
        a = k.piece(tt, chip_at(pos - 1 - s))
        b = k.piece(tt, chip_at(pos + 1 + s))
        if s == S - 1:
            a, b = half(k, a, 0), half(k, b, 1)
        copy(a, a, k.rs.at[tt, 0, s], k.rr.at[tt, 0, s], nxt).wait_recv()
        copy(b, b, k.rs.at[tt, 1, s], k.rr.at[tt, 1, s], prv).wait_recv()

    def twin_o(tt, qq):
        ref = r.Wo.at[tt, 2 * qq + c]
        copy(ref, ref, r.tw_s.at[0], r.tw_r.at[0], partner).start()

    def twin_q(tt, qq):
        ref = r.Wq.at[2 * qq + c]
        copy(ref, ref, r.tw_s.at[1], r.tw_r.at[1], partner).start()

    def arrived(k, tt, s, twin):
        ring_wait(k, tt, s)
        if twin is not None:
            twin(tt, chip_at(pos + 1 + s))
            if s < S - 1:
                twin(tt, chip_at(pos - 1 - s))

    def ring_adv(k, tt, twin=None):
        for s in range(1, S):
            arrived(k, tt, s - 1, twin)
            ring_send(k, tt, s)

    def ring_fin(k, tt, twin=None):
        arrived(k, tt, S - 1, twin)

    def add(dst, src):
        dst[...] = (dst[...].astype(F32) + src[...].astype(F32)).astype(BF)

    def rs_send(k, tt, s, op="start"):
        a = k.piece(tt, chip_at(pos + S - s))
        b = k.piece(tt, chip_at(pos - S + s))
        if s == 0:
            a, b = half(k, a, 0), half(k, b, 1)
            da, db = k.HB.at[tt, 0], k.HB.at[tt, 1]
        else:
            da, db = k.FB.at[tt, 0, s - 1], k.FB.at[tt, 1, s - 1]
        go(copy(a, da, k.gs.at[tt, 0, s], k.gr.at[tt, 0, s], nxt), op)
        go(copy(b, db, k.gs.at[tt, 1, s], k.gr.at[tt, 1, s], prv), op)

    def rs_add(k, tt, s):
        a = k.piece(tt, chip_at(pos + S - s - 1))
        b = k.piece(tt, chip_at(pos - S + s + 1))
        if s == 0:
            a, b = half(k, a, 0), half(k, b, 1)
            da, db = k.HB.at[tt, 0], k.HB.at[tt, 1]
        else:
            da, db = k.FB.at[tt, 0, s - 1], k.FB.at[tt, 1, s - 1]
        copy(da, da, k.gs.at[tt, 0, s], k.gr.at[tt, 0, s], nxt).wait_recv()
        add(a, da)
        copy(db, db, k.gs.at[tt, 1, s], k.gr.at[tt, 1, s], prv).wait_recv()
        add(b, db)

    def rs_mid(k, tt):
        for s in range(1, S):
            rs_add(k, tt, s - 1)
            rs_send(k, tt, s)

    def rs_last(k, tt):
        rs_add(k, tt, S - 1)

    def chain_send(k, tt, op="start"):
        ref = k.piece(tt, q)

        @pl.when(tt > t)
        def _():
            go(copy(ref, k.ZB.at[tt], k.cs.at[tt], k.cr.at[tt], (d, t + 1)), op)

        @pl.when(tt < t)
        def _():
            slot = tt + (T - tt) * ind(tt, t - 1, T)
            go(copy(ref, k.ZB.at[slot], k.cs.at[tt], k.cr.at[slot], (d, t - 1)), op)

    def chain_take(k, tt, slot):
        copy(k.ZB.at[slot], k.ZB.at[slot], k.cs.at[tt], k.cr.at[slot], partner).wait_recv()
        add(k.piece(tt, q), k.ZB.at[slot])

    def chain(k, tt):
        @pl.when(((tt >= t) & (t > 0)) | ((tt < t) & (t < T - 1)))
        def _():
            chain_take(k, tt, tt)

        @pl.when((tt == t) & (t < T - 1))
        def _():
            chain_take(k, tt, T)

        chain_send(k, tt)

    barrier = pltpu.get_barrier_semaphore()
    peers = [partner]
    peers += [(2 * lax.rem(q + k, NQ) + c, t) for k in range(1, NQ)]
    peers += [(d, lax.rem(t + k, T)) for k in range(1, T)]
    for peer in peers:
        pl.semaphore_signal(barrier, inc=1, device_id=peer, device_id_type=MESH)
    get_tok = pltpu.make_async_copy(r.tok, r.X.at[t], r.in_s.at[0])
    get_tok.start()
    get_og = pltpu.make_async_copy(r.og, r.out, r.in_s.at[1])
    get_og.start()
    r.Wq[d] = r.wq[...]
    r.Wo[t, d] = r.wo[...]
    lo = pl.multiple_of(c * HC, 128)
    r.Wu[t, q, c] = r.wu[:, pl.ds(lo, HC)]
    r.Wd[t, q, c] = r.wd[:, pl.ds(lo, HC)]
    ro = pl.multiple_of(oc * HC, 128)
    r.FSW[0] = r.wu[:, pl.ds(ro, HC)]
    r.FSW[1] = r.wd[:, pl.ds(ro, HC)]
    r.BU[t] = r.bup[c]
    get_tok.wait()
    get_og.wait()
    pl.semaphore_wait(barrier, len(peers))

    z_send(kt, t)
    z_send(ko, t)
    twin_q(0, q)
    ring_send(kq, 0, 0)
    swap_u = copy(r.FSW.at[0], r.Wu.at[t, q, c], r.sw_s.at[0], r.sw_r.at[0], partner)
    swap_d = copy(r.FSW.at[1], r.Wd.at[t, q, c], r.sw_s.at[1], r.sw_r.at[1], partner)
    swap_u.start()
    swap_d.start()
    twin_o(t, q)
    ring_send(ko, t, 0)
    for k in range(1, T):
        tt = lax.rem(t + k, T)
        copy(r.BU.at[t], r.BU.at[t], r.b_s.at[tt], r.b_r.at[t], (d, tt)).start()
    r.SACC[...] = jnp.zeros_like(r.SACC)
    r.SB[...] = jnp.zeros_like(r.SB)
    r.DK[...] = jnp.zeros_like(r.DK)
    r.DV[...] = jnp.zeros_like(r.DV)
    for n, (ref, w) in enumerate(((r.Wu, ku), (r.Wd, kd_))):
        copy(ref.at[t, q, oc], ref.at[t, q, oc], r.sw_s.at[n], r.sw_r.at[n], partner).wait_recv()
        ring_send(w, t, 0)

    def weights_z(tt):
        @pl.when(tt == 0)
        def _():
            z_right(ku, t, "start")

        @pl.when(tt == T - 1)
        def _():
            z_left(ku, t, "start")

    def project(tt):
        x = r.X[tt]
        at = pl.ds(pl.multiple_of(tt * TB, TB), TB)
        for part, name in enumerate(("Q", "K", "V")):
            w = merge(r.Wq[:, :, part * C : (part + 1) * C])
            y = nn(x, w) + r.bqkv[:, part * C : (part + 1) * C]
            y = y.astype(BF)
            if part == 0:
                r.Q[at, :] = y * jnp.asarray(HD ** (-0.5), BF)
            elif part == 1:
                r.K[at, :] = y
                r.KT[:, at] = y.astype(F32).T.astype(BF)
            else:
                r.V[at, :] = y
                r.VT[:, at] = y.astype(F32).T.astype(BF)

    weights_z(t)
    for s in range(S):
        arrived(kq, 0, s, twin_q)
        if s + 1 < S:
            ring_send(kq, 0, s + 1)
    copy(r.RQ, r.RQ, r.tw_s.at[1], r.tw_r.at[1], partner).wait_recv()
    project(t)
    for j in range(1, T):
        tt = tp(j)
        z_wait(kt, tt)
        z_send(kt, tt)
        z_wait(ko, tt)
        z_send(ko, tt)
        weights_z(tt)
        twin_o(tt, q)
        ring_send(ko, tt, 0)
        ring_adv(ko, tp(j - 1), twin_o)
        if j == 1:
            ring_adv(ku, t)
            ring_adv(kd_, t)
        else:
            ring_fin(ko, tp(j - 2), twin_o)
        project(tt)
    ring_adv(ko, tp(T - 1), twin_o)
    if T > 1:
        ring_fin(ko, tp(T - 2), twin_o)
    ring_fin(ko, tp(T - 1), twin_o)

    line = [(ku, j) for j in range(1, T)] + [(kd_, j) for j in range(1, T)]
    done = [0]

    def serve():
        n = done[0]
        done[0] += 1
        if n > len(line):
            return
        if n > 0:
            ring_adv(line[n - 1][0], tp(line[n - 1][1]))
        if n < len(line):
            k, j = line[n]
            tt = tp(j)
            z_wait(k, tt)
            z_send(k, tt)
            if n == 0:
                z_send(kd_, t)
            ring_send(k, tt, 0)

    lane = lax.broadcasted_iota(jnp.int32, (1, 128), 1)
    picks = [(lane < HD).astype(F32).astype(BF), (lane >= HD).astype(F32).astype(BF)]

    def bias_for(i):
        same = r.segc[:, 0:1] == r.segr[i]
        r.BIAS[...] = jnp.where(same, 0.0, NEG)

    def attend(j):
        i = lax.rem(t + 1 + j, T)
        at = pl.ds(pl.multiple_of(i * TB, TB), TB)
        bias_for(i)
        for h in range(heads):
            pair = slice((h // 2) * 128, (h // 2) * 128 + 128)
            qh = r.Q[at, pair] * picks[h % 2]
            sc = nt(r.K[:, pair], qh) + r.BIAS[...]
            top = jnp.max(sc, axis=0, keepdims=True)
            e = jnp.exp(sc - top)
            total = jnp.sum(e, axis=0, keepdims=True)
            ct = nn(r.VT[h * HD : (h + 1) * HD, :], e.astype(BF))
            r.CT[h * HD : (h + 1) * HD, :] = ct / total
            r.LSE[i, h : h + 1, :] = top + jnp.log(total)
        r.CXR[i] = r.CT[...].T.astype(BF)

        @pl.when(i != t)
        def _():
            copy(r.CXR.at[i], r.CTX.at[t], r.c_s.at[i], r.c_r.at[t], (d, i)).start()

    spin(0, T // 2, attend)
    serve()
    spin(T // 2, T, attend)
    serve()
    r.CTX[t] = r.CXR[t]
    for k in range(1, T):
        tt = lax.rem(t + k, T)
        copy(r.CTX.at[tt], r.CTX.at[tt], r.c_s.at[tt], r.c_r.at[tt], partner).wait_recv()
    copy(r.RWO, r.RWO, r.tw_s.at[0], r.tw_r.at[0], partner).wait_recv()

    def out_dot(j):
        y = nt(r.CTX[j], merge(r.Wo[j]))

        @pl.when(j == 0)
        def _():
            r.FEED[0] = y

        @pl.when(j > 0)
        def _():
            r.FEED[0] += y

    spin(0, T, out_dot)

    def rows_of(body):
        def step(i):
            body(pl.ds(pl.multiple_of(i * RC, RC), RC))

        spin(0, TB // RC, step)

    def tally(n, x):
        r.SACC[n] += x.reshape(RC // 8, 8, D).sum(axis=0)

    def norm(x):
        mid = x - jnp.mean(x, axis=-1, keepdims=True)
        inverse = lax.rsqrt(jnp.mean(mid * mid, axis=-1, keepdims=True) + 1e-05)
        return mid * inverse, inverse

    def norm_back(up, gain, normed, inverse):
        e = up * gain
        return inverse * (
            e - jnp.mean(e, axis=-1, keepdims=True) - normed * jnp.mean(e * normed, axis=-1, keepdims=True)
        )

    def vec(n):
        return r.vecs[n : n + 1, :]

    def first_norm(at):
        x = r.X[t, at, :].astype(F32) + r.FEED[0, at, :] + vec(0)
        normed, inverse = norm(x)
        h1 = normed * vec(1) + vec(2)
        r.N1[at, :] = normed
        r.IV1[at, :] = inverse
        r.H1[at, :] = h1
        r.POOL[MID + c, at, :] = h1.astype(BF)

    rows_of(first_norm)

    def exchange(n, base, op="start"):
        ref = r.POOL.at[base + c]
        go(copy(ref, ref, r.e_s.at[n], r.e_r.at[n], partner), op)

    def exchanged(n, base):
        ref = r.POOL.at[base + oc]
        copy(ref, ref, r.e_s.at[n], r.e_r.at[n], partner).wait_recv()

    exchange(0, MID)
    for k in range(1, T):
        tt = lax.rem(t + k, T)
        copy(r.BU.at[tt], r.BU.at[tt], r.b_s.at[tt], r.b_r.at[tt], partner).wait_recv()
    exchanged(0, MID)

    def turn(src, dst):
        def step(b):
            y = r.POOL[src + b].astype(F32).T.astype(BF)
            dst[:, pl.ds(pl.multiple_of(b * TB, TB), TB)] = y

        spin(0, 2, step)

    def up(j):
        tt = tp(j)
        ring_fin(ku, tt)
        w = merge(r.Wu[tt])
        bias = r.BU[tt]

        def block(b):
            r.PRE[...] = nn(r.POOL[MID + b], w) + bias

            def piece(i):
                at = pl.ds(pl.multiple_of(i * RC, RC), RC)
                v = r.PRE[at, :]
                cdf = 0.5 * (1.0 + lax.erf(v * 2.0 ** (-0.5)))
                slope = cdf + v * jnp.exp(-0.5 * v * v) * (2.0 * math.pi) ** (-0.5)
                to = pl.ds(pl.multiple_of(b * TB + i * RC, RC), RC)
                r.ACT[tt, to, :] = (v * cdf).astype(BF)
                r.SL[tt, to, :] = slope.astype(BF)

            spin(0, TB // RC, piece)

        spin(0, 2, block)

    up(0)
    for j in range(1, T):
        serve()
        up(j)
    turn(MID, r.MIDT)

    def down(j):
        tt = tp(j)
        ring_fin(kd_, tt)
        w = merge(r.Wd[tt])

        def block(b):
            y = nt(r.ACT[tt, pl.ds(pl.multiple_of(b * TB, TB), TB), :], w)
            if j == 0:
                r.FEED[b] = y
            else:
                r.FEED[b] += y

        spin(0, 2, block)

    for j in range(T):
        serve()
        down(j)
    while done[0] <= len(line):
        serve()

    def give(n):
        def step(at):
            r.POOL[FSND, at, :] = r.FEED[oc, at, :].astype(BF)

        rows_of(step)
        copy(r.POOL.at[FSND], r.POOL.at[FRCV], r.e_s.at[n], r.e_r.at[n], partner).start()
        copy(r.POOL.at[FRCV], r.POOL.at[FRCV], r.e_s.at[n], r.e_r.at[n], partner).wait_recv()
        copy(r.POOL.at[FSND], r.POOL.at[FRCV], r.e_s.at[n], r.e_r.at[n], partner).wait_send()

    def given(n, at):
        return r.FEED[c, at, :] + r.POOL[FRCV, at, :].astype(F32)

    give(1)

    def second_norm(at):
        x = r.H1[at, :] + given(1, at) + vec(3)
        normed, inverse = norm(x)
        g = r.out[at, :].astype(F32)
        r.out[at, :] = (normed * vec(4) + vec(5)).astype(BF)
        tally(0, g * normed)
        tally(1, g)
        back = norm_back(g, vec(4), normed, inverse)
        r.H1[at, :] = back
        low = back.astype(BF)
        r.POOL[GF + c, at, :] = low
        tally(2, low.astype(F32))

    rows_of(second_norm)
    exchange(2, GF)

    def drain_gather(k):
        def step(tt):
            if hasattr(k, "zs"):
                z_send(k, tt, "drain")
            for s in range(S):
                ring_send(k, tt, s, "drain")

        spin(0, T, step)

    drain_gather(ku)
    drain_gather(kd_)
    swap_u.wait_send()
    swap_d.wait_send()
    exchanged(2, GF)
    turn(GF, r.GFT)

    def slot_back(k):
        tt = tp(T - 1 - k)

        def block(b):
            to = pl.ds(pl.multiple_of(b * TB, TB), TB)
            r.PRE[...] = nn(r.POOL[GF + b], merge(r.Wd[tt]))

            def piece(i):
                at = pl.ds(pl.multiple_of(i * RC, RC), RC)
                tr = pl.ds(pl.multiple_of(b * TB + i * RC, RC), RC)
                gp = (r.PRE[at, :] * r.SL[tt, tr, :].astype(F32)).astype(BF)
                r.SL[tt, tr, :] = gp
                r.SBA[...] += gp.astype(F32).reshape(RC // 8, 8, HC).sum(axis=0)

            spin(0, TB // RC, piece)
            y = nt(r.SL[tt, to, :], merge(r.Wu[tt]))

            @pl.when(k == 0)
            def _():
                r.FEED[b] = y

            @pl.when(k > 0)
            def _():
                r.FEED[b] += y

        r.SBA[...] = jnp.zeros_like(r.SBA)
        spin(0, 2, block)
        r.SB[pl.ds(2 * tt + c, 1)] = r.SBA[...].sum(axis=0, keepdims=True)[None]

        def weight(qq):
            at = pl.ds(pl.multiple_of(qq * 2 * R, 2 * R), 2 * R)
            y = nn(r.GFT[at, :], r.ACT[tt])
            r.Wd[tt, qq] = y.astype(BF).reshape(2, R, HC)
            y = nn(r.MIDT[at, :], r.SL[tt])
            r.Wu[tt, qq] = y.astype(BF).reshape(2, R, HC)

        spin(0, NQ, weight)
        rs_send(kd_, tt, 0)
        rs_send(ku, tt, 0)

    spin(0, T, slot_back)
    give(3)

    def first_back(at):
        g = r.H1[at, :] + given(3, at)
        normed = r.N1[at, :]
        tally(3, g * normed)
        tally(4, g)
        back = norm_back(g, vec(1), normed, r.IV1[at, :])
        r.H1[at, :] = back
        low = back.astype(BF)
        r.gtok[at, :] = low
        tally(5, low.astype(F32))

    rows_of(first_back)

    def context_back(k):
        tt = tp(T - 1 - k)
        r.CXR[tt] = nn(r.gtok[...], merge(r.Wo[tt])).astype(BF)

        @pl.when(tt != t)
        def _():
            copy(r.CXR.at[tt], r.GC.at[t], r.gc_s.at[tt], r.gc_r.at[t], (d, tt)).start()

        @pl.when(tt == t)
        def _():
            r.GC[t] = r.CXR[t]

    for k in range(1, T):
        tt = lax.rem(t + k, T)
        copy(r.CXR.at[tt], r.CTX.at[t], r.c_s.at[tt], r.c_r.at[t], (d, tt)).wait_send()
    spin(0, T, context_back)
    drain_gather(ko)
    copy(r.RWO, r.RWO, r.tw_s.at[0], r.tw_r.at[0], partner).wait_send()

    r.GFT[:, 0:TB] = r.gtok[...].astype(F32).T.astype(BF)

    def out_back(tt):
        def weight(qq):
            at = pl.ds(pl.multiple_of(qq * 2 * R, 2 * R), 2 * R)
            y = nn(r.GFT[at, 0:TB], r.CTX[tt]).astype(BF)
            r.Wo[tt, pl.ds(2 * qq, 2)] = y.reshape(2, R, C)
            copy(r.Wo.at[tt, 2 * qq + oc], r.RWO.at[tt, qq], r.go_s.at[0], r.go_r.at[0], partner).start()

        spin(0, NQ, weight)

    spin(0, T, out_back)

    for n in range(6):
        r.SV[n : n + 1, :] = r.SACC[n].sum(axis=0, keepdims=True)
    r.SV[6:8, :] = jnp.zeros((2, D), F32)

    def sum_core(n, ref, box, op):
        cp = copy(ref, box, r.a_s.at[0, n], r.a_r.at[0, n], partner)
        if op == "start":
            cp.start()
        else:
            copy(box, box, r.a_s.at[0, n], r.a_r.at[0, n], partner).wait_recv()
            cp.wait_send()
            ref[...] += box[...]

    def sum_group(stage, n, ref, box, me, count, dev, op):
        if op == "start":
            box[me] = ref[...]
        for k in range(1, count):
            other = lax.rem(me + k, count)
            sems = r.ag_s.at[stage, n, other], r.ag_r.at[stage, n, me]
            if op == "start":
                copy(box.at[me], box.at[me], *sems, dev(other)).start()
            else:
                copy(box.at[me], box.at[me], *sems, dev(other)).wait_send()
                copy(
                    box.at[other], box.at[other], r.ag_s.at[stage, n, other],
                    r.ag_r.at[stage, n, other], dev(other),
                ).wait_recv()
        if op != "start":
            total = box[0]
            for k in range(1, count):
                total = total + box[k]
            ref[...] = total

    def chip_dev(other):
        return (2 * other + c, t)

    def row_dev(other):
        return (d, other)

    sum_core(0, r.SV, r.SV1, "start")
    sum_core(1, r.SB, r.SB1, "start")

    copy(r.RWO, r.RWO, r.go_s.at[0], r.go_r.at[0], partner).wait_recv()

    def out_join(k):
        tt = tp(T - 1 - k)

        def step(qq):
            add(r.Wo.at[tt, 2 * qq + c], r.RWO.at[tt, qq])

        spin(0, NQ, step)
        rs_send(ko, tt, 0)

    spin(0, T, out_join)
    sum_core(0, r.SV, r.SV1, "end")
    sum_core(1, r.SB, r.SB1, "end")
    sum_group(0, 0, r.SV, r.SV2, q, NQ, chip_dev, "start")
    sum_group(0, 1, r.SB, r.SB2, q, NQ, chip_dev, "start")

    def attend_back(j):
        i = tp(j)
        at = pl.ds(pl.multiple_of(i * TB, TB), TB)

        @pl.when(i != t)
        def _():
            copy(r.GC.at[i], r.GC.at[i], r.gc_s.at[i], r.gc_r.at[i], partner).wait_recv()

        bias_for(i)
        for h in range(heads):
            pair = slice((h // 2) * 128, (h // 2) * 128 + 128)
            qh = r.Q[at, pair] * picks[h % 2]
            gh = r.GC[i, :, pair] * picks[h % 2]
            pr = jnp.exp(nt(r.K[:, pair], qh) + r.BIAS[...] - r.LSE[i, h : h + 1, :])
            gp = nt(r.V[:, pair], gh)
            r.DV[:, pair] += nn(pr.astype(BF), gh)
            prod = pr * gp
            delta = jnp.sum(prod, axis=0, keepdims=True)
            ds = (prod - pr * delta).astype(BF)
            r.DK[:, pair] += nn(ds, qh)
            r.CT[h * HD : (h + 1) * HD, :] = nn(r.KT[h * HD : (h + 1) * HD, :], ds) * HD ** (-0.5)
        r.DPJ[i, :, 0:C] = r.CT[...].T.astype(BF)
        tt = tp(T - 1 - j)
        rs_mid(kd_, tt)
        rs_mid(ku, tt)
        rs_mid(ko, tt)

    spin(0, T, attend_back)
    sum_group(0, 0, r.SV, r.SV2, q, NQ, chip_dev, "end")
    sum_group(0, 1, r.SB, r.SB2, q, NQ, chip_dev, "end")
    sum_group(1, 0, r.SV, r.SV3, t, T, row_dev, "start")
    sum_group(1, 1, r.SB, r.SB3, t, T, row_dev, "start")

    exchange(0, MID, "drain")
    exchange(2, GF, "drain")

    r.SQ[...] = jnp.zeros_like(r.SQ)

    def input_back(k):
        tt = tp(T - 1 - k)
        at = pl.ds(pl.multiple_of(tt * TB, TB), TB)
        r.DPJ[tt, :, C : 2 * C] = r.DK[at, :].astype(BF)
        r.DPJ[tt, :, 2 * C : 3 * C] = r.DV[at, :].astype(BF)
        r.SQ[0:1, :] += r.DPJ[tt, :, 0:C].astype(F32).sum(axis=0, keepdims=True)
        r.SQ[1:2, :] += r.DPJ[tt, :, 2 * C : 3 * C].astype(F32).sum(axis=0, keepdims=True)
        r.POOL[tt] = nt(r.DPJ[tt], merge(r.Wq[...])).astype(BF)

        @pl.when(tt != t)
        def _():
            chain(kg, tt)

    spin(0, T, input_back)

    def settle(k, tt):
        rs_last(k, tt)

        @pl.when(tt != t)
        def _():
            chain(k, tt)

    sum_core(2, r.SQ, r.SQ1, "start")
    settle(kd_, tp(T - 1))
    settle(ku, tp(T - 1))

    copy(r.RQ, r.RQ, r.tw_s.at[1], r.tw_r.at[1], partner).wait_send()
    for s in range(S):
        ring_send(kq, 0, s, "drain")

    many = max(2, 256 // R)

    def qkv_weight(g):
        cols = pl.ds(pl.multiple_of(g * many * R, 128), many * R)
        x = merge(r.X[:, :, cols])
        y = lax.dot_general(
            x, merge(r.DPJ[...]), (((0,), (0,)), ((), ())), preferred_element_type=F32
        )
        r.Wq[pl.ds(many * g, many)] = y.astype(BF).reshape(many, R, 3 * C)
        for k in range(many // 2):
            qq = g * (many // 2) + k
            copy(r.Wq.at[2 * qq + oc], r.RQ.at[qq], r.go_s.at[1], r.go_r.at[1], partner).start()

    spin(0, DP // many, qkv_weight)
    sum_core(2, r.SQ, r.SQ1, "end")
    sum_group(0, 2, r.SQ, r.SQ2, q, NQ, chip_dev, "start")
    copy(r.RQ, r.RQ, r.go_s.at[1], r.go_r.at[1], partner).wait_recv()

    def q_join(qq):
        add(r.Wq.at[2 * qq + c], r.RQ.at[qq])

    spin(0, NQ, q_join)
    rs_send(kq, 0, 0)
    settle(ko, tp(T - 1))
    for j in range(T - 2, 0, -1):
        settle(kd_, tp(j))
        settle(ku, tp(j))
        settle(ko, tp(j))
        if j == T - 2:
            rs_mid(kq, 0)
    rs_last(kd_, t)
    rs_last(ku, t)
    rs_last(ko, t)
    rs_last(kq, 0)
    sum_group(1, 0, r.SV, r.SV3, t, T, row_dev, "end")
    sum_group(1, 1, r.SB, r.SB3, t, T, row_dev, "end")
    sum_group(0, 2, r.SQ, r.SQ2, q, NQ, chip_dev, "end")
    chain(kg, t)

    def finish(at):
        r.gtok[at, :] = (r.H1[at, :] + r.POOL[t, at, :].astype(F32)).astype(BF)

    rows_of(finish)
    chain(kd_, t)
    chain(ku, t)
    chain(ko, t)
    cps = []
    for n, ref in enumerate((r.Wu, r.Wd)):
        cp = copy(ref.at[t, q, oc], r.FSW.at[n], r.fs_s.at[n], r.fs_r.at[n], partner)
        cp.start()
        cps.append(cp)
    r.gwq[...] = r.Wq[d].astype(F32)
    r.gwo[...] = r.Wo[t, d].astype(F32)
    r.sv[...] = r.SV[...]
    r.sbq[...] = r.SQ[...]
    r.sbu[...] = r.SB[pl.ds(2 * t, 2)]
    for n, (ref, o) in enumerate(((r.Wu, r.gwu), (r.Wd, r.gwd))):
        copy(r.FSW.at[n], r.FSW.at[n], r.fs_s.at[n], r.fs_r.at[n], partner).wait_recv()
        o[:, pl.ds(lo, HC)] = ref[t, q, c].astype(F32)
        o[:, pl.ds(ro, HC)] = r.FSW[n].astype(F32)
        cps[n].wait_send()

    def drain(tt):
        z_send(kt, tt, "drain")
        for k in (kd_, ku, ko):
            for s in range(S):
                rs_send(k, tt, s, "drain")
            chain_send(k, tt, "drain")
        chain_send(kg, tt, "drain")

        @pl.when(tt != t)
        def _():
            copy(r.CXR.at[tt], r.GC.at[t], r.gc_s.at[tt], r.gc_r.at[t], (d, tt)).wait_send()
            copy(r.BU.at[t], r.BU.at[t], r.b_s.at[tt], r.b_r.at[t], (d, tt)).wait_send()

    spin(0, T, drain)
    for s in range(S):
        rs_send(kq, 0, s, "drain")
    copy(r.RWO, r.RWO, r.go_s.at[0], r.go_r.at[0], partner).wait_send()
    copy(r.RQ, r.RQ, r.go_s.at[1], r.go_r.at[1], partner).wait_send()


def layer(cf, *args):
    T, NQ, TB, D, R, C, HC, DP = cf.T, cf.NQ, cf.TB, cf.D, cf.R, cf.C, cf.HC, cf.DP
    S = NQ // 2
    RW = T * TB
    Cq = 3 * C
    heads = C // HD
    hp = -(-heads // 8) * 8
    dma = pltpu.SemaphoreType.DMA
    V = pltpu.VMEM
    ins = ["tok", "og", "wq", "wo", "wu", "wd", "bqkv", "bup", "vecs", "segc", "segr"]
    outs = {
        "out": ((TB, D), BF), "gtok": ((TB, D), BF), "gwq": ((R, Cq), F32), "gwo": ((R, C), F32),
        "gwu": ((R, 2 * HC), F32), "gwd": ((R, 2 * HC), F32), "sv": ((8, D), F32),
        "sbq": ((8, C), F32), "sbu": ((2, 1, HC), F32),
    }
    scratch = {
        "X": V((T, TB, D), BF), "Wq": V((DP, R, Cq), BF), "Wo": V((T, DP, R, C), BF),
        "Wu": V((T, NQ, 2, R, HC), BF), "Wd": V((T, NQ, 2, R, HC), BF), "BU": V((T, 1, HC), F32),
        "Q": V((RW, C), BF), "K": V((RW, C), BF), "V": V((RW, C), BF),
        "KT": V((C, RW), BF), "VT": V((C, RW), BF), "BIAS": V((RW, TB), F32),
        "CT": V((C, TB), F32), "LSE": V((T, hp, TB), F32), "CXR": V((T, TB, C), BF),
        "CTX": V((T, TB, C), BF), "FEED": V((2, TB, D), F32), "N1": V((TB, D), F32),
        "IV1": V((TB, 1), F32), "H1": V((TB, D), F32), "POOL": V((max(6, T), TB, D), BF),
        "MIDT": V((D, 2 * TB), BF), "PRE": V((TB, HC), F32), "ACT": V((T, 2 * TB, HC), BF),
        "SL": V((T, 2 * TB, HC), BF),
        "GFT": V((D, 2 * TB), BF),
        "GC": V((T, TB, C), BF),
        "DK": V((RW, C), F32), "DV": V((RW, C), F32), "DPJ": V((T, TB, Cq), BF),
        "g_ZB": V((T + 1, TB, D), BF), "RWO": V((T, NQ, R, C), BF), "RQ": V((NQ, R, Cq), BF),
        "FSW": V((2, R, HC), BF),
        "q_HB": V((1, 2, R // 2, Cq), BF), "q_FB": V((1, 2, S - 1, R, Cq), BF),
        "o_HB": V((T, 2, R // 2, C), BF), "o_FB": V((T, 2, S - 1, R, C), BF), "o_ZB": V((T + 1, R, C), BF),
        "u_HB": V((T, 2, R, HC), BF), "u_FB": V((T, 2, S - 1, 2, R, HC), BF), "u_ZB": V((T + 1, 2, R, HC), BF),
        "d_HB": V((T, 2, R, HC), BF), "d_FB": V((T, 2, S - 1, 2, R, HC), BF), "d_ZB": V((T + 1, 2, R, HC), BF),
        "SACC": V((6, 8, D), F32), "SBA": V((8, HC), F32),
        "SV": V((8, D), F32), "SV1": V((8, D), F32), "SV2": V((NQ, 8, D), F32), "SV3": V((T, 8, D), F32),
        "SB": V((2 * T, 1, HC), F32), "SB1": V((2 * T, 1, HC), F32), "SB2": V((NQ, 2 * T, 1, HC), F32),
        "SB3": V((T, 2 * T, 1, HC), F32),
        "SQ": V((8, C), F32), "SQ1": V((8, C), F32), "SQ2": V((NQ, 8, C), F32),
        "t_zs": dma((T, 2)), "t_zr": dma((T,)),
        "q_rs": dma((1, 2, S)), "q_rr": dma((1, 2, S)), "q_gs": dma((1, 2, S)), "q_gr": dma((1, 2, S)),
        "tw_s": dma((2,)), "tw_r": dma((2,)), "sw_s": dma((2,)), "sw_r": dma((2,)),
        "b_s": dma((T,)), "b_r": dma((T,)), "c_s": dma((T,)), "c_r": dma((T,)),
        "e_s": dma((4,)), "e_r": dma((4,)), "gc_s": dma((T,)), "gc_r": dma((T,)),
        "go_s": dma((2,)), "go_r": dma((2,)), "g_cs": dma((T,)), "g_cr": dma((T + 1,)),
        "a_s": dma((1, 3)), "a_r": dma((1, 3)),
        "ag_s": dma((2, 3, max(NQ, T))), "ag_r": dma((2, 3, max(NQ, T))),
        "fs_s": dma((2,)), "fs_r": dma((2,)), "in_s": dma((2,)),
    }
    for n in "oud":
        scratch[n + "_zs"] = dma((T, 2))
        scratch[n + "_zr"] = dma((T,))
        for m in ("_rs", "_rr", "_gs", "_gr"):
            scratch[n + m] = dma((T, 2, S))
        scratch[n + "_cs"] = dma((T,))
        scratch[n + "_cr"] = dma((T + 1,))
    names = ins + list(outs) + list(scratch)
    vm = pl.BlockSpec(memory_space=pltpu.VMEM)
    return pl.pallas_call(
        functools.partial(layer_kernel, cf, names),
        out_shape=tuple(jax.ShapeDtypeStruct(s, k) for s, k in outs.values()),
        in_specs=[pl.BlockSpec(memory_space=pl.ANY)] * 2 + [vm] * (len(ins) - 2),
        out_specs=(vm,) * len(outs),
        scratch_shapes=list(scratch.values()),
        compiler_params=pltpu.CompilerParams(
            collective_id=0, has_side_effects=True, vmem_limit_bytes=VMEM_LIMIT
        ),
        name="layer",
    )(*args)


def shards(
    tokens, segment_ids, out_grad, w_qkv, b_qv, w_out, b_out, norm1_gain, norm1_bias,
    w_up, b_up, w_down, b_down, norm2_gain, norm2_bias,
):
    DP, T = lax.axis_size("dp"), lax.axis_size("tensor")
    TB, D = tokens.shape
    R, _, C = w_qkv.shape
    HC = w_up.shape[1] // 2
    RW = segment_ids.shape[1]
    cf = SimpleNamespace(T=T, NQ=DP // 2, TB=TB, D=D, R=R, C=C, HC=HC, DP=DP)
    bq = b_qv.astype(F32)
    bqkv = jnp.concatenate([bq[0:1], jnp.zeros_like(bq[0:1]), bq[1:2]], axis=1)
    vecs = jnp.stack(
        [b_out, norm1_gain, norm1_bias, b_down, norm2_gain, norm2_bias, b_out, b_out]
    ).astype(F32)
    segc = jnp.broadcast_to(segment_ids[0][:, None], (RW, 128))
    segr = segment_ids.reshape(T, 1, TB)
    res = layer(
        cf, tokens, out_grad, w_qkv.reshape(R, 3 * C), w_out.T, w_up, w_down.T, bqkv,
        b_up.astype(F32).reshape(2, 1, HC), vecs, segc, segr,
    )
    out, gtok, gwq, gwo, gwu, gwd, sv, sbq, sbu = res
    return (
        out, gtok, gwq.reshape(R, 3, C), sbq[0:2], gwo.T, sv[5], sv[3], sv[4],
        gwu, sbu.reshape(2 * HC), gwd.T, sv[2], sv[0], sv[1],
    )


def solution(mesh):
    tok = P(("dp", "tensor"), None)
    in_specs = (
        tok, P("dp", None), tok, P("dp", None, "tensor"), P(None, "tensor"), P("tensor", "dp"),
        P(), P(), P(), P("dp", "tensor"), P("tensor"), P("tensor", "dp"), P(), P(), P(),
    )
    out_specs = (
        tok, tok, P("dp", None, "tensor"), P(None, "tensor"), P("tensor", "dp"),
        P(), P(), P(), P("dp", "tensor"), P("tensor"), P("tensor", "dp"), P(), P(), P(),
    )
    return jax.shard_map(shards, mesh=mesh, in_specs=in_specs, out_specs=out_specs, check_vma=False)
```

```python
import functools
import math
from types import SimpleNamespace

import jax
import jax.numpy as jnp
from jax import lax
from jax.experimental import pallas as pl
from jax.experimental.pallas import tpu as pltpu
from jax.sharding import PartitionSpec as P

HD = 64
MESH = pl.DeviceIdType.MESH
BF = jnp.bfloat16
F32 = jnp.float32
NEG = -1e30
VMEM_LIMIT = 67043328
MID, GF, FSND, FRCV = 0, 2, 4, 5


def nn(a, b):
    return jnp.dot(a, b, preferred_element_type=F32)


def nt(a, b):
    return lax.dot_general(a, b, (((1,), (1,)), ((), ())), preferred_element_type=F32)


def merge(x):
    return x.reshape(-1, x.shape[-1])


def spin(lo, hi, body):
    def step(i, carry):
        body(i)
        return carry

    lax.fori_loop(lo, hi, step, 0)


def order_table(T):
    return [sorted(range(T), key=lambda b: (abs(b - a), b if a < T / 2 else -b)) for a in range(T)]


def layer_kernel(cf, names, *refs):
    r = SimpleNamespace(**dict(zip(names, refs)))
    T, NQ, TB, D, R, C, HC, DP = cf.T, cf.NQ, cf.TB, cf.D, cf.R, cf.C, cf.HC, cf.DP
    S = NQ // 2
    RW = T * TB
    RC = 32
    heads = C // HD
    table = order_table(T)

    d = lax.axis_index("dp")
    t = lax.axis_index("tensor")
    q = lax.div(d, 2)
    c = d - 2 * q
    oc = 1 - c
    partner = (2 * q + oc, t)

    def perm(x):
        if NQ % 4:
            return x
        m = lax.rem(x, 4)
        return x + lax.div(m, 2) * (1 - 2 * lax.rem(m, 2))

    pos = perm(q)

    def chip_at(x):
        return perm(lax.rem(x + 4 * NQ, NQ))

    nxt = (2 * chip_at(pos + 1) + c, t)
    prv = (2 * chip_at(pos - 1) + c, t)

    def ind(a, b, n):
        x = lax.rem(a - b + n, n)
        return 1 - lax.div(x + n - 1, n)

    def tp(j):
        if isinstance(j, int):
            return sum(table[a][j] * ind(t, a, T) for a in range(T))
        js = [ind(j, b, T) for b in range(T)]
        total = 0
        for a in range(T):
            total = total + ind(t, a, T) * sum(table[a][b] * js[b] for b in range(T))
        return total

    def copy(src, dst, ss, rs, dev):
        return pltpu.make_async_remote_copy(
            src_ref=src, dst_ref=dst, send_sem=ss, recv_sem=rs, device_id=dev, device_id_type=MESH
        )

    def go(cp, op):
        if op == "start":
            cp.start()
        else:
            cp.wait_send()

    def half(kd, ref, h):
        if kd.split:
            return ref.at[h]
        n = kd.rows // 2
        return ref.at[pl.ds(h * n, n)]

    kt = SimpleNamespace(piece=lambda tt, qq: r.X.at[tt], zs=r.t_zs, zr=r.t_zr)
    kq = SimpleNamespace(
        piece=lambda tt, qq: r.Wq.at[2 * qq + c], split=False, rows=R, rs=r.q_rs, rr=r.q_rr,
        gs=r.q_gs, gr=r.q_gr, HB=r.q_HB, FB=r.q_FB,
    )
    ko = SimpleNamespace(
        piece=lambda tt, qq: r.Wo.at[tt, 2 * qq + c], split=False, rows=R, zs=r.o_zs, zr=r.o_zr,
        rs=r.o_rs, rr=r.o_rr, gs=r.o_gs, gr=r.o_gr, HB=r.o_HB, FB=r.o_FB,
        cs=r.o_cs, cr=r.o_cr, ZB=r.o_ZB,
    )
    ku = SimpleNamespace(
        piece=lambda tt, qq: r.Wu.at[tt, qq], split=True, rows=2 * R, zs=r.u_zs, zr=r.u_zr,
        rs=r.u_rs, rr=r.u_rr, gs=r.u_gs, gr=r.u_gr, HB=r.u_HB, FB=r.u_FB,
        cs=r.u_cs, cr=r.u_cr, ZB=r.u_ZB,
    )
    kd_ = SimpleNamespace(
        piece=lambda tt, qq: r.Wd.at[tt, qq], split=True, rows=2 * R, zs=r.d_zs, zr=r.d_zr,
        rs=r.d_rs, rr=r.d_rr, gs=r.d_gs, gr=r.d_gr, HB=r.d_HB, FB=r.d_FB,
        cs=r.d_cs, cr=r.d_cr, ZB=r.d_ZB,
    )
    kg = SimpleNamespace(piece=lambda tt, qq: r.POOL.at[tt], cs=r.g_cs, cr=r.g_cr, ZB=r.g_ZB)

    def z_right(k, tt, op):
        @pl.when((tt <= t) & (t < T - 1))
        def _():
            ref = k.piece(tt, q)
            go(copy(ref, ref, k.zs.at[tt, 0], k.zr.at[tt], (d, t + 1)), op)

    def z_left(k, tt, op):
        @pl.when((tt >= t) & (t > 0))
        def _():
            ref = k.piece(tt, q)
            go(copy(ref, ref, k.zs.at[tt, 1], k.zr.at[tt], (d, t - 1)), op)

    def z_send(k, tt, op="start"):
        z_right(k, tt, op)
        z_left(k, tt, op)

    def z_wait(k, tt):
        ref = k.piece(tt, q)
        copy(ref, ref, k.zs.at[tt, 0], k.zr.at[tt], partner).wait_recv()

    def ring_send(k, tt, s, op="start"):
        a = k.piece(tt, chip_at(pos - s))
        b = k.piece(tt, chip_at(pos + s))
        if s == S - 1:
            a, b = half(k, a, 0), half(k, b, 1)
        go(copy(a, a, k.rs.at[tt, 0, s], k.rr.at[tt, 0, s], nxt), op)
        go(copy(b, b, k.rs.at[tt, 1, s], k.rr.at[tt, 1, s], prv), op)

    def ring_wait(k, tt, s):
        a = k.piece(tt, chip_at(pos - 1 - s))
        b = k.piece(tt, chip_at(pos + 1 + s))
        if s == S - 1:
            a, b = half(k, a, 0), half(k, b, 1)
        copy(a, a, k.rs.at[tt, 0, s], k.rr.at[tt, 0, s], nxt).wait_recv()
        copy(b, b, k.rs.at[tt, 1, s], k.rr.at[tt, 1, s], prv).wait_recv()

    def twin_o(tt, qq):
        ref = r.Wo.at[tt, 2 * qq + c]
        copy(ref, ref, r.tw_s.at[0], r.tw_r.at[0], partner).start()

    def twin_q(tt, qq):
        ref = r.Wq.at[2 * qq + c]
        copy(ref, ref, r.tw_s.at[1], r.tw_r.at[1], partner).start()

    def arrived(k, tt, s, twin):
        ring_wait(k, tt, s)
        if twin is not None:
            twin(tt, chip_at(pos + 1 + s))
            if s < S - 1:
                twin(tt, chip_at(pos - 1 - s))

    def ring_adv(k, tt, twin=None):
        for s in range(1, S):
            arrived(k, tt, s - 1, twin)
            ring_send(k, tt, s)

    def ring_fin(k, tt, twin=None):
        arrived(k, tt, S - 1, twin)

    def add(dst, src):
        dst[...] = (dst[...].astype(F32) + src[...].astype(F32)).astype(BF)

    def rs_send(k, tt, s, op="start"):
        a = k.piece(tt, chip_at(pos + S - s))
        b = k.piece(tt, chip_at(pos - S + s))
        if s == 0:
            a, b = half(k, a, 0), half(k, b, 1)
            da, db = k.HB.at[tt, 0], k.HB.at[tt, 1]
        else:
            da, db = k.FB.at[tt, 0, s - 1], k.FB.at[tt, 1, s - 1]
        go(copy(a, da, k.gs.at[tt, 0, s], k.gr.at[tt, 0, s], nxt), op)
        go(copy(b, db, k.gs.at[tt, 1, s], k.gr.at[tt, 1, s], prv), op)

    def rs_add(k, tt, s):
        a = k.piece(tt, chip_at(pos + S - s - 1))
        b = k.piece(tt, chip_at(pos - S + s + 1))
        if s == 0:
            a, b = half(k, a, 0), half(k, b, 1)
            da, db = k.HB.at[tt, 0], k.HB.at[tt, 1]
        else:
            da, db = k.FB.at[tt, 0, s - 1], k.FB.at[tt, 1, s - 1]
        copy(da, da, k.gs.at[tt, 0, s], k.gr.at[tt, 0, s], nxt).wait_recv()
        add(a, da)
        copy(db, db, k.gs.at[tt, 1, s], k.gr.at[tt, 1, s], prv).wait_recv()
        add(b, db)

    def rs_mid(k, tt):
        for s in range(1, S):
            rs_add(k, tt, s - 1)
            rs_send(k, tt, s)

    def rs_last(k, tt):
        rs_add(k, tt, S - 1)

    def chain_send(k, tt, op="start"):
        ref = k.piece(tt, q)

        @pl.when(tt > t)
        def _():
            go(copy(ref, k.ZB.at[tt], k.cs.at[tt], k.cr.at[tt], (d, t + 1)), op)

        @pl.when(tt < t)
        def _():
            slot = tt + (T - tt) * ind(tt, t - 1, T)
            go(copy(ref, k.ZB.at[slot], k.cs.at[tt], k.cr.at[slot], (d, t - 1)), op)

    def chain_take(k, tt, slot):
        copy(k.ZB.at[slot], k.ZB.at[slot], k.cs.at[tt], k.cr.at[slot], partner).wait_recv()
        add(k.piece(tt, q), k.ZB.at[slot])

    def chain_first(k, tt):
        @pl.when(((tt > t) & (t == 0)) | ((tt < t) & (t == T - 1)))
        def _():
            chain_send(k, tt)

    def chain_on(k, tt):
        @pl.when(((tt > t) & (t > 0)) | ((tt < t) & (t < T - 1)))
        def _():
            chain_take(k, tt, tt)
            chain_send(k, tt)

    def chain_end(k):
        @pl.when(t > 0)
        def _():
            chain_take(k, t, t)

        @pl.when(t < T - 1)
        def _():
            chain_take(k, t, T)

    barrier = pltpu.get_barrier_semaphore()
    peers = [partner]
    peers += [(2 * lax.rem(q + k, NQ) + c, t) for k in range(1, NQ)]
    peers += [(d, lax.rem(t + k, T)) for k in range(1, T)]
    for peer in peers:
        pl.semaphore_signal(barrier, inc=1, device_id=peer, device_id_type=MESH)
    gets = [
        pltpu.make_async_copy(r.tok, r.X.at[t], r.in_s.at[0]),
        pltpu.make_async_copy(r.og, r.out, r.in_s.at[1]),
    ]
    for n in range(3):
        gets.append(
            pltpu.make_async_copy(r.wq.at[n], r.Wq.at[d, :, pl.ds(n * C, C)], r.in_s.at[2 + n])
        )
    for get in gets:
        get.start()
    lo = pl.multiple_of(c * HC, 128)
    ro = pl.multiple_of(oc * HC, 128)

    def flipped(x):
        return x.astype(F32).T.astype(BF)

    r.Wo[t, d] = flipped(r.wo[...])
    r.FSW[0] = r.wu[:, pl.ds(ro, HC)]
    r.FSW[1] = flipped(r.wd[pl.ds(ro, HC), :])
    r.Wu[t, q, c] = r.wu[:, pl.ds(lo, HC)]
    r.Wd[t, q, c] = flipped(r.wd[pl.ds(lo, HC), :])
    r.BU[t] = r.bup[...].astype(F32).reshape(1, 2 * HC)
    for n, name in enumerate(("b_out", "g1", "n1", "b_down", "g2", "n2")):
        r.vecs[n : n + 1, :] = getattr(r, name)[...].astype(F32).reshape(1, D)
    r.segc[...] = jnp.broadcast_to(r.seg[...].astype(F32), (128, RW)).T
    for get in gets:
        get.wait()
    pl.semaphore_wait(barrier, len(peers))

    swap_u = copy(r.FSW.at[0], r.Wu.at[t, q, c], r.sw_s.at[0], r.sw_r.at[0], partner)
    swap_d = copy(r.FSW.at[1], r.Wd.at[t, q, c], r.sw_s.at[1], r.sw_r.at[1], partner)
    swap_u.start()
    z_send(ko, t)
    twin_q(0, q)
    ring_send(kq, 0, 0)
    swap_d.start()
    twin_o(t, q)
    ring_send(ko, t, 0)

    def swapped(n, ref):
        ref = ref.at[t, q, oc]
        copy(ref, ref, r.sw_s.at[n], r.sw_r.at[n], partner).wait_recv()

    swapped(0, r.Wu)
    z_send(ku, t)
    z_send(kt, t)
    ring_send(ku, t, 0)
    swapped(1, r.Wd)

    def weights_z(tt):
        @pl.when(tt == 0)
        def _():
            z_right(kd_, t, "start")

        @pl.when(tt == T - 1)
        def _():
            z_left(kd_, t, "start")

    weights_z(t)
    for k in range(1, T):
        tt = lax.rem(t + k, T)
        copy(r.BU.at[t], r.BU.at[t], r.b_s.at[tt], r.b_r.at[t], (d, tt)).start()
    r.SACC[...] = jnp.zeros_like(r.SACC)
    r.SB[...] = jnp.zeros_like(r.SB)
    r.DK[...] = jnp.zeros_like(r.DK)
    r.DV[...] = jnp.zeros_like(r.DV)

    def project(tt):
        x = r.X[tt]
        at = pl.ds(pl.multiple_of(tt * TB, TB), TB)
        for part, name in enumerate(("Q", "K", "V")):
            w = merge(r.Wq[:, :, part * C : (part + 1) * C])
            y = nn(x, w)
            if part != 1:
                y = y + r.bqv[part // 2 : part // 2 + 1, :].astype(F32)
            y = y.astype(BF)
            if part == 0:
                r.Q[at, :] = y * jnp.asarray(HD ** (-0.5), BF)
            elif part == 1:
                r.K[at, :] = y
                r.KT[:, at] = y.astype(F32).T.astype(BF)
            else:
                r.V[at, :] = y
                r.VT[:, at] = y.astype(F32).T.astype(BF)

    arrived(kq, 0, 0, twin_q)
    ring_send(kq, 0, 1)
    ring_send(kd_, t, 0)
    for j in range(1, T):
        tt = tp(j)
        for k in (ko, ku):
            z_wait(k, tt)
            z_send(k, tt)
            ring_send(k, tt, 0)
        twin_o(tt, q)
        ring_adv(ko, tp(j - 1), twin_o)
        ring_adv(ku, tp(j - 1))
        if j == 1:
            for s in range(1, S):
                arrived(kq, 0, s, twin_q)
                if s + 1 < S:
                    ring_send(kq, 0, s + 1)
            copy(r.RQ, r.RQ, r.tw_s.at[1], r.tw_r.at[1], partner).wait_recv()
            project(t)
        else:
            ring_fin(ko, tp(j - 2), twin_o)
        z_wait(kt, tt)
        z_send(kt, tt)
        weights_z(tt)
        if j == 1:
            ring_adv(kd_, t)
        project(tt)
    ring_adv(ko, tp(T - 1), twin_o)
    ring_adv(ku, tp(T - 1))
    ring_fin(ko, tp(T - 2), twin_o)
    ring_fin(ko, tp(T - 1), twin_o)

    def take_down(j):
        tt = tp(j)
        z_wait(kd_, tt)
        z_send(kd_, tt)
        ring_send(kd_, tt, 0)

    lane = lax.broadcasted_iota(jnp.int32, (1, 128), 1)
    picks = [(lane < HD).astype(F32).astype(BF), (lane >= HD).astype(F32).astype(BF)]

    def bias_for(i):
        same = r.segc[:, 0:1] == r.seg[:, pl.ds(pl.multiple_of(i * TB, TB), TB)].astype(F32)
        r.BIAS[...] = jnp.where(same, 0.0, NEG)

    def attend(j):
        i = lax.rem(t + 1 + j, T)
        at = pl.ds(pl.multiple_of(i * TB, TB), TB)
        bias_for(i)
        for h in range(heads):
            pair = slice((h // 2) * 128, (h // 2) * 128 + 128)
            qh = r.Q[at, pair] * picks[h % 2]
            sc = nt(r.K[:, pair], qh) + r.BIAS[...]
            top = jnp.max(sc, axis=0, keepdims=True)
            e = jnp.exp(sc - top)
            total = jnp.sum(e, axis=0, keepdims=True)
            ct = nn(r.VT[h * HD : (h + 1) * HD, :], e.astype(BF))
            r.CT[h * HD : (h + 1) * HD, :] = ct / total
            r.LSE[i, h : h + 1, :] = top + jnp.log(total)
        r.CXR[i] = r.CT[...].T.astype(BF)

        @pl.when(i != t)
        def _():
            copy(r.CXR.at[i], r.CTX.at[t], r.c_s.at[i], r.c_r.at[t], (d, i)).start()

    spin(0, T // 2, attend)
    take_down(1)
    spin(T // 2, T, attend)
    for j in range(2, T):
        take_down(j)
        if j == 2:
            ring_adv(kd_, tp(1))
    r.CTX[t] = r.CXR[t]
    for k in range(1, T):
        tt = lax.rem(t + k, T)
        copy(r.CTX.at[tt], r.CTX.at[tt], r.c_s.at[tt], r.c_r.at[tt], partner).wait_recv()
    copy(r.RWO, r.RWO, r.tw_s.at[0], r.tw_r.at[0], partner).wait_recv()

    def out_dot(j):
        y = nt(r.CTX[j], merge(r.Wo[j]))

        @pl.when(j == 0)
        def _():
            r.FEED[0] = y

        @pl.when(j > 0)
        def _():
            r.FEED[0] += y

    spin(0, T, out_dot)

    def rows_of(body):
        def step(i):
            body(pl.ds(pl.multiple_of(i * RC, RC), RC))

        spin(0, TB // RC, step)

    def tally(n, x):
        r.SACC[n] += x.reshape(RC // 8, 8, D).sum(axis=0)

    def norm(x):
        mid = x - jnp.mean(x, axis=-1, keepdims=True)
        inverse = lax.rsqrt(jnp.mean(mid * mid, axis=-1, keepdims=True) + 1e-05)
        return mid * inverse, inverse

    def norm_back(up, gain, normed, inverse):
        e = up * gain
        return inverse * (
            e - jnp.mean(e, axis=-1, keepdims=True) - normed * jnp.mean(e * normed, axis=-1, keepdims=True)
        )

    def vec(n):
        return r.vecs[n : n + 1, :]

    def first_norm(at):
        x = r.X[t, at, :].astype(F32) + r.FEED[0, at, :] + vec(0)
        normed, inverse = norm(x)
        h1 = normed * vec(1) + vec(2)
        r.N1[at, :] = normed
        r.IV1[at, :] = inverse
        r.H1[at, :] = h1
        r.POOL[MID + c, at, :] = h1.astype(BF)

    rows_of(first_norm)

    def exchange(n, base, op="start"):
        ref = r.POOL.at[base + c]
        go(copy(ref, ref, r.e_s.at[n], r.e_r.at[n], partner), op)

    def exchanged(n, base):
        ref = r.POOL.at[base + oc]
        copy(ref, ref, r.e_s.at[n], r.e_r.at[n], partner).wait_recv()

    exchange(0, MID)
    for k in range(1, T):
        tt = lax.rem(t + k, T)
        copy(r.BU.at[tt], r.BU.at[tt], r.b_s.at[tt], r.b_r.at[tt], partner).wait_recv()
    exchanged(0, MID)

    def turn(src, dst):
        def step(b):
            y = r.POOL[src + b].astype(F32).T.astype(BF)
            dst[:, pl.ds(pl.multiple_of(b * TB, TB), TB)] = y

        spin(0, 2, step)

    def up(j):
        tt = tp(j)
        ring_fin(ku, tt)
        w = merge(r.Wu[tt])
        bias = r.BU[tt, :, pl.ds(lo, HC)]

        def block(b):
            r.PRE[...] = nn(r.POOL[MID + b], w) + bias

            def piece(i):
                at = pl.ds(pl.multiple_of(i * RC, RC), RC)
                v = r.PRE[at, :]
                cdf = 0.5 * (1.0 + lax.erf(v * 2.0 ** (-0.5)))
                slope = cdf + v * jnp.exp(-0.5 * v * v) * (2.0 * math.pi) ** (-0.5)
                to = pl.ds(pl.multiple_of(b * TB + i * RC, RC), RC)
                r.ACT[tt, to, :] = (v * cdf).astype(BF)
                r.SL[tt, to, :] = slope.astype(BF)

            spin(0, TB // RC, piece)

        spin(0, 2, block)

    for j in range(T):
        ahead = 2 if j == 0 else j + 1 if j >= 2 else T
        if ahead < T:
            ring_adv(kd_, tp(ahead))
        up(j)
    turn(MID, r.MIDT)

    def down(j):
        tt = tp(j)
        ring_fin(kd_, tt)
        w = merge(r.Wd[tt])

        def block(b):
            y = nt(r.ACT[tt, pl.ds(pl.multiple_of(b * TB, TB), TB), :], w)
            if j == 0:
                r.FEED[b] = y
            else:
                r.FEED[b] += y

        spin(0, 2, block)

    for j in range(T):
        down(j)

    def give(n):
        def step(at):
            r.POOL[FSND, at, :] = r.FEED[oc, at, :].astype(BF)

        rows_of(step)
        copy(r.POOL.at[FSND], r.POOL.at[FRCV], r.e_s.at[n], r.e_r.at[n], partner).start()
        copy(r.POOL.at[FRCV], r.POOL.at[FRCV], r.e_s.at[n], r.e_r.at[n], partner).wait_recv()
        copy(r.POOL.at[FSND], r.POOL.at[FRCV], r.e_s.at[n], r.e_r.at[n], partner).wait_send()

    def given(n, at):
        return r.FEED[c, at, :] + r.POOL[FRCV, at, :].astype(F32)

    give(1)

    def second_norm(at):
        x = r.H1[at, :] + given(1, at) + vec(3)
        normed, inverse = norm(x)
        g = r.out[at, :].astype(F32)
        r.out[at, :] = (normed * vec(4) + vec(5)).astype(BF)
        tally(0, g * normed)
        tally(1, g)
        back = norm_back(g, vec(4), normed, inverse)
        r.H1[at, :] = back
        low = back.astype(BF)
        r.POOL[GF + c, at, :] = low
        tally(2, low.astype(F32))

    rows_of(second_norm)
    exchange(2, GF)

    def drain_gather(k):
        def step(tt):
            if hasattr(k, "zs"):
                z_send(k, tt, "drain")
            for s in range(S):
                ring_send(k, tt, s, "drain")

        spin(0, T, step)

    drain_gather(ku)
    drain_gather(kd_)
    swap_u.wait_send()
    swap_d.wait_send()
    exchanged(2, GF)
    turn(GF, r.GFT)

    def slot_back(k):
        tt = tp(T - 1 - k)

        def block(b):
            to = pl.ds(pl.multiple_of(b * TB, TB), TB)
            r.PRE[...] = nn(r.POOL[GF + b], merge(r.Wd[tt]))

            def piece(i):
                at = pl.ds(pl.multiple_of(i * RC, RC), RC)
                tr = pl.ds(pl.multiple_of(b * TB + i * RC, RC), RC)
                gp = (r.PRE[at, :] * r.SL[tt, tr, :].astype(F32)).astype(BF)
                r.SL[tt, tr, :] = gp
                r.SBA[...] += gp.astype(F32).reshape(RC // 8, 8, HC).sum(axis=0)

            spin(0, TB // RC, piece)
            y = nt(r.SL[tt, to, :], merge(r.Wu[tt]))

            @pl.when(k == 0)
            def _():
                r.FEED[b] = y

            @pl.when(k > 0)
            def _():
                r.FEED[b] += y

        r.SBA[...] = jnp.zeros_like(r.SBA)
        spin(0, 2, block)
        r.SB[pl.ds(2 * tt + c, 1)] = r.SBA[...].sum(axis=0, keepdims=True)[None]

    def slot_weights(k):
        tt = tp(T - 1 - k)

        def weight(qq):
            at = pl.ds(pl.multiple_of(qq * 2 * R, 2 * R), 2 * R)
            y = nn(r.GFT[at, :], r.ACT[tt])
            r.Wd[tt, qq] = y.astype(BF).reshape(2, R, HC)
            y = nn(r.MIDT[at, :], r.SL[tt])
            r.Wu[tt, qq] = y.astype(BF).reshape(2, R, HC)

        spin(0, NQ, weight)
        rs_send(kd_, tt, 0)
        rs_send(ku, tt, 0)

    def slot_both(k):
        slot_back(k)
        slot_weights(k)

    H = T // 2

    def far(k):
        return tp(T - 1 - k)

    def pair_mid(k):
        rs_mid(kd_, far(k))
        rs_mid(ku, far(k))

    def pair_last(k):
        for w in (kd_, ku):
            rs_last(w, far(k))
            chain_first(w, far(k))

    def pair_on(k):
        chain_on(kd_, far(k))
        chain_on(ku, far(k))

    spin(0, H, slot_both)
    spin(H, T, slot_back)
    pair_mid(0)
    give(3)

    def first_back(at):
        g = r.H1[at, :] + given(3, at)
        normed = r.N1[at, :]
        tally(3, g * normed)
        tally(4, g)
        back = norm_back(g, vec(1), normed, r.IV1[at, :])
        r.H1[at, :] = back
        low = back.astype(BF)
        r.gtok[at, :] = low
        tally(5, low.astype(F32))

    rows_of(first_back)

    def context_back(k):
        tt = tp(T - 1 - k)
        r.CXR[tt] = nn(r.gtok[...], merge(r.Wo[tt])).astype(BF)

        @pl.when(tt != t)
        def _():
            copy(r.CXR.at[tt], r.GC.at[t], r.gc_s.at[tt], r.gc_r.at[t], (d, tt)).start()

        @pl.when(tt == t)
        def _():
            r.GC[t] = r.CXR[t]

    for k in range(1, T):
        tt = lax.rem(t + k, T)
        copy(r.CXR.at[tt], r.CTX.at[t], r.c_s.at[tt], r.c_r.at[t], (d, tt)).wait_send()
    spin(0, T, context_back)
    for k in range(1, H):
        pair_mid(k)
    spin(H, T, slot_weights)
    for n in range(6):
        r.SV[n : n + 1, :] = r.SACC[n].sum(axis=0, keepdims=True)
    r.SV[6:8, :] = jnp.zeros((2, D), F32)

    def sum_core(n, ref, box, op):
        cp = copy(ref, box, r.a_s.at[0, n], r.a_r.at[0, n], partner)
        if op == "start":
            cp.start()
        else:
            copy(box, box, r.a_s.at[0, n], r.a_r.at[0, n], partner).wait_recv()
            cp.wait_send()
            ref[...] += box[...]

    def sum_group(stage, n, ref, box, me, count, dev, op):
        if op == "start":
            box[me] = ref[...]
        for k in range(1, count):
            other = lax.rem(me + k, count)
            sems = r.ag_s.at[stage, n, other], r.ag_r.at[stage, n, me]
            if op == "start":
                copy(box.at[me], box.at[me], *sems, dev(other)).start()
            else:
                copy(box.at[me], box.at[me], *sems, dev(other)).wait_send()
                copy(
                    box.at[other], box.at[other], r.ag_s.at[stage, n, other],
                    r.ag_r.at[stage, n, other], dev(other),
                ).wait_recv()
        if op != "start":
            total = box[0]
            for k in range(1, count):
                total = total + box[k]
            ref[...] = total

    def chip_dev(other):
        return (2 * other + c, t)

    def row_dev(other):
        return (d, other)

    sum_core(0, r.SV, r.SV1, "start")
    sum_core(1, r.SB, r.SB1, "start")

    sum_core(0, r.SV, r.SV1, "end")
    sum_core(1, r.SB, r.SB1, "end")
    sum_group(0, 0, r.SV, r.SV2, q, NQ, chip_dev, "start")
    sum_group(0, 1, r.SB, r.SB2, q, NQ, chip_dev, "start")

    def attend_back(j):
        i = tp(j)
        at = pl.ds(pl.multiple_of(i * TB, TB), TB)

        @pl.when(i != t)
        def _():
            copy(r.GC.at[i], r.GC.at[i], r.gc_s.at[i], r.gc_r.at[i], partner).wait_recv()

        bias_for(i)
        for h in range(heads):
            pair = slice((h // 2) * 128, (h // 2) * 128 + 128)
            qh = r.Q[at, pair] * picks[h % 2]
            gh = r.GC[i, :, pair] * picks[h % 2]
            pr = jnp.exp(nt(r.K[:, pair], qh) + r.BIAS[...] - r.LSE[i, h : h + 1, :])
            gp = nt(r.V[:, pair], gh)
            r.DV[:, pair] += nn(pr.astype(BF), gh)
            prod = pr * gp
            delta = jnp.sum(prod, axis=0, keepdims=True)
            ds = (prod - pr * delta).astype(BF)
            r.DK[:, pair] += nn(ds, qh)
            r.CT[h * HD : (h + 1) * HD, :] = nn(r.KT[h * HD : (h + 1) * HD, :], ds) * HD ** (-0.5)
        r.DPJ[i, :, 0:C] = r.CT[...].T.astype(BF)

    spin(0, H, attend_back)
    pair_last(0)
    spin(H, T, attend_back)
    sum_group(0, 0, r.SV, r.SV2, q, NQ, chip_dev, "end")
    sum_group(0, 1, r.SB, r.SB2, q, NQ, chip_dev, "end")
    sum_group(1, 0, r.SV, r.SV3, t, T, row_dev, "start")
    sum_group(1, 1, r.SB, r.SB3, t, T, row_dev, "start")
    exchange(0, MID, "drain")
    exchange(2, GF, "drain")

    r.SQ[...] = jnp.zeros_like(r.SQ)

    def input_back(k):
        tt = far(k)
        at = pl.ds(pl.multiple_of(tt * TB, TB), TB)
        r.DPJ[tt, :, C : 2 * C] = r.DK[at, :].astype(BF)
        r.DPJ[tt, :, 2 * C : 3 * C] = r.DV[at, :].astype(BF)
        r.SQ[0:1, :] += r.DPJ[tt, :, 0:C].astype(F32).sum(axis=0, keepdims=True)
        r.SQ[1:2, :] += r.DPJ[tt, :, 2 * C : 3 * C].astype(F32).sum(axis=0, keepdims=True)
        r.POOL[tt] = nt(r.DPJ[tt], merge(r.Wq[...])).astype(BF)

        @pl.when(k == 0)
        def _():
            chain_first(kg, tt)

    spin(0, T, input_back)
    sum_core(2, r.SQ, r.SQ1, "start")
    for k in range(1, H):
        pair_last(k)
    for k in range(1, T - 1):
        chain_first(kg, far(k))
    pair_on(0)
    for k in range(H, T - 1):
        pair_mid(k)
    drain_gather(ko)
    copy(r.RWO, r.RWO, r.tw_s.at[0], r.tw_r.at[0], partner).wait_send()

    r.GFT[:, 0:TB] = r.gtok[...].astype(F32).T.astype(BF)

    def out_back(tt):
        def weight(qq):
            at = pl.ds(pl.multiple_of(qq * 2 * R, 2 * R), 2 * R)
            y = nn(r.GFT[at, 0:TB], r.CTX[tt]).astype(BF)
            r.Wo[tt, pl.ds(2 * qq, 2)] = y.reshape(2, R, C)
            copy(r.Wo.at[tt, 2 * qq + oc], r.RWO.at[tt, qq], r.go_s.at[0], r.go_r.at[0], partner).start()

        spin(0, NQ, weight)

    spin(0, T, out_back)

    pair_mid(T - 1)
    chain_on(kg, far(0))
    copy(r.RWO, r.RWO, r.go_s.at[0], r.go_r.at[0], partner).wait_recv()

    def out_join(k):
        tt = tp(T - 1 - k)

        def step(qq):
            add(r.Wo.at[tt, 2 * qq + c], r.RWO.at[tt, qq])

        spin(0, NQ, step)
        rs_send(ko, tt, 0)

    spin(0, T, out_join)

    copy(r.RQ, r.RQ, r.tw_s.at[1], r.tw_r.at[1], partner).wait_send()
    for s in range(S):
        ring_send(kq, 0, s, "drain")
    many = max(2, 256 // R)

    def qkv_weight(g):
        cols = pl.ds(pl.multiple_of(g * many * R, 128), many * R)
        x = merge(r.X[:, :, cols])
        y = lax.dot_general(
            x, merge(r.DPJ[...]), (((0,), (0,)), ((), ())), preferred_element_type=F32
        )
        r.Wq[pl.ds(many * g, many)] = y.astype(BF).reshape(many, R, 3 * C)
        for k in range(many // 2):
            qq = g * (many // 2) + k
            copy(r.Wq.at[2 * qq + oc], r.RQ.at[qq], r.go_s.at[1], r.go_r.at[1], partner).start()

    spin(0, DP // many, qkv_weight)
    sum_core(2, r.SQ, r.SQ1, "end")
    sum_group(0, 2, r.SQ, r.SQ2, q, NQ, chip_dev, "start")
    copy(r.RQ, r.RQ, r.go_s.at[1], r.go_r.at[1], partner).wait_recv()

    def q_join(qq):
        add(r.Wq.at[2 * qq + c], r.RQ.at[qq])

    spin(0, NQ, q_join)
    rs_send(kq, 0, 0)
    order = [2, 1] if T == 4 else list(range(1, T - 1))
    for k in range(H, T - 1):
        pair_last(k)
    for n, k in enumerate(order):
        pair_on(k)
        if n > 0 or T != 4:
            chain_on(kg, far(k))
        else:
            chain_on(kg, far(k))
            for m in range(T):
                rs_mid(ko, far(m))
            rs_mid(kq, 0)
    if T != 4:
        for m in range(T):
            rs_mid(ko, far(m))
        rs_mid(kq, 0)
    for k in range(T - 1):
        rs_last(ko, far(k))
        chain_first(ko, far(k))
    for k in range(T - 1):
        chain_on(ko, far(k))
    rs_last(kd_, t)
    rs_last(ku, t)
    rs_last(ko, t)
    rs_last(kq, 0)
    sum_group(1, 0, r.SV, r.SV3, t, T, row_dev, "end")
    sum_group(1, 1, r.SB, r.SB3, t, T, row_dev, "end")
    sum_group(0, 2, r.SQ, r.SQ2, q, NQ, chip_dev, "end")
    chain_end(kg)

    def finish(at):
        r.gtok[at, :] = (r.H1[at, :] + r.POOL[t, at, :].astype(F32)).astype(BF)

    rows_of(finish)
    chain_end(kd_)
    chain_end(ku)
    chain_end(ko)
    cps = []
    for n, ref in enumerate((r.Wu, r.Wd)):
        cp = copy(ref.at[t, q, oc], r.FSW.at[n], r.fs_s.at[n], r.fs_r.at[n], partner)
        cp.start()
        cps.append(cp)
    for n in range(3):
        r.gwq[n] = r.Wq[d, :, n * C : (n + 1) * C]
    r.gwo[...] = r.Wo[t, d]
    r.sv[...] = r.SV[...]
    r.sbq[...] = r.SQ[...]
    r.sbu[...] = r.SB[pl.ds(2 * t, 2)]
    for n, (ref, o) in enumerate(((r.Wu, r.gwu), (r.Wd, r.gwd))):
        copy(r.FSW.at[n], r.FSW.at[n], r.fs_s.at[n], r.fs_r.at[n], partner).wait_recv()
        o[:, pl.ds(lo, HC)] = ref[t, q, c]
        o[:, pl.ds(ro, HC)] = r.FSW[n]
        cps[n].wait_send()

    def drain(tt):
        z_send(kt, tt, "drain")
        for k in (kd_, ku, ko):
            for s in range(S):
                rs_send(k, tt, s, "drain")
            chain_send(k, tt, "drain")
        chain_send(kg, tt, "drain")

        @pl.when(tt != t)
        def _():
            copy(r.CXR.at[tt], r.GC.at[t], r.gc_s.at[tt], r.gc_r.at[t], (d, tt)).wait_send()
            copy(r.BU.at[t], r.BU.at[t], r.b_s.at[tt], r.b_r.at[t], (d, tt)).wait_send()

    spin(0, T, drain)
    for s in range(S):
        rs_send(kq, 0, s, "drain")
    copy(r.RWO, r.RWO, r.go_s.at[0], r.go_r.at[0], partner).wait_send()
    copy(r.RQ, r.RQ, r.go_s.at[1], r.go_r.at[1], partner).wait_send()


def layer(cf, *args):
    T, NQ, TB, D, R, C, HC, DP = cf.T, cf.NQ, cf.TB, cf.D, cf.R, cf.C, cf.HC, cf.DP
    S = NQ // 2
    RW = T * TB
    Cq = 3 * C
    heads = C // HD
    hp = -(-heads // 8) * 8
    dma = pltpu.SemaphoreType.DMA
    V = pltpu.VMEM
    ins = ["tok", "og", "wq", "wo", "wu", "wd", "bqv", "bup", "b_out", "g1", "n1", "b_down", "g2", "n2", "seg"]
    outs = {
        "out": ((TB, D), BF), "gtok": ((TB, D), BF), "gwq": ((3, R, C), BF), "gwo": ((R, C), BF),
        "gwu": ((R, 2 * HC), BF), "gwd": ((R, 2 * HC), BF), "sv": ((8, D), F32),
        "sbq": ((8, C), F32), "sbu": ((2, 1, HC), F32),
    }
    scratch = {
        "X": V((T, TB, D), BF), "Wq": V((DP, R, Cq), BF), "Wo": V((T, DP, R, C), BF),
        "Wu": V((T, NQ, 2, R, HC), BF), "Wd": V((T, NQ, 2, R, HC), BF), "BU": V((T, 1, 2 * HC), F32), "vecs": V((8, D), F32), "segc": V((RW, 128), F32),
        "Q": V((RW, C), BF), "K": V((RW, C), BF), "V": V((RW, C), BF),
        "KT": V((C, RW), BF), "VT": V((C, RW), BF), "BIAS": V((RW, TB), F32),
        "CT": V((C, TB), F32), "LSE": V((T, hp, TB), F32), "CXR": V((T, TB, C), BF),
        "CTX": V((T, TB, C), BF), "FEED": V((2, TB, D), F32), "N1": V((TB, D), F32),
        "IV1": V((TB, 1), F32), "H1": V((TB, D), F32), "POOL": V((max(6, T), TB, D), BF),
        "MIDT": V((D, 2 * TB), BF), "PRE": V((TB, HC), F32), "ACT": V((T, 2 * TB, HC), BF),
        "SL": V((T, 2 * TB, HC), BF),
        "GFT": V((D, 2 * TB), BF),
        "GC": V((T, TB, C), BF),
        "DK": V((RW, C), F32), "DV": V((RW, C), F32), "DPJ": V((T, TB, Cq), BF),
        "g_ZB": V((T + 1, TB, D), BF), "RWO": V((T, NQ, R, C), BF), "RQ": V((NQ, R, Cq), BF),
        "FSW": V((2, R, HC), BF),
        "q_HB": V((1, 2, R // 2, Cq), BF), "q_FB": V((1, 2, S - 1, R, Cq), BF),
        "o_HB": V((T, 2, R // 2, C), BF), "o_FB": V((T, 2, S - 1, R, C), BF), "o_ZB": V((T + 1, R, C), BF),
        "u_HB": V((T, 2, R, HC), BF), "u_FB": V((T, 2, S - 1, 2, R, HC), BF), "u_ZB": V((T + 1, 2, R, HC), BF),
        "d_HB": V((T, 2, R, HC), BF), "d_FB": V((T, 2, S - 1, 2, R, HC), BF), "d_ZB": V((T + 1, 2, R, HC), BF),
        "SACC": V((6, 8, D), F32), "SBA": V((8, HC), F32),
        "SV": V((8, D), F32), "SV1": V((8, D), F32), "SV2": V((NQ, 8, D), F32), "SV3": V((T, 8, D), F32),
        "SB": V((2 * T, 1, HC), F32), "SB1": V((2 * T, 1, HC), F32), "SB2": V((NQ, 2 * T, 1, HC), F32),
        "SB3": V((T, 2 * T, 1, HC), F32),
        "SQ": V((8, C), F32), "SQ1": V((8, C), F32), "SQ2": V((NQ, 8, C), F32),
        "t_zs": dma((T, 2)), "t_zr": dma((T,)),
        "q_rs": dma((1, 2, S)), "q_rr": dma((1, 2, S)), "q_gs": dma((1, 2, S)), "q_gr": dma((1, 2, S)),
        "tw_s": dma((2,)), "tw_r": dma((2,)), "sw_s": dma((2,)), "sw_r": dma((2,)),
        "b_s": dma((T,)), "b_r": dma((T,)), "c_s": dma((T,)), "c_r": dma((T,)),
        "e_s": dma((4,)), "e_r": dma((4,)), "gc_s": dma((T,)), "gc_r": dma((T,)),
        "go_s": dma((2,)), "go_r": dma((2,)), "g_cs": dma((T,)), "g_cr": dma((T + 1,)),
        "a_s": dma((1, 3)), "a_r": dma((1, 3)),
        "ag_s": dma((2, 3, max(NQ, T))), "ag_r": dma((2, 3, max(NQ, T))),
        "fs_s": dma((2,)), "fs_r": dma((2,)), "in_s": dma((5,)),
    }
    for n in "oud":
        scratch[n + "_zs"] = dma((T, 2))
        scratch[n + "_zr"] = dma((T,))
        for m in ("_rs", "_rr", "_gs", "_gr"):
            scratch[n + m] = dma((T, 2, S))
        scratch[n + "_cs"] = dma((T,))
        scratch[n + "_cr"] = dma((T + 1,))
    names = ins + list(outs) + list(scratch)
    vm = pl.BlockSpec(memory_space=pltpu.VMEM)
    return pl.pallas_call(
        functools.partial(layer_kernel, cf, names),
        out_shape=tuple(jax.ShapeDtypeStruct(s, k) for s, k in outs.values()),
        in_specs=[pl.BlockSpec(memory_space=pl.ANY)] * 3 + [vm] * (len(ins) - 3),
        out_specs=(vm,) * len(outs),
        scratch_shapes=list(scratch.values()),
        compiler_params=pltpu.CompilerParams(
            collective_id=0, has_side_effects=True, vmem_limit_bytes=VMEM_LIMIT
        ),
        name="layer",
    )(*args)


def tail_kernel(cf, *refs):
    src, dst = refs[:9], refs[9:]
    out, gtok, gwq, gwo, gwu, gwd, sv, sbq, sbu = src
    dst[0][...] = out[...]
    dst[1][...] = gtok[...]
    dst[2][...] = gwq[...].astype(F32)
    dst[3][...] = sbq[0:2, :]
    dst[4][...] = gwo[...].astype(F32).T
    for n, row in ((5, 5), (6, 3), (7, 4), (11, 2), (12, 0), (13, 1)):
        dst[n][...] = sv[row : row + 1, :].reshape(cf.D)
    dst[8][...] = gwu[...].astype(F32)
    for n in range(2):
        dst[9][pl.ds(n * cf.HC, cf.HC)] = sbu[n].reshape(cf.HC)
    dst[10][...] = gwd[...].astype(F32).T


def tail(cf, *args):
    R, C, D, HC, TB = cf.R, cf.C, cf.D, cf.HC, cf.TB
    vm = pl.BlockSpec(memory_space=pltpu.VMEM)
    shapes = [
        ((TB, D), BF), ((TB, D), BF), ((3, R, C), F32), ((2, C), F32), ((C, R), F32),
        ((D,), F32), ((D,), F32), ((D,), F32), ((R, 2 * HC), F32), ((2 * HC,), F32),
        ((2 * HC, R), F32), ((D,), F32), ((D,), F32), ((D,), F32),
    ]
    return pl.pallas_call(
        functools.partial(tail_kernel, cf),
        out_shape=tuple(jax.ShapeDtypeStruct(*s) for s in shapes),
        in_specs=[vm] * len(args),
        out_specs=(vm,) * len(shapes),
        name="tail",
    )(*args)


def shards(
    tokens, segment_ids, out_grad, w_qkv, b_qv, w_out, b_out, norm1_gain, norm1_bias,
    w_up, b_up, w_down, b_down, norm2_gain, norm2_bias,
):
    DP, T = lax.axis_size("dp"), lax.axis_size("tensor")
    TB, D = tokens.shape
    R, _, C = w_qkv.shape
    HC = w_up.shape[1] // 2
    cf = SimpleNamespace(T=T, NQ=DP // 2, TB=TB, D=D, R=R, C=C, HC=HC, DP=DP)
    res = layer(
        cf, tokens, out_grad, w_qkv.transpose(1, 0, 2), w_out, w_up, w_down, b_qv, b_up,
        b_out, norm1_gain, norm1_bias, b_down, norm2_gain, norm2_bias, segment_ids,
    )
    res = list(tail(cf, *res))
    res[2] = res[2].transpose(1, 0, 2)
    return tuple(res)


def solution(mesh):
    tok = P(("dp", "tensor"), None)
    in_specs = (
        tok, P("dp", None), tok, P("dp", None, "tensor"), P(None, "tensor"), P("tensor", "dp"),
        P(), P(), P(), P("dp", "tensor"), P("tensor"), P("tensor", "dp"), P(), P(), P(),
    )
    out_specs = (
        tok, tok, P("dp", None, "tensor"), P(None, "tensor"), P("tensor", "dp"),
        P(), P(), P(), P("dp", "tensor"), P("tensor"), P("tensor", "dp"), P(), P(), P(),
    )
    return jax.shard_map(shards, mesh=mesh, in_specs=in_specs, out_specs=out_specs, check_vma=False)
```

```python
import functools
import math
from types import SimpleNamespace

import jax
import jax.numpy as jnp
from jax import lax
from jax.experimental import pallas as pl
from jax.experimental.pallas import tpu as pltpu
from jax.sharding import PartitionSpec as P

HD = 64
SEG_MOST = 512
MESH = pl.DeviceIdType.MESH
BF = jnp.bfloat16
F32 = jnp.float32
NEG = -1e30
VMEM_LIMIT = 67043328
MID, GF, FSND, FRCV = 0, 2, 4, 5


def nn(a, b):
    return jnp.dot(a, b, preferred_element_type=F32)


def nt(a, b):
    return lax.dot_general(a, b, (((1,), (1,)), ((), ())), preferred_element_type=F32)


def merge(x):
    return x.reshape(-1, x.shape[-1])


def spin(lo, hi, body):
    def step(i, carry):
        body(i)
        return carry

    lax.fori_loop(lo, hi, step, 0)


def order_table(T):
    return [sorted(range(T), key=lambda b: (abs(b - a), b if a < T / 2 else -b)) for a in range(T)]


def layer_kernel(cf, names, *refs):
    r = SimpleNamespace(**dict(zip(names, refs)))
    T, NQ, TB, D, R, C, HC, DP = cf.T, cf.NQ, cf.TB, cf.D, cf.R, cf.C, cf.HC, cf.DP
    S = NQ // 2
    RW = T * TB
    RC = 32
    heads = C // HD
    table = order_table(T)

    d = lax.axis_index("dp")
    t = lax.axis_index("tensor")
    q = lax.div(d, 2)
    c = d - 2 * q
    oc = 1 - c
    partner = (2 * q + oc, t)

    def perm(x):
        if NQ % 4:
            return x
        m = lax.rem(x, 4)
        return x + lax.div(m, 2) * (1 - 2 * lax.rem(m, 2))

    pos = perm(q)

    def chip_at(x):
        return perm(lax.rem(x + 4 * NQ, NQ))

    nxt = (2 * chip_at(pos + 1) + c, t)
    prv = (2 * chip_at(pos - 1) + c, t)

    def ind(a, b, n):
        x = lax.rem(a - b + n, n)
        return 1 - lax.div(x + n - 1, n)

    def tp(j):
        if isinstance(j, int):
            return sum(table[a][j] * ind(t, a, T) for a in range(T))
        js = [ind(j, b, T) for b in range(T)]
        total = 0
        for a in range(T):
            total = total + ind(t, a, T) * sum(table[a][b] * js[b] for b in range(T))
        return total

    def copy(src, dst, ss, rs, dev):
        return pltpu.make_async_remote_copy(
            src_ref=src, dst_ref=dst, send_sem=ss, recv_sem=rs, device_id=dev, device_id_type=MESH
        )

    def go(cp, op):
        if op == "start":
            cp.start()
        else:
            cp.wait_send()

    def half(kd, ref, h):
        if kd.split:
            return ref.at[h]
        n = kd.rows // 2
        return ref.at[pl.ds(h * n, n)]

    kt = SimpleNamespace(piece=lambda tt, qq: r.X.at[tt], zs=r.t_zs, zr=r.t_zr)
    kq = SimpleNamespace(
        piece=lambda tt, qq: r.Wq.at[2 * qq + c], split=False, rows=R, rs=r.q_rs, rr=r.q_rr,
        gs=r.q_gs, gr=r.q_gr, HB=r.q_HB, FB=r.q_FB,
    )
    ko = SimpleNamespace(
        piece=lambda tt, qq: r.Wo.at[tt, 2 * qq + c], split=False, rows=R, zs=r.o_zs, zr=r.o_zr,
        rs=r.o_rs, rr=r.o_rr, gs=r.o_gs, gr=r.o_gr, HB=r.o_HB, FB=r.o_FB,
        cs=r.o_cs, cr=r.o_cr, ZB=r.o_ZB,
    )
    ku = SimpleNamespace(
        piece=lambda tt, qq: r.Wu.at[tt, qq], split=True, rows=2 * R, zs=r.u_zs, zr=r.u_zr,
        rs=r.u_rs, rr=r.u_rr, gs=r.u_gs, gr=r.u_gr, HB=r.u_HB, FB=r.u_FB,
        cs=r.u_cs, cr=r.u_cr, ZB=r.u_ZB,
    )
    kd_ = SimpleNamespace(
        piece=lambda tt, qq: r.Wd.at[tt, qq], split=True, rows=2 * R, zs=r.d_zs, zr=r.d_zr,
        rs=r.d_rs, rr=r.d_rr, gs=r.d_gs, gr=r.d_gr, HB=r.d_HB, FB=r.d_FB,
        cs=r.d_cs, cr=r.d_cr, ZB=r.d_ZB,
    )
    kg = SimpleNamespace(piece=lambda tt, qq: r.POOL.at[tt], cs=r.g_cs, cr=r.g_cr, ZB=r.g_ZB)

    def z_right(k, tt, op):
        @pl.when((tt <= t) & (t < T - 1))
        def _():
            ref = k.piece(tt, q)
            go(copy(ref, ref, k.zs.at[tt, 0], k.zr.at[tt], (d, t + 1)), op)

    def z_left(k, tt, op):
        @pl.when((tt >= t) & (t > 0))
        def _():
            ref = k.piece(tt, q)
            go(copy(ref, ref, k.zs.at[tt, 1], k.zr.at[tt], (d, t - 1)), op)

    def z_send(k, tt, op="start"):
        z_right(k, tt, op)
        z_left(k, tt, op)

    def z_wait(k, tt):
        ref = k.piece(tt, q)
        copy(ref, ref, k.zs.at[tt, 0], k.zr.at[tt], partner).wait_recv()

    def ring_send(k, tt, s, op="start"):
        a = k.piece(tt, chip_at(pos - s))
        b = k.piece(tt, chip_at(pos + s))
        if s == S - 1:
            a, b = half(k, a, 0), half(k, b, 1)
        go(copy(a, a, k.rs.at[tt, 0, s], k.rr.at[tt, 0, s], nxt), op)
        go(copy(b, b, k.rs.at[tt, 1, s], k.rr.at[tt, 1, s], prv), op)

    def ring_wait(k, tt, s):
        a = k.piece(tt, chip_at(pos - 1 - s))
        b = k.piece(tt, chip_at(pos + 1 + s))
        if s == S - 1:
            a, b = half(k, a, 0), half(k, b, 1)
        copy(a, a, k.rs.at[tt, 0, s], k.rr.at[tt, 0, s], nxt).wait_recv()
        copy(b, b, k.rs.at[tt, 1, s], k.rr.at[tt, 1, s], prv).wait_recv()

    def twin_o(tt, qq):
        ref = r.Wo.at[tt, 2 * qq + c]
        copy(ref, ref, r.tw_s.at[0], r.tw_r.at[0], partner).start()

    def twin_q(tt, qq):
        ref = r.Wq.at[2 * qq + c]
        copy(ref, ref, r.tw_s.at[1], r.tw_r.at[1], partner).start()

    def arrived(k, tt, s, twin):
        ring_wait(k, tt, s)
        if twin is not None:
            twin(tt, chip_at(pos + 1 + s))
            if s < S - 1:
                twin(tt, chip_at(pos - 1 - s))

    def ring_adv(k, tt, twin=None):
        for s in range(1, S):
            arrived(k, tt, s - 1, twin)
            ring_send(k, tt, s)

    def ring_fin(k, tt, twin=None):
        arrived(k, tt, S - 1, twin)

    def add(dst, src):
        dst[...] = (dst[...].astype(F32) + src[...].astype(F32)).astype(BF)

    def rs_send(k, tt, s, op="start"):
        a = k.piece(tt, chip_at(pos + S - s))
        b = k.piece(tt, chip_at(pos - S + s))
        if s == 0:
            a, b = half(k, a, 0), half(k, b, 1)
            da, db = k.HB.at[tt, 0], k.HB.at[tt, 1]
        else:
            da, db = k.FB.at[tt, 0, s - 1], k.FB.at[tt, 1, s - 1]
        go(copy(a, da, k.gs.at[tt, 0, s], k.gr.at[tt, 0, s], nxt), op)
        go(copy(b, db, k.gs.at[tt, 1, s], k.gr.at[tt, 1, s], prv), op)

    def rs_add(k, tt, s):
        a = k.piece(tt, chip_at(pos + S - s - 1))
        b = k.piece(tt, chip_at(pos - S + s + 1))
        if s == 0:
            a, b = half(k, a, 0), half(k, b, 1)
            da, db = k.HB.at[tt, 0], k.HB.at[tt, 1]
        else:
            da, db = k.FB.at[tt, 0, s - 1], k.FB.at[tt, 1, s - 1]
        copy(da, da, k.gs.at[tt, 0, s], k.gr.at[tt, 0, s], nxt).wait_recv()
        add(a, da)
        copy(db, db, k.gs.at[tt, 1, s], k.gr.at[tt, 1, s], prv).wait_recv()
        add(b, db)

    def rs_mid(k, tt):
        for s in range(1, S):
            rs_add(k, tt, s - 1)
            rs_send(k, tt, s)

    def rs_last(k, tt):
        rs_add(k, tt, S - 1)

    def chain_send(k, tt, op="start"):
        ref = k.piece(tt, q)

        @pl.when(tt > t)
        def _():
            go(copy(ref, k.ZB.at[tt], k.cs.at[tt], k.cr.at[tt], (d, t + 1)), op)

        @pl.when(tt < t)
        def _():
            slot = tt + (T - tt) * ind(tt, t - 1, T)
            go(copy(ref, k.ZB.at[slot], k.cs.at[tt], k.cr.at[slot], (d, t - 1)), op)

    def chain_take(k, tt, slot):
        copy(k.ZB.at[slot], k.ZB.at[slot], k.cs.at[tt], k.cr.at[slot], partner).wait_recv()
        add(k.piece(tt, q), k.ZB.at[slot])

    def chain_first(k, tt):
        @pl.when(((tt > t) & (t == 0)) | ((tt < t) & (t == T - 1)))
        def _():
            chain_send(k, tt)

    def chain_on(k, tt):
        @pl.when(((tt > t) & (t > 0)) | ((tt < t) & (t < T - 1)))
        def _():
            chain_take(k, tt, tt)
            chain_send(k, tt)

    def chain_end(k):
        @pl.when(t > 0)
        def _():
            chain_take(k, t, t)

        @pl.when(t < T - 1)
        def _():
            chain_take(k, t, T)

    barrier = pltpu.get_barrier_semaphore()
    peers = [partner]
    peers += [(2 * lax.rem(q + k, NQ) + c, t) for k in range(1, NQ)]
    peers += [(d, lax.rem(t + k, T)) for k in range(1, T)]
    for peer in peers:
        pl.semaphore_signal(barrier, inc=1, device_id=peer, device_id_type=MESH)
    gets = [
        pltpu.make_async_copy(r.tok, r.X.at[t], r.in_s.at[0]),
        pltpu.make_async_copy(r.og, r.out, r.in_s.at[1]),
    ]
    for n in range(3):
        gets.append(
            pltpu.make_async_copy(r.wq.at[n], r.Wq.at[d, :, pl.ds(n * C, C)], r.in_s.at[2 + n])
        )
    for get in gets:
        get.start()
    lo = pl.multiple_of(c * HC, 128)
    ro = pl.multiple_of(oc * HC, 128)

    def flipped(x):
        return x.astype(F32).T.astype(BF)

    r.Wo[t, d] = flipped(r.wo[...])
    r.FSW[0] = r.wu[:, pl.ds(ro, HC)]
    r.FSW[1] = flipped(r.wd[pl.ds(ro, HC), :])
    r.Wu[t, q, c] = r.wu[:, pl.ds(lo, HC)]
    r.Wd[t, q, c] = flipped(r.wd[pl.ds(lo, HC), :])
    r.BU[t] = r.bup[...].astype(F32).reshape(1, 2 * HC)
    for n, name in enumerate(("b_out", "g1", "n1", "b_down", "g2", "n2")):
        r.vecs[n : n + 1, :] = getattr(r, name)[...].astype(F32).reshape(1, D)
    r.segc[...] = jnp.broadcast_to(r.seg[...].astype(F32), (128, RW)).T
    for get in gets:
        get.wait()
    pl.semaphore_wait(barrier, len(peers))

    swap_u = copy(r.FSW.at[0], r.Wu.at[t, q, c], r.sw_s.at[0], r.sw_r.at[0], partner)
    swap_d = copy(r.FSW.at[1], r.Wd.at[t, q, c], r.sw_s.at[1], r.sw_r.at[1], partner)
    swap_u.start()
    z_send(ko, t)
    twin_q(0, q)
    ring_send(kq, 0, 0)
    swap_d.start()
    twin_o(t, q)
    ring_send(ko, t, 0)

    def swapped(n, ref):
        ref = ref.at[t, q, oc]
        copy(ref, ref, r.sw_s.at[n], r.sw_r.at[n], partner).wait_recv()

    swapped(0, r.Wu)
    z_send(ku, t)
    z_send(kt, t)
    ring_send(ku, t, 0)
    swapped(1, r.Wd)

    def weights_z(tt):
        @pl.when(tt == 0)
        def _():
            z_right(kd_, t, "start")

        @pl.when(tt == T - 1)
        def _():
            z_left(kd_, t, "start")

    weights_z(t)
    for k in range(1, T):
        tt = lax.rem(t + k, T)
        copy(r.BU.at[t], r.BU.at[t], r.b_s.at[tt], r.b_r.at[t], (d, tt)).start()
    r.SACC[...] = jnp.zeros_like(r.SACC)
    r.SB[...] = jnp.zeros_like(r.SB)
    r.DK[...] = jnp.zeros_like(r.DK)
    r.DV[...] = jnp.zeros_like(r.DV)
    r.AM[...] = jnp.full_like(r.AM, NEG)
    r.AL[...] = jnp.zeros_like(r.AL)
    r.ACC[...] = jnp.zeros_like(r.ACC)

    def project(tt):
        x = r.X[tt]
        at = pl.ds(pl.multiple_of(tt * TB, TB), TB)
        for part, name in enumerate(("Q", "K", "V")):
            w = merge(r.Wq[:, :, part * C : (part + 1) * C])
            y = nn(x, w)
            if part != 1:
                y = y + r.bqv[part // 2 : part // 2 + 1, :].astype(F32)
            y = y.astype(BF)
            if part == 0:
                r.Q[at, :] = y * jnp.asarray(HD ** (-0.5), BF)
            elif part == 1:
                r.K[at, :] = y
                r.KT[:, at] = y.astype(F32).T.astype(BF)
            else:
                r.V[at, :] = y
                r.VT[:, at] = y.astype(F32).T.astype(BF)

    lane = lax.broadcasted_iota(jnp.int32, (1, 128), 1)
    picks = [(lane < HD).astype(F32).astype(BF), (lane >= HD).astype(F32).astype(BF)]
    reach = (SEG_MOST - 2) // TB + 1

    def rows_at(i):
        return pl.ds(pl.multiple_of(i * TB, TB), TB)

    def seg_row(i):
        return r.seg[:, rows_at(i)].astype(F32)

    def pair_up(i, b):
        bias = jnp.where(r.segc[rows_at(b), 0:1] == seg_row(i), 0.0, NEG)
        pairs = [slice((h // 2) * 128, (h // 2) * 128 + 128) for h in range(heads)]
        owns = [slice(h * HD, (h + 1) * HD) for h in range(heads)]
        before = [r.AM[i, h : h + 1, :] for h in range(heads)]
        sums = [r.AL[i, h : h + 1, :] for h in range(heads)]
        scs = [
            nt(r.K[rows_at(b), pairs[h]], r.Q[rows_at(i), pairs[h]] * picks[h % 2]) + bias
            for h in range(heads)
        ]
        tops = [jnp.maximum(before[h], jnp.max(scs[h], axis=0, keepdims=True)) for h in range(heads)]
        es = [jnp.exp(scs[h] - tops[h]) for h in range(heads)]
        shrinks = [jnp.exp(before[h] - tops[h]) for h in range(heads)]
        news = [nn(r.VT[owns[h], rows_at(b)], es[h].astype(BF)) for h in range(heads)]
        for h in range(heads):
            r.AM[i, h : h + 1, :] = tops[h]
            r.AL[i, h : h + 1, :] = sums[h] * shrinks[h] + jnp.sum(es[h], axis=0, keepdims=True)
            r.ACC[i, owns[h], :] = r.ACC[i, owns[h], :] * shrinks[h] + news[h]

    def attend(j):
        new = tp(j)

        def one(n):
            other = tp(lax.div(n, 2))
            side = lax.rem(n, 2)
            i = other + (new - other) * side
            b = new + (other - new) * side

            @pl.when((i - b <= reach) & (b - i <= reach))
            def _():
                pair_up(i, b)

        spin(0, 2 * j + 1, one)

    def finish_context(j):
        i = lax.rem(t + 1 + j, T)
        for h in range(heads):
            own = slice(h * HD, (h + 1) * HD)
            r.CT[own, :] = r.ACC[i, own, :] / r.AL[i, h : h + 1, :]
        r.AM[i, 0:heads, :] = r.AM[i, 0:heads, :] + jnp.log(r.AL[i, 0:heads, :])
        r.CXR[i] = r.CT[...].T.astype(BF)

        @pl.when(i != t)
        def _():
            copy(r.CXR.at[i], r.CTX.at[t], r.c_s.at[i], r.c_r.at[t], (d, i)).start()

    def bias_for(i):
        r.BIAS[...] = jnp.where(r.segc[:, 0:1] == seg_row(i), 0.0, NEG)

    arrived(kq, 0, 0, twin_q)
    ring_send(kq, 0, 1)
    ring_send(kd_, t, 0)
    def at_distance(k, take):
        @pl.when(t - k >= 0)
        def _():
            take(t - k)

        @pl.when(t + k < T)
        def _():
            take(t + k)

    def take_weights(tt):
        for k in (ko, ku):
            z_wait(k, tt)
            z_send(k, tt)
            ring_send(k, tt, 0)
        twin_o(tt, q)

    def take_tokens(tt):
        z_wait(kt, tt)
        z_send(kt, tt)
        weights_z(tt)

    for j in range(1, T):
        at_distance(j, take_weights)
        ring_adv(ko, tp(j - 1), twin_o)
        ring_adv(ku, tp(j - 1))
        if j == 1:
            for s in range(1, S):
                arrived(kq, 0, s, twin_q)
                if s + 1 < S:
                    ring_send(kq, 0, s + 1)
            copy(r.RQ, r.RQ, r.tw_s.at[1], r.tw_r.at[1], partner).wait_recv()
            project(t)
            attend(0)
        else:
            ring_fin(ko, tp(j - 2), twin_o)
        at_distance(j, take_tokens)
        if j == 1:
            ring_adv(kd_, t)
        project(tp(j))
        attend(j)
    inner = (t > 0) & (t < T - 1)
    edge = (t == 0) | (t == T - 1)

    def take_down(j):
        tt = tp(j)
        z_wait(kd_, tt)
        z_send(kd_, tt)
        ring_send(kd_, tt, 0)

    spin(0, T, finish_context)
    ring_adv(ko, tp(T - 1), twin_o)
    ring_adv(ku, tp(T - 1))
    ring_fin(ko, tp(T - 2), twin_o)
    ring_fin(ko, tp(T - 1), twin_o)
    take_down(1)

    @pl.when(inner)
    def _():
        for j in range(2, T):
            take_down(j)
            if j == 2:
                ring_adv(kd_, tp(1))

    r.CTX[t] = r.CXR[t]
    for k in range(1, T):
        tt = lax.rem(t + k, T)
        copy(r.CTX.at[tt], r.CTX.at[tt], r.c_s.at[tt], r.c_r.at[tt], partner).wait_recv()
    copy(r.RWO, r.RWO, r.tw_s.at[0], r.tw_r.at[0], partner).wait_recv()

    def out_dot(j):
        y = nt(r.CTX[j], merge(r.Wo[j]))

        @pl.when(j == 0)
        def _():
            r.FEED[0] = y

        @pl.when(j > 0)
        def _():
            r.FEED[0] += y

    spin(0, T, out_dot)

    def rows_of(body):
        def step(i):
            body(pl.ds(pl.multiple_of(i * RC, RC), RC))

        spin(0, TB // RC, step)

    def tally(n, x):
        r.SACC[n] += x.reshape(RC // 8, 8, D).sum(axis=0)

    def norm(x):
        mid = x - jnp.mean(x, axis=-1, keepdims=True)
        inverse = lax.rsqrt(jnp.mean(mid * mid, axis=-1, keepdims=True) + 1e-05)
        return mid * inverse, inverse

    def norm_back(up, gain, normed, inverse):
        e = up * gain
        return inverse * (
            e - jnp.mean(e, axis=-1, keepdims=True) - normed * jnp.mean(e * normed, axis=-1, keepdims=True)
        )

    def vec(n):
        return r.vecs[n : n + 1, :]

    def first_norm(at):
        x = r.X[t, at, :].astype(F32) + r.FEED[0, at, :] + vec(0)
        normed, inverse = norm(x)
        h1 = normed * vec(1) + vec(2)
        r.N1[at, :] = normed
        r.IV1[at, :] = inverse
        r.H1[at, :] = h1
        r.POOL[MID + c, at, :] = h1.astype(BF)

    rows_of(first_norm)

    def exchange(n, base, op="start"):
        ref = r.POOL.at[base + c]
        go(copy(ref, ref, r.e_s.at[n], r.e_r.at[n], partner), op)

    def exchanged(n, base):
        ref = r.POOL.at[base + oc]
        copy(ref, ref, r.e_s.at[n], r.e_r.at[n], partner).wait_recv()

    exchange(0, MID)

    @pl.when(edge)
    def _():
        for j in range(2, T):
            take_down(j)
            if j == 2:
                ring_adv(kd_, tp(1))

    for k in range(1, T):
        tt = lax.rem(t + k, T)
        copy(r.BU.at[tt], r.BU.at[tt], r.b_s.at[tt], r.b_r.at[tt], partner).wait_recv()
    exchanged(0, MID)

    def turn(src, dst):
        def step(b):
            y = r.POOL[src + b].astype(F32).T.astype(BF)
            dst[:, pl.ds(pl.multiple_of(b * TB, TB), TB)] = y

        spin(0, 2, step)

    def up(j):
        tt = tp(j)
        ring_fin(ku, tt)
        w = merge(r.Wu[tt])
        bias = r.BU[tt, :, pl.ds(lo, HC)]

        def block(b):
            r.PRE[...] = nn(r.POOL[MID + b], w) + bias

            def piece(i):
                at = pl.ds(pl.multiple_of(i * RC, RC), RC)
                v = r.PRE[at, :]
                cdf = 0.5 * (1.0 + lax.erf(v * 2.0 ** (-0.5)))
                slope = cdf + v * jnp.exp(-0.5 * v * v) * (2.0 * math.pi) ** (-0.5)
                to = pl.ds(pl.multiple_of(b * TB + i * RC, RC), RC)
                r.ACT[tt, to, :] = (v * cdf).astype(BF)
                r.SL[tt, to, :] = slope.astype(BF)

            spin(0, TB // RC, piece)

        spin(0, 2, block)

    for j in range(T):
        ahead = 2 if j == 0 else j + 1 if j >= 2 else T
        if ahead < T:
            ring_adv(kd_, tp(ahead))
        up(j)
    turn(MID, r.MIDT)

    def down(j):
        tt = tp(j)
        ring_fin(kd_, tt)
        w = merge(r.Wd[tt])

        def block(b):
            y = nt(r.ACT[tt, pl.ds(pl.multiple_of(b * TB, TB), TB), :], w)
            if j == 0:
                r.FEED[b] = y
            else:
                r.FEED[b] += y

        spin(0, 2, block)

    for j in range(T):
        down(j)

    def give(n):
        def step(at):
            r.POOL[FSND, at, :] = r.FEED[oc, at, :].astype(BF)

        rows_of(step)
        copy(r.POOL.at[FSND], r.POOL.at[FRCV], r.e_s.at[n], r.e_r.at[n], partner).start()
        copy(r.POOL.at[FRCV], r.POOL.at[FRCV], r.e_s.at[n], r.e_r.at[n], partner).wait_recv()
        copy(r.POOL.at[FSND], r.POOL.at[FRCV], r.e_s.at[n], r.e_r.at[n], partner).wait_send()

    def given(n, at):
        return r.FEED[c, at, :] + r.POOL[FRCV, at, :].astype(F32)

    give(1)

    def second_norm(at):
        x = r.H1[at, :] + given(1, at) + vec(3)
        normed, inverse = norm(x)
        g = r.out[at, :].astype(F32)
        r.out[at, :] = (normed * vec(4) + vec(5)).astype(BF)
        tally(0, g * normed)
        tally(1, g)
        back = norm_back(g, vec(4), normed, inverse)
        r.H1[at, :] = back
        low = back.astype(BF)
        r.POOL[GF + c, at, :] = low
        tally(2, low.astype(F32))

    rows_of(second_norm)
    exchange(2, GF)

    def drain_gather(k):
        def step(tt):
            if hasattr(k, "zs"):
                z_send(k, tt, "drain")
            for s in range(S):
                ring_send(k, tt, s, "drain")

        spin(0, T, step)

    drain_gather(ku)
    drain_gather(kd_)
    swap_u.wait_send()
    swap_d.wait_send()
    exchanged(2, GF)
    turn(GF, r.GFT)

    def slot_back(k):
        tt = tp(T - 1 - k)

        def block(b):
            to = pl.ds(pl.multiple_of(b * TB, TB), TB)
            r.PRE[...] = nn(r.POOL[GF + b], merge(r.Wd[tt]))

            def piece(i):
                at = pl.ds(pl.multiple_of(i * RC, RC), RC)
                tr = pl.ds(pl.multiple_of(b * TB + i * RC, RC), RC)
                gp = (r.PRE[at, :] * r.SL[tt, tr, :].astype(F32)).astype(BF)
                r.SL[tt, tr, :] = gp
                r.SBA[...] += gp.astype(F32).reshape(RC // 8, 8, HC).sum(axis=0)

            spin(0, TB // RC, piece)
            y = nt(r.SL[tt, to, :], merge(r.Wu[tt]))

            @pl.when(k == 0)
            def _():
                r.FEED[b] = y

            @pl.when(k > 0)
            def _():
                r.FEED[b] += y

        r.SBA[...] = jnp.zeros_like(r.SBA)
        spin(0, 2, block)
        r.SB[pl.ds(2 * tt + c, 1)] = r.SBA[...].sum(axis=0, keepdims=True)[None]

    def slot_weights(k):
        tt = tp(T - 1 - k)

        def down_weight(qq):
            at = pl.ds(pl.multiple_of(qq * 2 * R, 2 * R), 2 * R)
            r.Wd[tt, qq] = nn(r.GFT[at, :], r.ACT[tt]).astype(BF).reshape(2, R, HC)

        def up_weight(qq):
            at = pl.ds(pl.multiple_of(qq * 2 * R, 2 * R), 2 * R)
            r.Wu[tt, qq] = nn(r.MIDT[at, :], r.SL[tt]).astype(BF).reshape(2, R, HC)

        spin(0, NQ, down_weight)

        @pl.when(k < T - 1)
        def _():
            rs_send(kd_, tt, 0)

        spin(0, NQ, up_weight)

        @pl.when(k < T - 1)
        def _():
            rs_send(ku, tt, 0)

    H = T // 2

    def far(k):
        return tp(T - 1 - k)

    def pair_mid(k):
        rs_mid(kd_, far(k))
        rs_mid(ku, far(k))

    def pair_last(k):
        for w in (kd_, ku):
            rs_last(w, far(k))
            chain_first(w, far(k))

    def pair_on(k):
        chain_on(kd_, far(k))
        chain_on(ku, far(k))

    def part_last(w, k):
        rs_last(w, far(k))
        chain_first(w, far(k))

    def slots(k):
        slot_back(k)

        @pl.when(k == 0)
        def _():
            slot_weights(k)

        @pl.when(k == 1)
        def _():
            rs_mid(kd_, far(0))

        @pl.when(k == 2)
        def _():
            rs_mid(ku, far(0))

    spin(0, T, slots)
    give(3)

    def first_back(at):
        g = r.H1[at, :] + given(3, at)
        normed = r.N1[at, :]
        tally(3, g * normed)
        tally(4, g)
        back = norm_back(g, vec(1), normed, r.IV1[at, :])
        r.H1[at, :] = back
        low = back.astype(BF)
        r.gtok[at, :] = low
        tally(5, low.astype(F32))

    rows_of(first_back)

    def context_back(k):
        tt = tp(T - 1 - k)
        r.CXR[tt] = nn(r.gtok[...], merge(r.Wo[tt])).astype(BF)

        @pl.when(tt != t)
        def _():
            copy(r.CXR.at[tt], r.GC.at[t], r.gc_s.at[tt], r.gc_r.at[t], (d, tt)).start()

        @pl.when(tt == t)
        def _():
            r.GC[t] = r.CXR[t]

    for k in range(1, T):
        tt = lax.rem(t + k, T)
        copy(r.CXR.at[tt], r.CTX.at[t], r.c_s.at[tt], r.c_r.at[t], (d, tt)).wait_send()
    spin(0, T, context_back)
    spin(1, H, slot_weights)
    part_last(kd_, 0)
    for n in range(6):
        r.SV[n : n + 1, :] = r.SACC[n].sum(axis=0, keepdims=True)
    r.SV[6:8, :] = jnp.zeros((2, D), F32)

    def sum_core(n, ref, box, op):
        cp = copy(ref, box, r.a_s.at[0, n], r.a_r.at[0, n], partner)
        if op == "start":
            cp.start()
        else:
            copy(box, box, r.a_s.at[0, n], r.a_r.at[0, n], partner).wait_recv()
            cp.wait_send()
            ref[...] += box[...]

    def sum_group(stage, n, ref, box, me, count, dev, op):
        if op == "start":
            box[me] = ref[...]
        for k in range(1, count):
            other = lax.rem(me + k, count)
            sems = r.ag_s.at[stage, n, other], r.ag_r.at[stage, n, me]
            if op == "start":
                copy(box.at[me], box.at[me], *sems, dev(other)).start()
            else:
                copy(box.at[me], box.at[me], *sems, dev(other)).wait_send()
                copy(
                    box.at[other], box.at[other], r.ag_s.at[stage, n, other],
                    r.ag_r.at[stage, n, other], dev(other),
                ).wait_recv()
        if op != "start":
            total = box[0]
            for k in range(1, count):
                total = total + box[k]
            ref[...] = total

    def chip_dev(other):
        return (2 * other + c, t)

    def row_dev(other):
        return (d, other)

    sum_core(0, r.SV, r.SV1, "start")
    sum_core(1, r.SB, r.SB1, "start")

    outer = ind(t, 0, T) + ind(t, T - 1, T)

    def attend_back(j):
        i = tp(j) + (tp(T - 1 - j) - tp(j)) * outer
        at = pl.ds(pl.multiple_of(i * TB, TB), TB)

        @pl.when(i != t)
        def _():
            copy(r.GC.at[i], r.GC.at[i], r.gc_s.at[i], r.gc_r.at[i], partner).wait_recv()

        bias_for(i)
        for h in range(heads):
            pair = slice((h // 2) * 128, (h // 2) * 128 + 128)
            qh = r.Q[at, pair] * picks[h % 2]
            gh = r.GC[i, :, pair] * picks[h % 2]
            pr = jnp.exp(nt(r.K[:, pair], qh) + r.BIAS[...] - r.AM[i, h : h + 1, :])
            gp = nt(r.V[:, pair], gh)
            r.DV[:, pair] += nn(pr.astype(BF), gh)
            prod = pr * gp
            delta = jnp.sum(prod, axis=0, keepdims=True)
            ds = (prod - pr * delta).astype(BF)
            r.DK[:, pair] += nn(ds, qh)
            r.CT[h * HD : (h + 1) * HD, :] = nn(r.KT[h * HD : (h + 1) * HD, :], ds) * HD ** (-0.5)
        r.DPJ[i, :, 0:C] = r.CT[...].T.astype(BF)

    exchange(0, MID, "drain")
    exchange(2, GF, "drain")

    r.SQ[...] = jnp.zeros_like(r.SQ)

    def input_back(k):
        tt = far(k)
        at = pl.ds(pl.multiple_of(tt * TB, TB), TB)
        r.DPJ[tt, :, C : 2 * C] = r.DK[at, :].astype(BF)
        r.DPJ[tt, :, 2 * C : 3 * C] = r.DV[at, :].astype(BF)
        r.SQ[0:1, :] += r.DPJ[tt, :, 0:C].astype(F32).sum(axis=0, keepdims=True)
        r.SQ[1:2, :] += r.DPJ[tt, :, 2 * C : 3 * C].astype(F32).sum(axis=0, keepdims=True)
        r.POOL[tt] = nt(r.DPJ[tt], merge(r.Wq[...])).astype(BF)

        @pl.when(jnp.int32(k) < 2)
        def _():
            chain_first(kg, tt)

    spin(0, H, attend_back)
    part_last(ku, 0)
    for k in range(1, H):
        pair_mid(k)
    spin(H, T - 1, slot_weights)
    sum_core(0, r.SV, r.SV1, "end")
    sum_core(1, r.SB, r.SB1, "end")
    sum_group(0, 0, r.SV, r.SV2, q, NQ, chip_dev, "start")
    sum_group(0, 1, r.SB, r.SB2, q, NQ, chip_dev, "start")

    def attend_late(j):
        attend_back(j)
        if T - 1 > reach:

            @pl.when((j == T - 2) & edge)
            def _():
                input_back(0)

    spin(H, T, attend_late)
    def input_rest(k):
        @pl.when((k > 0) | inner | (T - 1 <= reach))
        def _():
            input_back(k)

    spin(0, T, input_rest)
    spin(T - 1, T, slot_weights)
    for k in range(H, T - 1):
        pair_mid(k)
    sum_core(2, r.SQ, r.SQ1, "start")
    drain_gather(ko)
    copy(r.RWO, r.RWO, r.tw_s.at[0], r.tw_r.at[0], partner).wait_send()

    r.GFT[:, 0:TB] = r.gtok[...].astype(F32).T.astype(BF)

    def out_back(tt):
        def weight(qq):
            at = pl.ds(pl.multiple_of(qq * 2 * R, 2 * R), 2 * R)
            y = nn(r.GFT[at, 0:TB], r.CTX[tt]).astype(BF)
            r.Wo[tt, pl.ds(2 * qq, 2)] = y.reshape(2, R, C)
            copy(r.Wo.at[tt, 2 * qq + oc], r.RWO.at[tt, qq], r.go_s.at[0], r.go_r.at[0], partner).start()

        spin(0, NQ, weight)

    spin(0, T, out_back)

    pair_on(0)
    copy(r.RWO, r.RWO, r.go_s.at[0], r.go_r.at[0], partner).wait_recv()

    def out_join(k):
        tt = tp(T - 1 - k)

        def step(qq):
            add(r.Wo.at[tt, 2 * qq + c], r.RWO.at[tt, qq])

        spin(0, NQ, step)
        rs_send(ko, tt, 0)

    spin(0, T, out_join)

    copy(r.RQ, r.RQ, r.tw_s.at[1], r.tw_r.at[1], partner).wait_send()
    for s in range(S):
        ring_send(kq, 0, s, "drain")
    many = max(2, 256 // R)

    def qkv_weight(g):
        cols = pl.ds(pl.multiple_of(g * many * R, 128), many * R)
        x = merge(r.X[:, :, cols])
        y = lax.dot_general(
            x, merge(r.DPJ[...]), (((0,), (0,)), ((), ())), preferred_element_type=F32
        )
        r.Wq[pl.ds(many * g, many)] = y.astype(BF).reshape(many, R, 3 * C)
        for k in range(many // 2):
            qq = g * (many // 2) + k
            copy(r.Wq.at[2 * qq + oc], r.RQ.at[qq], r.go_s.at[1], r.go_r.at[1], partner).start()

    spin(0, DP // many, qkv_weight)
    sum_core(2, r.SQ, r.SQ1, "end")
    sum_group(0, 2, r.SQ, r.SQ2, q, NQ, chip_dev, "start")
    copy(r.RQ, r.RQ, r.go_s.at[1], r.go_r.at[1], partner).wait_recv()

    def q_join(qq):
        add(r.Wq.at[2 * qq + c], r.RQ.at[qq])

    spin(0, NQ, q_join)
    rs_send(kq, 0, 0)
    rs_send(kd_, t, 0)
    rs_send(ku, t, 0)
    chain_on(kg, far(0))
    for k in range(1, H):
        pair_last(k)
    for k in range(2, T - 1):
        chain_first(kg, far(k))
    sum_group(0, 0, r.SV, r.SV2, q, NQ, chip_dev, "end")
    sum_group(0, 1, r.SB, r.SB2, q, NQ, chip_dev, "end")
    sum_group(1, 0, r.SV, r.SV3, t, T, row_dev, "start")
    sum_group(1, 1, r.SB, r.SB3, t, T, row_dev, "start")
    for k in range(H, T - 1):
        rs_last(kd_, far(k))
        rs_last(ku, far(k))
    for k in range(T):
        rs_mid(ko, far(k))
    rs_mid(kq, 0)
    order = [2, 1] if T == 4 else list(range(1, T - 1))
    for n, k in enumerate(order):
        pair_on(k)
        chain_on(kg, far(k))
        if n == 0:
            pair_mid(T - 1)
    for k in range(T - 1):
        rs_last(ko, far(k))
        chain_first(ko, far(k))
    for k in range(H, T - 1):
        chain_first(kd_, far(k))
        chain_first(ku, far(k))
    for k in range(T - 1):
        chain_on(ko, far(k))
    rs_last(kd_, t)
    rs_last(ku, t)
    rs_last(ko, t)
    rs_last(kq, 0)
    sum_group(1, 0, r.SV, r.SV3, t, T, row_dev, "end")
    sum_group(1, 1, r.SB, r.SB3, t, T, row_dev, "end")
    sum_group(0, 2, r.SQ, r.SQ2, q, NQ, chip_dev, "end")
    chain_end(kg)

    def finish(at):
        r.gtok[at, :] = (r.H1[at, :] + r.POOL[t, at, :].astype(F32)).astype(BF)

    rows_of(finish)
    chain_end(kd_)
    chain_end(ku)
    chain_end(ko)
    cps = []
    for n, ref in enumerate((r.Wu, r.Wd)):
        cp = copy(ref.at[t, q, oc], r.FSW.at[n], r.fs_s.at[n], r.fs_r.at[n], partner)
        cp.start()
        cps.append(cp)
    for n in range(3):
        r.gwq[n] = r.Wq[d, :, n * C : (n + 1) * C]
    r.gwo[...] = r.Wo[t, d]
    r.sv[...] = r.SV[...]
    r.sbq[...] = r.SQ[...]
    r.sbu[...] = r.SB[pl.ds(2 * t, 2)]
    for n, (ref, o) in enumerate(((r.Wu, r.gwu), (r.Wd, r.gwd))):
        copy(r.FSW.at[n], r.FSW.at[n], r.fs_s.at[n], r.fs_r.at[n], partner).wait_recv()
        o[:, pl.ds(lo, HC)] = ref[t, q, c]
        o[:, pl.ds(ro, HC)] = r.FSW[n]
        cps[n].wait_send()

    def drain(tt):
        z_send(kt, tt, "drain")
        for k in (kd_, ku, ko):
            for s in range(S):
                rs_send(k, tt, s, "drain")
            chain_send(k, tt, "drain")
        chain_send(kg, tt, "drain")

        @pl.when(tt != t)
        def _():
            copy(r.CXR.at[tt], r.GC.at[t], r.gc_s.at[tt], r.gc_r.at[t], (d, tt)).wait_send()
            copy(r.BU.at[t], r.BU.at[t], r.b_s.at[tt], r.b_r.at[t], (d, tt)).wait_send()

    spin(0, T, drain)
    for s in range(S):
        rs_send(kq, 0, s, "drain")
    copy(r.RWO, r.RWO, r.go_s.at[0], r.go_r.at[0], partner).wait_send()
    copy(r.RQ, r.RQ, r.go_s.at[1], r.go_r.at[1], partner).wait_send()


def layer(cf, *args):
    T, NQ, TB, D, R, C, HC, DP = cf.T, cf.NQ, cf.TB, cf.D, cf.R, cf.C, cf.HC, cf.DP
    S = NQ // 2
    RW = T * TB
    Cq = 3 * C
    heads = C // HD
    hp = -(-heads // 8) * 8
    dma = pltpu.SemaphoreType.DMA
    V = pltpu.VMEM
    ins = ["tok", "og", "wq", "wo", "wu", "wd", "bqv", "bup", "b_out", "g1", "n1", "b_down", "g2", "n2", "seg"]
    outs = {
        "out": ((TB, D), BF), "gtok": ((TB, D), BF), "gwq": ((3, R, C), BF), "gwo": ((R, C), BF),
        "gwu": ((R, 2 * HC), BF), "gwd": ((R, 2 * HC), BF), "sv": ((8, D), F32),
        "sbq": ((8, C), F32), "sbu": ((2, 1, HC), F32),
    }
    scratch = {
        "X": V((T, TB, D), BF), "Wq": V((DP, R, Cq), BF), "Wo": V((T, DP, R, C), BF),
        "Wu": V((T, NQ, 2, R, HC), BF), "Wd": V((T, NQ, 2, R, HC), BF), "BU": V((T, 1, 2 * HC), F32), "vecs": V((8, D), F32), "segc": V((RW, 128), F32),
        "Q": V((RW, C), BF), "K": V((RW, C), BF), "V": V((RW, C), BF),
        "KT": V((C, RW), BF), "VT": V((C, RW), BF), "BIAS": V((RW, TB), F32),
        "CT": V((C, TB), F32), "AM": V((T, hp, TB), F32), "AL": V((T, hp, TB), F32), "ACC": V((T, C, TB), F32), "CXR": V((T, TB, C), BF),
        "CTX": V((T, TB, C), BF), "FEED": V((2, TB, D), F32), "N1": V((TB, D), F32),
        "IV1": V((TB, 1), F32), "H1": V((TB, D), F32), "POOL": V((max(6, T), TB, D), BF),
        "MIDT": V((D, 2 * TB), BF), "PRE": V((TB, HC), F32), "ACT": V((T, 2 * TB, HC), BF),
        "SL": V((T, 2 * TB, HC), BF),
        "GFT": V((D, 2 * TB), BF),
        "GC": V((T, TB, C), BF),
        "DK": V((RW, C), F32), "DV": V((RW, C), F32), "DPJ": V((T, TB, Cq), BF),
        "g_ZB": V((T + 1, TB, D), BF), "RWO": V((T, NQ, R, C), BF), "RQ": V((NQ, R, Cq), BF),
        "FSW": V((2, R, HC), BF),
        "q_HB": V((1, 2, R // 2, Cq), BF), "q_FB": V((1, 2, S - 1, R, Cq), BF),
        "o_HB": V((T, 2, R // 2, C), BF), "o_FB": V((T, 2, S - 1, R, C), BF), "o_ZB": V((T + 1, R, C), BF),
        "u_HB": V((T, 2, R, HC), BF), "u_FB": V((T, 2, S - 1, 2, R, HC), BF), "u_ZB": V((T + 1, 2, R, HC), BF),
        "d_HB": V((T, 2, R, HC), BF), "d_FB": V((T, 2, S - 1, 2, R, HC), BF), "d_ZB": V((T + 1, 2, R, HC), BF),
        "SACC": V((6, 8, D), F32), "SBA": V((8, HC), F32),
        "SV": V((8, D), F32), "SV1": V((8, D), F32), "SV2": V((NQ, 8, D), F32), "SV3": V((T, 8, D), F32),
        "SB": V((2 * T, 1, HC), F32), "SB1": V((2 * T, 1, HC), F32), "SB2": V((NQ, 2 * T, 1, HC), F32),
        "SB3": V((T, 2 * T, 1, HC), F32),
        "SQ": V((8, C), F32), "SQ1": V((8, C), F32), "SQ2": V((NQ, 8, C), F32),
        "t_zs": dma((T, 2)), "t_zr": dma((T,)),
        "q_rs": dma((1, 2, S)), "q_rr": dma((1, 2, S)), "q_gs": dma((1, 2, S)), "q_gr": dma((1, 2, S)),
        "tw_s": dma((2,)), "tw_r": dma((2,)), "sw_s": dma((2,)), "sw_r": dma((2,)),
        "b_s": dma((T,)), "b_r": dma((T,)), "c_s": dma((T,)), "c_r": dma((T,)),
        "e_s": dma((4,)), "e_r": dma((4,)), "gc_s": dma((T,)), "gc_r": dma((T,)),
        "go_s": dma((2,)), "go_r": dma((2,)), "g_cs": dma((T,)), "g_cr": dma((T + 1,)),
        "a_s": dma((1, 3)), "a_r": dma((1, 3)),
        "ag_s": dma((2, 3, max(NQ, T))), "ag_r": dma((2, 3, max(NQ, T))),
        "fs_s": dma((2,)), "fs_r": dma((2,)), "in_s": dma((5,)),
    }
    for n in "oud":
        scratch[n + "_zs"] = dma((T, 2))
        scratch[n + "_zr"] = dma((T,))
        for m in ("_rs", "_rr", "_gs", "_gr"):
            scratch[n + m] = dma((T, 2, S))
        scratch[n + "_cs"] = dma((T,))
        scratch[n + "_cr"] = dma((T + 1,))
    names = ins + list(outs) + list(scratch)
    vm = pl.BlockSpec(memory_space=pltpu.VMEM)
    return pl.pallas_call(
        functools.partial(layer_kernel, cf, names),
        out_shape=tuple(jax.ShapeDtypeStruct(s, k) for s, k in outs.values()),
        in_specs=[pl.BlockSpec(memory_space=pl.ANY)] * 3 + [vm] * (len(ins) - 3),
        out_specs=(vm,) * len(outs),
        scratch_shapes=list(scratch.values()),
        compiler_params=pltpu.CompilerParams(
            collective_id=0, has_side_effects=True, vmem_limit_bytes=VMEM_LIMIT
        ),
        name="layer",
    )(*args)


def tail_kernel(cf, *refs):
    src, dst = refs[:9], refs[9:]
    out, gtok, gwq, gwo, gwu, gwd, sv, sbq, sbu = src
    dst[0][...] = out[...]
    dst[1][...] = gtok[...]
    dst[2][...] = gwq[...].astype(F32)
    dst[3][...] = sbq[0:2, :]
    dst[4][...] = gwo[...].astype(F32).T
    for n, row in ((5, 5), (6, 3), (7, 4), (11, 2), (12, 0), (13, 1)):
        dst[n][...] = sv[row : row + 1, :].reshape(cf.D)
    dst[8][...] = gwu[...].astype(F32)
    for n in range(2):
        dst[9][pl.ds(n * cf.HC, cf.HC)] = sbu[n].reshape(cf.HC)
    dst[10][...] = gwd[...].astype(F32).T


def tail(cf, *args):
    R, C, D, HC, TB = cf.R, cf.C, cf.D, cf.HC, cf.TB
    vm = pl.BlockSpec(memory_space=pltpu.VMEM)
    shapes = [
        ((TB, D), BF), ((TB, D), BF), ((3, R, C), F32), ((2, C), F32), ((C, R), F32),
        ((D,), F32), ((D,), F32), ((D,), F32), ((R, 2 * HC), F32), ((2 * HC,), F32),
        ((2 * HC, R), F32), ((D,), F32), ((D,), F32), ((D,), F32),
    ]
    return pl.pallas_call(
        functools.partial(tail_kernel, cf),
        out_shape=tuple(jax.ShapeDtypeStruct(*s) for s in shapes),
        in_specs=[vm] * len(args),
        out_specs=(vm,) * len(shapes),
        name="tail",
    )(*args)


def shards(
    tokens, segment_ids, out_grad, w_qkv, b_qv, w_out, b_out, norm1_gain, norm1_bias,
    w_up, b_up, w_down, b_down, norm2_gain, norm2_bias,
):
    DP, T = lax.axis_size("dp"), lax.axis_size("tensor")
    TB, D = tokens.shape
    R, _, C = w_qkv.shape
    HC = w_up.shape[1] // 2
    cf = SimpleNamespace(T=T, NQ=DP // 2, TB=TB, D=D, R=R, C=C, HC=HC, DP=DP)
    res = layer(
        cf, tokens, out_grad, w_qkv.transpose(1, 0, 2), w_out, w_up, w_down, b_qv, b_up,
        b_out, norm1_gain, norm1_bias, b_down, norm2_gain, norm2_bias, segment_ids,
    )
    res = list(tail(cf, *res))
    res[2] = res[2].transpose(1, 0, 2)
    return tuple(res)


def solution(mesh):
    tok = P(("dp", "tensor"), None)
    in_specs = (
        tok, P("dp", None), tok, P("dp", None, "tensor"), P(None, "tensor"), P("tensor", "dp"),
        P(), P(), P(), P("dp", "tensor"), P("tensor"), P("tensor", "dp"), P(), P(), P(),
    )
    out_specs = (
        tok, tok, P("dp", None, "tensor"), P(None, "tensor"), P("tensor", "dp"),
        P(), P(), P(), P("dp", "tensor"), P("tensor"), P("tensor", "dp"), P(), P(), P(),
    )
    return jax.shard_map(shards, mesh=mesh, in_specs=in_specs, out_specs=out_specs, check_vma=False)
```

```python
import functools
import math
from types import SimpleNamespace

import jax
import jax.numpy as jnp
from jax import lax
from jax.experimental import pallas as pl
from jax.experimental.pallas import tpu as pltpu
from jax.sharding import PartitionSpec as P

HD = 64
SEG_MOST = 512
MESH = pl.DeviceIdType.MESH
BF = jnp.bfloat16
F32 = jnp.float32
NEG = -1e30
VMEM_LIMIT = 67043328
MID, GF, FSND, FRCV = 0, 2, 4, 5


def nn(a, b):
    return jnp.dot(a, b, preferred_element_type=F32)


def nt(a, b):
    return lax.dot_general(a, b, (((1,), (1,)), ((), ())), preferred_element_type=F32)


def merge(x):
    return x.reshape(-1, x.shape[-1])


def spin(lo, hi, body):
    def step(i, carry):
        body(i)
        return carry

    lax.fori_loop(lo, hi, step, 0)


def order_table(T):
    return [sorted(range(T), key=lambda b: (abs(b - a), b if a < T / 2 else -b)) for a in range(T)]


def layer_kernel(cf, names, *refs):
    r = SimpleNamespace(**dict(zip(names, refs)))
    T, NQ, TB, D, R, C, HC, DP = cf.T, cf.NQ, cf.TB, cf.D, cf.R, cf.C, cf.HC, cf.DP
    S = NQ // 2
    RW = T * TB
    RC = 32
    heads = C // HD
    table = order_table(T)

    d = lax.axis_index("dp")
    t = lax.axis_index("tensor")
    q = lax.div(d, 2)
    c = d - 2 * q
    oc = 1 - c
    partner = (2 * q + oc, t)

    def perm(x):
        if NQ % 4:
            return x
        m = lax.rem(x, 4)
        return x + lax.div(m, 2) * (1 - 2 * lax.rem(m, 2))

    pos = perm(q)

    def chip_at(x):
        return perm(lax.rem(x + 4 * NQ, NQ))

    nxt = (2 * chip_at(pos + 1) + c, t)
    prv = (2 * chip_at(pos - 1) + c, t)

    def ind(a, b, n):
        x = lax.rem(a - b + n, n)
        return 1 - lax.div(x + n - 1, n)

    def tp(j):
        if isinstance(j, int):
            return sum(table[a][j] * ind(t, a, T) for a in range(T))
        js = [ind(j, b, T) for b in range(T)]
        total = 0
        for a in range(T):
            total = total + ind(t, a, T) * sum(table[a][b] * js[b] for b in range(T))
        return total

    def copy(src, dst, ss, rs, dev):
        return pltpu.make_async_remote_copy(
            src_ref=src, dst_ref=dst, send_sem=ss, recv_sem=rs, device_id=dev, device_id_type=MESH
        )

    def go(cp, op):
        if op == "start":
            cp.start()
        else:
            cp.wait_send()

    def half(kd, ref, h):
        if kd.split:
            return ref.at[h]
        n = kd.rows // 2
        return ref.at[pl.ds(h * n, n)]

    kt = SimpleNamespace(piece=lambda tt, qq: r.X.at[tt], zs=r.t_zs, zr=r.t_zr)
    kq = SimpleNamespace(
        piece=lambda tt, qq: r.Wq.at[2 * qq + c], split=False, rows=R, rs=r.q_rs, rr=r.q_rr,
        gs=r.q_gs, gr=r.q_gr, HB=r.q_HB, FB=r.q_FB,
    )
    ko = SimpleNamespace(
        piece=lambda tt, qq: r.Wo.at[tt, 2 * qq + c], split=False, rows=R, zs=r.o_zs, zr=r.o_zr,
        rs=r.o_rs, rr=r.o_rr, gs=r.o_gs, gr=r.o_gr, HB=r.o_HB, FB=r.o_FB,
        cs=r.o_cs, cr=r.o_cr, ZB=r.o_ZB,
    )
    ku = SimpleNamespace(
        piece=lambda tt, qq: r.Wu.at[tt, qq], split=True, rows=2 * R, zs=r.u_zs, zr=r.u_zr,
        rs=r.u_rs, rr=r.u_rr, gs=r.u_gs, gr=r.u_gr, HB=r.u_HB, FB=r.u_FB,
        cs=r.u_cs, cr=r.u_cr, ZB=r.u_ZB,
    )
    kd_ = SimpleNamespace(
        piece=lambda tt, qq: r.Wd.at[tt, qq], split=True, rows=2 * R, zs=r.d_zs, zr=r.d_zr,
        rs=r.d_rs, rr=r.d_rr, gs=r.d_gs, gr=r.d_gr, HB=r.d_HB, FB=r.d_FB,
        cs=r.d_cs, cr=r.d_cr, ZB=r.d_ZB,
    )
    kg = SimpleNamespace(piece=lambda tt, qq: r.POOL.at[tt], cs=r.g_cs, cr=r.g_cr, ZB=r.g_ZB)

    def z_right(k, tt, op):
        @pl.when((tt <= t) & (t < T - 1))
        def _():
            ref = k.piece(tt, q)
            go(copy(ref, ref, k.zs.at[tt, 0], k.zr.at[tt], (d, t + 1)), op)

    def z_left(k, tt, op):
        @pl.when((tt >= t) & (t > 0))
        def _():
            ref = k.piece(tt, q)
            go(copy(ref, ref, k.zs.at[tt, 1], k.zr.at[tt], (d, t - 1)), op)

    def z_send(k, tt, op="start"):
        z_right(k, tt, op)
        z_left(k, tt, op)

    def z_wait(k, tt):
        ref = k.piece(tt, q)
        copy(ref, ref, k.zs.at[tt, 0], k.zr.at[tt], partner).wait_recv()

    def ring_send(k, tt, s, op="start"):
        a = k.piece(tt, chip_at(pos - s))
        b = k.piece(tt, chip_at(pos + s))
        if s == S - 1:
            a, b = half(k, a, 0), half(k, b, 1)
        go(copy(a, a, k.rs.at[tt, 0, s], k.rr.at[tt, 0, s], nxt), op)
        go(copy(b, b, k.rs.at[tt, 1, s], k.rr.at[tt, 1, s], prv), op)

    def ring_wait(k, tt, s):
        a = k.piece(tt, chip_at(pos - 1 - s))
        b = k.piece(tt, chip_at(pos + 1 + s))
        if s == S - 1:
            a, b = half(k, a, 0), half(k, b, 1)
        copy(a, a, k.rs.at[tt, 0, s], k.rr.at[tt, 0, s], nxt).wait_recv()
        copy(b, b, k.rs.at[tt, 1, s], k.rr.at[tt, 1, s], prv).wait_recv()

    def twin_o(tt, qq):
        ref = r.Wo.at[tt, 2 * qq + c]
        copy(ref, ref, r.tw_s.at[0], r.tw_r.at[0], partner).start()

    def twin_q(tt, qq):
        ref = r.Wq.at[2 * qq + c]
        copy(ref, ref, r.tw_s.at[1], r.tw_r.at[1], partner).start()

    def arrived(k, tt, s, twin):
        ring_wait(k, tt, s)
        if twin is not None:
            twin(tt, chip_at(pos + 1 + s))
            if s < S - 1:
                twin(tt, chip_at(pos - 1 - s))

    def ring_adv(k, tt, twin=None):
        for s in range(1, S):
            arrived(k, tt, s - 1, twin)
            ring_send(k, tt, s)

    def ring_fin(k, tt, twin=None):
        arrived(k, tt, S - 1, twin)

    def add(dst, src):
        dst[...] = (dst[...].astype(F32) + src[...].astype(F32)).astype(BF)

    def rs_send(k, tt, s, op="start"):
        a = k.piece(tt, chip_at(pos + S - s))
        b = k.piece(tt, chip_at(pos - S + s))
        if s == 0:
            a, b = half(k, a, 0), half(k, b, 1)
            da, db = k.HB.at[tt, 0], k.HB.at[tt, 1]
        else:
            da, db = k.FB.at[tt, 0, s - 1], k.FB.at[tt, 1, s - 1]
        go(copy(a, da, k.gs.at[tt, 0, s], k.gr.at[tt, 0, s], nxt), op)
        go(copy(b, db, k.gs.at[tt, 1, s], k.gr.at[tt, 1, s], prv), op)

    def rs_add(k, tt, s):
        a = k.piece(tt, chip_at(pos + S - s - 1))
        b = k.piece(tt, chip_at(pos - S + s + 1))
        if s == 0:
            a, b = half(k, a, 0), half(k, b, 1)
            da, db = k.HB.at[tt, 0], k.HB.at[tt, 1]
        else:
            da, db = k.FB.at[tt, 0, s - 1], k.FB.at[tt, 1, s - 1]
        copy(da, da, k.gs.at[tt, 0, s], k.gr.at[tt, 0, s], nxt).wait_recv()
        add(a, da)
        copy(db, db, k.gs.at[tt, 1, s], k.gr.at[tt, 1, s], prv).wait_recv()
        add(b, db)

    def rs_mid(k, tt):
        for s in range(1, S):
            rs_add(k, tt, s - 1)
            rs_send(k, tt, s)

    def rs_last(k, tt):
        rs_add(k, tt, S - 1)

    def chain_send(k, tt, op="start"):
        ref = k.piece(tt, q)

        @pl.when(tt > t)
        def _():
            go(copy(ref, k.ZB.at[tt], k.cs.at[tt], k.cr.at[tt], (d, t + 1)), op)

        @pl.when(tt < t)
        def _():
            slot = tt + (T - tt) * ind(tt, t - 1, T)
            go(copy(ref, k.ZB.at[slot], k.cs.at[tt], k.cr.at[slot], (d, t - 1)), op)

    def chain_take(k, tt, slot):
        copy(k.ZB.at[slot], k.ZB.at[slot], k.cs.at[tt], k.cr.at[slot], partner).wait_recv()
        add(k.piece(tt, q), k.ZB.at[slot])

    def chain_first(k, tt):
        @pl.when(((tt > t) & (t == 0)) | ((tt < t) & (t == T - 1)))
        def _():
            chain_send(k, tt)

    def chain_on(k, tt):
        @pl.when(((tt > t) & (t > 0)) | ((tt < t) & (t < T - 1)))
        def _():
            chain_take(k, tt, tt)
            chain_send(k, tt)

    def chain_end(k):
        @pl.when(t > 0)
        def _():
            chain_take(k, t, t)

        @pl.when(t < T - 1)
        def _():
            chain_take(k, t, T)

    barrier = pltpu.get_barrier_semaphore()
    peers = [partner]
    peers += [(2 * lax.rem(q + k, NQ) + c, t) for k in range(1, NQ)]
    peers += [(d, lax.rem(t + k, T)) for k in range(1, T)]
    for peer in peers:
        pl.semaphore_signal(barrier, inc=1, device_id=peer, device_id_type=MESH)
    gets = [
        pltpu.make_async_copy(r.tok, r.X.at[t], r.in_s.at[0]),
        pltpu.make_async_copy(r.og, r.out, r.in_s.at[1]),
    ]
    for n in range(3):
        gets.append(
            pltpu.make_async_copy(r.wq.at[n], r.Wq.at[d, :, pl.ds(n * C, C)], r.in_s.at[2 + n])
        )
    for get in gets:
        get.start()
    lo = pl.multiple_of(c * HC, 128)
    ro = pl.multiple_of(oc * HC, 128)

    def flipped(x):
        return x.astype(F32).T.astype(BF)

    r.Wo[t, d] = flipped(r.wo[...])
    r.FSW[0] = r.wu[:, pl.ds(ro, HC)]
    r.FSW[1] = flipped(r.wd[pl.ds(ro, HC), :])
    r.Wu[t, q, c] = r.wu[:, pl.ds(lo, HC)]
    r.Wd[t, q, c] = flipped(r.wd[pl.ds(lo, HC), :])
    r.BU[t] = r.bup[...].astype(F32).reshape(1, 2 * HC)
    for n, name in enumerate(("b_out", "g1", "n1", "b_down", "g2", "n2")):
        r.vecs[n : n + 1, :] = getattr(r, name)[...].astype(F32).reshape(1, D)
    r.segc[...] = jnp.broadcast_to(r.seg[...].astype(F32), (128, RW)).T
    for get in gets:
        get.wait()
    pl.semaphore_wait(barrier, len(peers))

    swap_u = copy(r.FSW.at[0], r.Wu.at[t, q, c], r.sw_s.at[0], r.sw_r.at[0], partner)
    swap_d = copy(r.FSW.at[1], r.Wd.at[t, q, c], r.sw_s.at[1], r.sw_r.at[1], partner)
    swap_u.start()
    z_send(ko, t)
    twin_q(0, q)
    ring_send(kq, 0, 0)
    swap_d.start()
    twin_o(t, q)
    ring_send(ko, t, 0)

    def swapped(n, ref):
        ref = ref.at[t, q, oc]
        copy(ref, ref, r.sw_s.at[n], r.sw_r.at[n], partner).wait_recv()

    swapped(0, r.Wu)
    z_send(ku, t)
    z_send(kt, t)
    ring_send(ku, t, 0)
    swapped(1, r.Wd)

    def weights_z(tt):
        @pl.when(tt == 0)
        def _():
            z_right(kd_, t, "start")

        @pl.when(tt == T - 1)
        def _():
            z_left(kd_, t, "start")

    weights_z(t)
    for k in range(1, T):
        tt = lax.rem(t + k, T)
        copy(r.BU.at[t], r.BU.at[t], r.b_s.at[tt], r.b_r.at[t], (d, tt)).start()
    r.SACC[...] = jnp.zeros_like(r.SACC)
    r.SB[...] = jnp.zeros_like(r.SB)
    r.DK[...] = jnp.zeros_like(r.DK)
    r.DV[...] = jnp.zeros_like(r.DV)
    r.AM[...] = jnp.full_like(r.AM, NEG)
    r.AL[...] = jnp.zeros_like(r.AL)
    r.ACC[...] = jnp.zeros_like(r.ACC)

    def project(tt):
        x = r.X[tt]
        at = pl.ds(pl.multiple_of(tt * TB, TB), TB)
        for part, name in enumerate(("Q", "K", "V")):
            w = merge(r.Wq[:, :, part * C : (part + 1) * C])
            y = nn(x, w)
            if part != 1:
                y = y + r.bqv[part // 2 : part // 2 + 1, :].astype(F32)
            y = y.astype(BF)
            if part == 0:
                r.Q[at, :] = y * jnp.asarray(HD ** (-0.5), BF)
            elif part == 1:
                r.K[at, :] = y
                r.KT[:, at] = y.astype(F32).T.astype(BF)
            else:
                r.V[at, :] = y
                r.VT[:, at] = y.astype(F32).T.astype(BF)

    lane = lax.broadcasted_iota(jnp.int32, (1, 128), 1)
    picks = [(lane < HD).astype(F32).astype(BF), (lane >= HD).astype(F32).astype(BF)]
    reach = (SEG_MOST - 2) // TB + 1

    def rows_at(i):
        return pl.ds(pl.multiple_of(i * TB, TB), TB)

    def seg_row(i):
        return r.seg[:, rows_at(i)].astype(F32)

    def pair_up(i, b):
        bias = jnp.where(r.segc[rows_at(b), 0:1] == seg_row(i), 0.0, NEG)
        pairs = [slice((h // 2) * 128, (h // 2) * 128 + 128) for h in range(heads)]
        owns = [slice(h * HD, (h + 1) * HD) for h in range(heads)]
        before = [r.AM[i, h : h + 1, :] for h in range(heads)]
        sums = [r.AL[i, h : h + 1, :] for h in range(heads)]
        scs = [
            nt(r.K[rows_at(b), pairs[h]], r.Q[rows_at(i), pairs[h]] * picks[h % 2]) + bias
            for h in range(heads)
        ]
        tops = [jnp.maximum(before[h], jnp.max(scs[h], axis=0, keepdims=True)) for h in range(heads)]
        es = [jnp.exp(scs[h] - tops[h]) for h in range(heads)]
        shrinks = [jnp.exp(before[h] - tops[h]) for h in range(heads)]
        news = [nn(r.VT[owns[h], rows_at(b)], es[h].astype(BF)) for h in range(heads)]
        for h in range(heads):
            r.AM[i, h : h + 1, :] = tops[h]
            r.AL[i, h : h + 1, :] = sums[h] * shrinks[h] + jnp.sum(es[h], axis=0, keepdims=True)
            r.ACC[i, owns[h], :] = r.ACC[i, owns[h], :] * shrinks[h] + news[h]

    def attend(j):
        new = tp(j)

        def one(n):
            other = tp(lax.div(n, 2))
            side = lax.rem(n, 2)
            i = other + (new - other) * side
            b = new + (other - new) * side

            @pl.when((i - b <= reach) & (b - i <= reach))
            def _():
                pair_up(i, b)

        spin(0, 2 * j + 1, one)

    def finish_context(j):
        i = lax.rem(t + 1 + j, T)
        for h in range(heads):
            own = slice(h * HD, (h + 1) * HD)
            r.CT[own, :] = r.ACC[i, own, :] / r.AL[i, h : h + 1, :]
        r.AM[i, 0:heads, :] = r.AM[i, 0:heads, :] + jnp.log(r.AL[i, 0:heads, :])
        r.CXR[i] = r.CT[...].T.astype(BF)

        @pl.when(i != t)
        def _():
            copy(r.CXR.at[i], r.CTX.at[t], r.c_s.at[i], r.c_r.at[t], (d, i)).start()

    def bias_for(i):
        r.BIAS[...] = jnp.where(r.segc[:, 0:1] == seg_row(i), 0.0, NEG)

    arrived(kq, 0, 0, twin_q)
    ring_send(kq, 0, 1)
    ring_send(kd_, t, 0)
    def at_distance(k, take):
        @pl.when(t - k >= 0)
        def _():
            take(t - k)

        @pl.when(t + k < T)
        def _():
            take(t + k)

    def take_weights(tt):
        for k in (ko, ku):
            z_wait(k, tt)
            z_send(k, tt)
            ring_send(k, tt, 0)
        twin_o(tt, q)

    def take_tokens(tt):
        z_wait(kt, tt)
        z_send(kt, tt)
        weights_z(tt)

    for j in range(1, T):
        at_distance(j, take_weights)
        ring_adv(ko, tp(j - 1), twin_o)
        ring_adv(ku, tp(j - 1))
        if j == 1:
            for s in range(1, S):
                arrived(kq, 0, s, twin_q)
                if s + 1 < S:
                    ring_send(kq, 0, s + 1)
            copy(r.RQ, r.RQ, r.tw_s.at[1], r.tw_r.at[1], partner).wait_recv()
            project(t)
            attend(0)
        else:
            ring_fin(ko, tp(j - 2), twin_o)
        at_distance(j, take_tokens)
        if j == 1:
            ring_adv(kd_, t)
        project(tp(j))
        attend(j)
    inner = (t > 0) & (t < T - 1)
    edge = (t == 0) | (t == T - 1)

    def take_down(j):
        tt = tp(j)
        z_wait(kd_, tt)
        z_send(kd_, tt)
        ring_send(kd_, tt, 0)

    spin(0, T, finish_context)
    ring_adv(ko, tp(T - 1), twin_o)
    ring_adv(ku, tp(T - 1))
    ring_fin(ko, tp(T - 2), twin_o)
    ring_fin(ko, tp(T - 1), twin_o)
    take_down(1)

    @pl.when(inner)
    def _():
        for j in range(2, T):
            take_down(j)
            if j == 2:
                ring_adv(kd_, tp(1))

    r.CTX[t] = r.CXR[t]
    for k in range(1, T):
        tt = lax.rem(t + k, T)
        copy(r.CTX.at[tt], r.CTX.at[tt], r.c_s.at[tt], r.c_r.at[tt], partner).wait_recv()
    copy(r.RWO, r.RWO, r.tw_s.at[0], r.tw_r.at[0], partner).wait_recv()

    def out_dot(j):
        y = nt(r.CTX[j], merge(r.Wo[j]))

        @pl.when(j == 0)
        def _():
            r.FEED[0] = y

        @pl.when(j > 0)
        def _():
            r.FEED[0] += y

    spin(0, T, out_dot)

    def rows_of(body):
        def step(i):
            body(pl.ds(pl.multiple_of(i * RC, RC), RC))

        spin(0, TB // RC, step)

    def tally(n, x):
        r.SACC[n] += x.reshape(RC // 8, 8, D).sum(axis=0)

    def norm(x):
        mid = x - jnp.mean(x, axis=-1, keepdims=True)
        inverse = lax.rsqrt(jnp.mean(mid * mid, axis=-1, keepdims=True) + 1e-05)
        return mid * inverse, inverse

    def norm_back(up, gain, normed, inverse):
        e = up * gain
        return inverse * (
            e - jnp.mean(e, axis=-1, keepdims=True) - normed * jnp.mean(e * normed, axis=-1, keepdims=True)
        )

    def vec(n):
        return r.vecs[n : n + 1, :]

    def first_norm(at):
        x = r.X[t, at, :].astype(F32) + r.FEED[0, at, :] + vec(0)
        normed, inverse = norm(x)
        h1 = normed * vec(1) + vec(2)
        r.N1[at, :] = normed
        r.IV1[at, :] = inverse
        r.H1[at, :] = h1
        r.POOL[MID + c, at, :] = h1.astype(BF)

    rows_of(first_norm)

    def exchange(n, base, op="start"):
        ref = r.POOL.at[base + c]
        go(copy(ref, ref, r.e_s.at[n], r.e_r.at[n], partner), op)

    def exchanged(n, base):
        ref = r.POOL.at[base + oc]
        copy(ref, ref, r.e_s.at[n], r.e_r.at[n], partner).wait_recv()

    exchange(0, MID)

    @pl.when(edge)
    def _():
        for j in range(2, T):
            take_down(j)
            if j == 2:
                ring_adv(kd_, tp(1))

    for k in range(1, T):
        tt = lax.rem(t + k, T)
        copy(r.BU.at[tt], r.BU.at[tt], r.b_s.at[tt], r.b_r.at[tt], partner).wait_recv()
    exchanged(0, MID)

    def turn(src, dst):
        def step(b):
            y = r.POOL[src + b].astype(F32).T.astype(BF)
            dst[:, pl.ds(pl.multiple_of(b * TB, TB), TB)] = y

        spin(0, 2, step)

    def up(j):
        tt = tp(j)
        ring_fin(ku, tt)
        w = merge(r.Wu[tt])
        bias = r.BU[tt, :, pl.ds(lo, HC)]

        def block(b):
            r.PRE[...] = nn(r.POOL[MID + b], w) + bias

            def piece(i):
                at = pl.ds(pl.multiple_of(i * RC, RC), RC)
                v = r.PRE[at, :]
                cdf = 0.5 * (1.0 + lax.erf(v * 2.0 ** (-0.5)))
                slope = cdf + v * jnp.exp(-0.5 * v * v) * (2.0 * math.pi) ** (-0.5)
                to = pl.ds(pl.multiple_of(b * TB + i * RC, RC), RC)
                r.ACT[tt, to, :] = (v * cdf).astype(BF)
                r.SL[tt, to, :] = slope.astype(BF)

            spin(0, TB // RC, piece)

        spin(0, 2, block)

    for j in range(T):
        ahead = 2 if j == 0 else j + 1 if j >= 2 else T
        if ahead < T:
            ring_adv(kd_, tp(ahead))
        up(j)
    turn(MID, r.MIDT)

    def down(j):
        tt = tp(j)
        ring_fin(kd_, tt)
        w = merge(r.Wd[tt])

        def block(b):
            y = nt(r.ACT[tt, pl.ds(pl.multiple_of(b * TB, TB), TB), :], w)
            if j == 0:
                r.FEED[b] = y
            else:
                r.FEED[b] += y

        spin(0, 2, block)

    for j in range(T):
        down(j)

    def give(n):
        def step(at):
            r.POOL[FSND, at, :] = r.FEED[oc, at, :].astype(BF)

        rows_of(step)
        copy(r.POOL.at[FSND], r.POOL.at[FRCV], r.e_s.at[n], r.e_r.at[n], partner).start()
        copy(r.POOL.at[FRCV], r.POOL.at[FRCV], r.e_s.at[n], r.e_r.at[n], partner).wait_recv()
        copy(r.POOL.at[FSND], r.POOL.at[FRCV], r.e_s.at[n], r.e_r.at[n], partner).wait_send()

    def given(n, at):
        return r.FEED[c, at, :] + r.POOL[FRCV, at, :].astype(F32)

    give(1)

    def second_norm(at):
        x = r.H1[at, :] + given(1, at) + vec(3)
        normed, inverse = norm(x)
        g = r.out[at, :].astype(F32)
        r.out[at, :] = (normed * vec(4) + vec(5)).astype(BF)
        tally(0, g * normed)
        tally(1, g)
        back = norm_back(g, vec(4), normed, inverse)
        r.H1[at, :] = back
        low = back.astype(BF)
        r.POOL[GF + c, at, :] = low
        tally(2, low.astype(F32))

    rows_of(second_norm)
    exchange(2, GF)

    def drain_gather(k):
        def step(tt):
            if hasattr(k, "zs"):
                z_send(k, tt, "drain")
            for s in range(S):
                ring_send(k, tt, s, "drain")

        spin(0, T, step)

    drain_gather(ku)
    drain_gather(kd_)
    swap_u.wait_send()
    swap_d.wait_send()
    exchanged(2, GF)
    turn(GF, r.GFT)

    def slot_back(k):
        tt = tp(T - 1 - k)

        def block(b):
            to = pl.ds(pl.multiple_of(b * TB, TB), TB)
            r.PRE[...] = nn(r.POOL[GF + b], merge(r.Wd[tt]))

            def piece(i):
                at = pl.ds(pl.multiple_of(i * RC, RC), RC)
                tr = pl.ds(pl.multiple_of(b * TB + i * RC, RC), RC)
                gp = (r.PRE[at, :] * r.SL[tt, tr, :].astype(F32)).astype(BF)
                r.SL[tt, tr, :] = gp
                r.SBA[...] += gp.astype(F32).reshape(RC // 8, 8, HC).sum(axis=0)

            spin(0, TB // RC, piece)
            y = nt(r.SL[tt, to, :], merge(r.Wu[tt]))

            @pl.when(k == 0)
            def _():
                r.FEED[b] = y

            @pl.when(k > 0)
            def _():
                r.FEED[b] += y

        r.SBA[...] = jnp.zeros_like(r.SBA)
        spin(0, 2, block)
        r.SB[pl.ds(2 * tt + c, 1)] = r.SBA[...].sum(axis=0, keepdims=True)[None]

    def slot_weights(k):
        tt = tp(T - 1 - k)

        def down_weight(qq):
            at = pl.ds(pl.multiple_of(qq * 2 * R, 2 * R), 2 * R)
            r.Wd[tt, qq] = nn(r.GFT[at, :], r.ACT[tt]).astype(BF).reshape(2, R, HC)

        def up_weight(qq):
            at = pl.ds(pl.multiple_of(qq * 2 * R, 2 * R), 2 * R)
            r.Wu[tt, qq] = nn(r.MIDT[at, :], r.SL[tt]).astype(BF).reshape(2, R, HC)

        spin(0, NQ, down_weight)

        @pl.when(k < T - 1)
        def _():
            rs_send(kd_, tt, 0)

        spin(0, NQ, up_weight)

        @pl.when(k < T - 1)
        def _():
            rs_send(ku, tt, 0)

    H = T // 2
    many = max(2, 256 // R)

    def far(k):
        return tp(T - 1 - k)

    def pair_mid(k):
        rs_mid(kd_, far(k))
        rs_mid(ku, far(k))

    def pair_last(k):
        for w in (kd_, ku):
            rs_last(w, far(k))
            chain_first(w, far(k))

    def pair_on(k):
        chain_on(kd_, far(k))
        chain_on(ku, far(k))

    def part_last(w, k):
        rs_last(w, far(k))
        chain_first(w, far(k))

    def slots(k):
        slot_back(k)

        @pl.when(k == 0)
        def _():
            slot_weights(k)

        @pl.when(k == 1)
        def _():
            rs_mid(kd_, far(0))

        @pl.when(k == 2)
        def _():
            rs_mid(ku, far(0))

    spin(0, T, slots)
    give(3)

    def first_back(at):
        g = r.H1[at, :] + given(3, at)
        normed = r.N1[at, :]
        tally(3, g * normed)
        tally(4, g)
        back = norm_back(g, vec(1), normed, r.IV1[at, :])
        r.H1[at, :] = back
        low = back.astype(BF)
        r.gtok[at, :] = low
        tally(5, low.astype(F32))

    rows_of(first_back)

    def context_back(k):
        tt = tp(T - 1 - k)
        r.CXR[tt] = nn(r.gtok[...], merge(r.Wo[tt])).astype(BF)

        @pl.when(tt != t)
        def _():
            copy(r.CXR.at[tt], r.GC.at[t], r.gc_s.at[tt], r.gc_r.at[t], (d, tt)).start()

        @pl.when(tt == t)
        def _():
            r.GC[t] = r.CXR[t]

    for k in range(1, T):
        tt = lax.rem(t + k, T)
        copy(r.CXR.at[tt], r.CTX.at[t], r.c_s.at[tt], r.c_r.at[t], (d, tt)).wait_send()
    spin(0, T, context_back)
    spin(1, H, slot_weights)
    part_last(kd_, 0)
    for n in range(6):
        r.SV[n : n + 1, :] = r.SACC[n].sum(axis=0, keepdims=True)
    r.SV[6:8, :] = jnp.zeros((2, D), F32)

    def sum_core(n, ref, box, op):
        cp = copy(ref, box, r.a_s.at[0, n], r.a_r.at[0, n], partner)
        if op == "start":
            cp.start()
        else:
            copy(box, box, r.a_s.at[0, n], r.a_r.at[0, n], partner).wait_recv()
            cp.wait_send()
            ref[...] += box[...]

    def sum_group(stage, n, ref, box, me, count, dev, op):
        if op == "start":
            box[me] = ref[...]
        for k in range(1, count):
            other = lax.rem(me + k, count)
            sems = r.ag_s.at[stage, n, other], r.ag_r.at[stage, n, me]
            if op == "start":
                copy(box.at[me], box.at[me], *sems, dev(other)).start()
            else:
                copy(box.at[me], box.at[me], *sems, dev(other)).wait_send()
                copy(
                    box.at[other], box.at[other], r.ag_s.at[stage, n, other],
                    r.ag_r.at[stage, n, other], dev(other),
                ).wait_recv()
        if op != "start":
            total = box[0]
            for k in range(1, count):
                total = total + box[k]
            ref[...] = total

    def chip_dev(other):
        return (2 * other + c, t)

    def row_dev(other):
        return (d, other)

    sum_core(0, r.SV, r.SV1, "start")
    sum_core(1, r.SB, r.SB1, "start")

    outer = ind(t, 0, T) + ind(t, T - 1, T)

    def attend_back(j):
        i = tp(j) + (tp(T - 1 - j) - tp(j)) * outer
        at = pl.ds(pl.multiple_of(i * TB, TB), TB)

        @pl.when(i != t)
        def _():
            copy(r.GC.at[i], r.GC.at[i], r.gc_s.at[i], r.gc_r.at[i], partner).wait_recv()

        bias_for(i)
        for h in range(heads):
            pair = slice((h // 2) * 128, (h // 2) * 128 + 128)
            qh = r.Q[at, pair] * picks[h % 2]
            gh = r.GC[i, :, pair] * picks[h % 2]
            pr = jnp.exp(nt(r.K[:, pair], qh) + r.BIAS[...] - r.AM[i, h : h + 1, :])
            gp = nt(r.V[:, pair], gh)
            r.DV[:, pair] += nn(pr.astype(BF), gh)
            prod = pr * gp
            delta = jnp.sum(prod, axis=0, keepdims=True)
            ds = (prod - pr * delta).astype(BF)
            r.DK[:, pair] += nn(ds, qh)
            r.CT[h * HD : (h + 1) * HD, :] = nn(r.KT[h * HD : (h + 1) * HD, :], ds) * HD ** (-0.5)
        r.DPJ[i, :, 0:C] = r.CT[...].T.astype(BF)

    exchange(0, MID, "drain")
    exchange(2, GF, "drain")

    r.SQ[...] = jnp.zeros_like(r.SQ)

    def input_back(k):
        tt = far(k)
        at = pl.ds(pl.multiple_of(tt * TB, TB), TB)
        r.DPJ[tt, :, C : 2 * C] = r.DK[at, :].astype(BF)
        r.DPJ[tt, :, 2 * C : 3 * C] = r.DV[at, :].astype(BF)
        r.SQ[0:1, :] += r.DPJ[tt, :, 0:C].astype(F32).sum(axis=0, keepdims=True)
        r.SQ[1:2, :] += r.DPJ[tt, :, 2 * C : 3 * C].astype(F32).sum(axis=0, keepdims=True)
        r.POOL[tt] = nt(r.DPJ[tt], merge(r.Wq[...])).astype(BF)

        @pl.when(jnp.int32(k) < 2)
        def _():
            chain_first(kg, tt)

    drain_gather(ko)
    copy(r.RWO, r.RWO, r.tw_s.at[0], r.tw_r.at[0], partner).wait_send()


    def out_back(tt):
        def weight(g):
            at = pl.ds(pl.multiple_of(g * many * R, 128), many * R)
            y = lax.dot_general(
                r.gtok[:, at], r.CTX[tt], (((0,), (0,)), ((), ())), preferred_element_type=F32
            ).astype(BF)
            r.Wo[tt, pl.ds(many * g, many)] = y.reshape(many, R, C)
            for k in range(many // 2):
                qq = g * (many // 2) + k
                copy(r.Wo.at[tt, 2 * qq + oc], r.RWO.at[tt, qq], r.go_s.at[0], r.go_r.at[0], partner).start()

        spin(0, DP // many, weight)

    spin(0, T, out_back)

    def attend_early(j):
        attend_back(j)

        @pl.when(j == 0)
        def _():
            part_last(ku, 0)

    spin(0, H, attend_early)
    copy(r.RWO, r.RWO, r.go_s.at[0], r.go_r.at[0], partner).wait_recv()

    def out_join(k):
        tt = tp(T - 1 - k)

        def step(qq):
            add(r.Wo.at[tt, 2 * qq + c], r.RWO.at[tt, qq])

        spin(0, NQ, step)
        rs_send(ko, tt, 0)

    spin(0, T, out_join)
    for k in range(1, H):
        pair_mid(k)
    spin(H, T - 1, slot_weights)
    sum_core(0, r.SV, r.SV1, "end")
    sum_core(1, r.SB, r.SB1, "end")
    sum_group(0, 0, r.SV, r.SV2, q, NQ, chip_dev, "start")
    sum_group(0, 1, r.SB, r.SB2, q, NQ, chip_dev, "start")

    def attend_late(j):
        attend_back(j)
        if T - 1 > reach:

            @pl.when((j == T - 2) & edge)
            def _():
                input_back(0)

    spin(H, T, attend_late)
    def input_rest(k):
        @pl.when((k > 0) | inner | (T - 1 <= reach))
        def _():
            input_back(k)

    spin(0, T, input_rest)
    spin(T - 1, T, slot_weights)
    for k in range(T):
        rs_mid(ko, far(k))
    for k in range(H, T - 1):
        pair_mid(k)
    sum_core(2, r.SQ, r.SQ1, "start")
    pair_on(0)

    copy(r.RQ, r.RQ, r.tw_s.at[1], r.tw_r.at[1], partner).wait_send()
    for s in range(S):
        ring_send(kq, 0, s, "drain")

    def qkv_weight(g):
        cols = pl.ds(pl.multiple_of(g * many * R, 128), many * R)
        x = merge(r.X[:, :, cols])
        y = lax.dot_general(
            x, merge(r.DPJ[...]), (((0,), (0,)), ((), ())), preferred_element_type=F32
        )
        r.Wq[pl.ds(many * g, many)] = y.astype(BF).reshape(many, R, 3 * C)
        for k in range(many // 2):
            qq = g * (many // 2) + k
            copy(r.Wq.at[2 * qq + oc], r.RQ.at[qq], r.go_s.at[1], r.go_r.at[1], partner).start()

    spin(0, DP // many, qkv_weight)
    sum_core(2, r.SQ, r.SQ1, "end")
    sum_group(0, 2, r.SQ, r.SQ2, q, NQ, chip_dev, "start")
    copy(r.RQ, r.RQ, r.go_s.at[1], r.go_r.at[1], partner).wait_recv()

    def q_join(qq):
        add(r.Wq.at[2 * qq + c], r.RQ.at[qq])

    spin(0, NQ, q_join)
    rs_send(kq, 0, 0)
    rs_send(kd_, t, 0)
    rs_send(ku, t, 0)
    for k in range(T - 1):
        rs_last(ko, far(k))
        chain_first(ko, far(k))
    chain_on(kg, far(0))
    for k in range(1, H):
        pair_last(k)
    for k in range(2, T - 1):
        chain_first(kg, far(k))
    sum_group(0, 0, r.SV, r.SV2, q, NQ, chip_dev, "end")
    sum_group(0, 1, r.SB, r.SB2, q, NQ, chip_dev, "end")
    sum_group(1, 0, r.SV, r.SV3, t, T, row_dev, "start")
    sum_group(1, 1, r.SB, r.SB3, t, T, row_dev, "start")
    for k in range(H, T - 1):
        pair_last(k)
    rs_mid(kq, 0)
    for k in range(H):
        chain_on(ko, far(k))
    order = [2, 1] if T == 4 else list(range(1, T - 1))
    for n, k in enumerate(order):
        pair_on(k)
        chain_on(kg, far(k))
        if n == 0:
            pair_mid(T - 1)
    for k in range(H, T - 1):
        chain_on(ko, far(k))
    rs_last(kd_, t)
    rs_last(ku, t)
    rs_last(ko, t)
    rs_last(kq, 0)
    sum_group(1, 0, r.SV, r.SV3, t, T, row_dev, "end")
    sum_group(1, 1, r.SB, r.SB3, t, T, row_dev, "end")
    sum_group(0, 2, r.SQ, r.SQ2, q, NQ, chip_dev, "end")
    chain_end(kg)

    def finish(at):
        r.gtok[at, :] = (r.H1[at, :] + r.POOL[t, at, :].astype(F32)).astype(BF)

    rows_of(finish)
    chain_end(kd_)
    chain_end(ku)
    chain_end(ko)
    cps = []
    for n, ref in enumerate((r.Wu, r.Wd)):
        cp = copy(ref.at[t, q, oc], r.FSW.at[n], r.fs_s.at[n], r.fs_r.at[n], partner)
        cp.start()
        cps.append(cp)
    for n in range(3):
        r.gwq[n] = r.Wq[d, :, n * C : (n + 1) * C]
    r.gwo[...] = r.Wo[t, d]
    r.sv[...] = r.SV[...]
    r.sbq[...] = r.SQ[...]
    r.sbu[...] = r.SB[pl.ds(2 * t, 2)]
    for n, (ref, o) in enumerate(((r.Wu, r.gwu), (r.Wd, r.gwd))):
        copy(r.FSW.at[n], r.FSW.at[n], r.fs_s.at[n], r.fs_r.at[n], partner).wait_recv()
        o[:, pl.ds(lo, HC)] = ref[t, q, c]
        o[:, pl.ds(ro, HC)] = r.FSW[n]
        cps[n].wait_send()

    def drain(tt):
        z_send(kt, tt, "drain")
        for k in (kd_, ku, ko):
            for s in range(S):
                rs_send(k, tt, s, "drain")
            chain_send(k, tt, "drain")
        chain_send(kg, tt, "drain")

        @pl.when(tt != t)
        def _():
            copy(r.CXR.at[tt], r.GC.at[t], r.gc_s.at[tt], r.gc_r.at[t], (d, tt)).wait_send()
            copy(r.BU.at[t], r.BU.at[t], r.b_s.at[tt], r.b_r.at[t], (d, tt)).wait_send()

    spin(0, T, drain)
    for s in range(S):
        rs_send(kq, 0, s, "drain")
    copy(r.RWO, r.RWO, r.go_s.at[0], r.go_r.at[0], partner).wait_send()
    copy(r.RQ, r.RQ, r.go_s.at[1], r.go_r.at[1], partner).wait_send()


def layer(cf, *args):
    T, NQ, TB, D, R, C, HC, DP = cf.T, cf.NQ, cf.TB, cf.D, cf.R, cf.C, cf.HC, cf.DP
    S = NQ // 2
    RW = T * TB
    Cq = 3 * C
    heads = C // HD
    hp = -(-heads // 8) * 8
    dma = pltpu.SemaphoreType.DMA
    V = pltpu.VMEM
    ins = ["tok", "og", "wq", "wo", "wu", "wd", "bqv", "bup", "b_out", "g1", "n1", "b_down", "g2", "n2", "seg"]
    outs = {
        "out": ((TB, D), BF), "gtok": ((TB, D), BF), "gwq": ((3, R, C), BF), "gwo": ((R, C), BF),
        "gwu": ((R, 2 * HC), BF), "gwd": ((R, 2 * HC), BF), "sv": ((8, D), F32),
        "sbq": ((8, C), F32), "sbu": ((2, 1, HC), F32),
    }
    scratch = {
        "X": V((T, TB, D), BF), "Wq": V((DP, R, Cq), BF), "Wo": V((T, DP, R, C), BF),
        "Wu": V((T, NQ, 2, R, HC), BF), "Wd": V((T, NQ, 2, R, HC), BF), "BU": V((T, 1, 2 * HC), F32), "vecs": V((8, D), F32), "segc": V((RW, 128), F32),
        "Q": V((RW, C), BF), "K": V((RW, C), BF), "V": V((RW, C), BF),
        "KT": V((C, RW), BF), "VT": V((C, RW), BF), "BIAS": V((RW, TB), F32),
        "CT": V((C, TB), F32), "AM": V((T, hp, TB), F32), "AL": V((T, hp, TB), F32), "ACC": V((T, C, TB), F32), "CXR": V((T, TB, C), BF),
        "CTX": V((T, TB, C), BF), "FEED": V((2, TB, D), F32), "N1": V((TB, D), F32),
        "IV1": V((TB, 1), F32), "H1": V((TB, D), F32), "POOL": V((max(6, T), TB, D), BF),
        "MIDT": V((D, 2 * TB), BF), "PRE": V((TB, HC), F32), "ACT": V((T, 2 * TB, HC), BF),
        "SL": V((T, 2 * TB, HC), BF),
        "GFT": V((D, 2 * TB), BF),
        "GC": V((T, TB, C), BF),
        "DK": V((RW, C), F32), "DV": V((RW, C), F32), "DPJ": V((T, TB, Cq), BF),
        "g_ZB": V((T + 1, TB, D), BF), "RWO": V((T, NQ, R, C), BF), "RQ": V((NQ, R, Cq), BF),
        "FSW": V((2, R, HC), BF),
        "q_HB": V((1, 2, R // 2, Cq), BF), "q_FB": V((1, 2, S - 1, R, Cq), BF),
        "o_HB": V((T, 2, R // 2, C), BF), "o_FB": V((T, 2, S - 1, R, C), BF), "o_ZB": V((T + 1, R, C), BF),
        "u_HB": V((T, 2, R, HC), BF), "u_FB": V((T, 2, S - 1, 2, R, HC), BF), "u_ZB": V((T + 1, 2, R, HC), BF),
        "d_HB": V((T, 2, R, HC), BF), "d_FB": V((T, 2, S - 1, 2, R, HC), BF), "d_ZB": V((T + 1, 2, R, HC), BF),
        "SACC": V((6, 8, D), F32), "SBA": V((8, HC), F32),
        "SV": V((8, D), F32), "SV1": V((8, D), F32), "SV2": V((NQ, 8, D), F32), "SV3": V((T, 8, D), F32),
        "SB": V((2 * T, 1, HC), F32), "SB1": V((2 * T, 1, HC), F32), "SB2": V((NQ, 2 * T, 1, HC), F32),
        "SB3": V((T, 2 * T, 1, HC), F32),
        "SQ": V((8, C), F32), "SQ1": V((8, C), F32), "SQ2": V((NQ, 8, C), F32),
        "t_zs": dma((T, 2)), "t_zr": dma((T,)),
        "q_rs": dma((1, 2, S)), "q_rr": dma((1, 2, S)), "q_gs": dma((1, 2, S)), "q_gr": dma((1, 2, S)),
        "tw_s": dma((2,)), "tw_r": dma((2,)), "sw_s": dma((2,)), "sw_r": dma((2,)),
        "b_s": dma((T,)), "b_r": dma((T,)), "c_s": dma((T,)), "c_r": dma((T,)),
        "e_s": dma((4,)), "e_r": dma((4,)), "gc_s": dma((T,)), "gc_r": dma((T,)),
        "go_s": dma((2,)), "go_r": dma((2,)), "g_cs": dma((T,)), "g_cr": dma((T + 1,)),
        "a_s": dma((1, 3)), "a_r": dma((1, 3)),
        "ag_s": dma((2, 3, max(NQ, T))), "ag_r": dma((2, 3, max(NQ, T))),
        "fs_s": dma((2,)), "fs_r": dma((2,)), "in_s": dma((5,)),
    }
    for n in "oud":
        scratch[n + "_zs"] = dma((T, 2))
        scratch[n + "_zr"] = dma((T,))
        for m in ("_rs", "_rr", "_gs", "_gr"):
            scratch[n + m] = dma((T, 2, S))
        scratch[n + "_cs"] = dma((T,))
        scratch[n + "_cr"] = dma((T + 1,))
    names = ins + list(outs) + list(scratch)
    vm = pl.BlockSpec(memory_space=pltpu.VMEM)
    return pl.pallas_call(
        functools.partial(layer_kernel, cf, names),
        out_shape=tuple(jax.ShapeDtypeStruct(s, k) for s, k in outs.values()),
        in_specs=[pl.BlockSpec(memory_space=pl.ANY)] * 3 + [vm] * (len(ins) - 3),
        out_specs=(vm,) * len(outs),
        scratch_shapes=list(scratch.values()),
        compiler_params=pltpu.CompilerParams(
            collective_id=0, has_side_effects=True, vmem_limit_bytes=VMEM_LIMIT
        ),
        name="layer",
    )(*args)


def tail_kernel(cf, *refs):
    src, dst = refs[:9], refs[9:]
    out, gtok, gwq, gwo, gwu, gwd, sv, sbq, sbu = src
    dst[0][...] = out[...]
    dst[1][...] = gtok[...]
    dst[2][...] = gwq[...].astype(F32)
    dst[3][...] = sbq[0:2, :]
    dst[4][...] = gwo[...].astype(F32).T
    for n, row in ((5, 5), (6, 3), (7, 4), (11, 2), (12, 0), (13, 1)):
        dst[n][...] = sv[row : row + 1, :].reshape(cf.D)
    dst[8][...] = gwu[...].astype(F32)
    for n in range(2):
        dst[9][pl.ds(n * cf.HC, cf.HC)] = sbu[n].reshape(cf.HC)
    dst[10][...] = gwd[...].astype(F32).T


def tail(cf, *args):
    R, C, D, HC, TB = cf.R, cf.C, cf.D, cf.HC, cf.TB
    vm = pl.BlockSpec(memory_space=pltpu.VMEM)
    shapes = [
        ((TB, D), BF), ((TB, D), BF), ((3, R, C), F32), ((2, C), F32), ((C, R), F32),
        ((D,), F32), ((D,), F32), ((D,), F32), ((R, 2 * HC), F32), ((2 * HC,), F32),
        ((2 * HC, R), F32), ((D,), F32), ((D,), F32), ((D,), F32),
    ]
    return pl.pallas_call(
        functools.partial(tail_kernel, cf),
        out_shape=tuple(jax.ShapeDtypeStruct(*s) for s in shapes),
        in_specs=[vm] * len(args),
        out_specs=(vm,) * len(shapes),
        name="tail",
    )(*args)


def shards(
    tokens, segment_ids, out_grad, w_qkv, b_qv, w_out, b_out, norm1_gain, norm1_bias,
    w_up, b_up, w_down, b_down, norm2_gain, norm2_bias,
):
    DP, T = lax.axis_size("dp"), lax.axis_size("tensor")
    TB, D = tokens.shape
    R, _, C = w_qkv.shape
    HC = w_up.shape[1] // 2
    cf = SimpleNamespace(T=T, NQ=DP // 2, TB=TB, D=D, R=R, C=C, HC=HC, DP=DP)
    res = layer(
        cf, tokens, out_grad, w_qkv.transpose(1, 0, 2), w_out, w_up, w_down, b_qv, b_up,
        b_out, norm1_gain, norm1_bias, b_down, norm2_gain, norm2_bias, segment_ids,
    )
    res = list(tail(cf, *res))
    res[2] = res[2].transpose(1, 0, 2)
    return tuple(res)


def solution(mesh):
    tok = P(("dp", "tensor"), None)
    in_specs = (
        tok, P("dp", None), tok, P("dp", None, "tensor"), P(None, "tensor"), P("tensor", "dp"),
        P(), P(), P(), P("dp", "tensor"), P("tensor"), P("tensor", "dp"), P(), P(), P(),
    )
    out_specs = (
        tok, tok, P("dp", None, "tensor"), P(None, "tensor"), P("tensor", "dp"),
        P(), P(), P(), P("dp", "tensor"), P("tensor"), P("tensor", "dp"), P(), P(), P(),
    )
    return jax.shard_map(shards, mesh=mesh, in_specs=in_specs, out_specs=out_specs, check_vma=False)
```

```python
import functools
import math
from types import SimpleNamespace

import jax
import jax.numpy as jnp
from jax import lax
from jax.experimental import pallas as pl
from jax.experimental.pallas import tpu as pltpu
from jax.sharding import PartitionSpec as P

HD = 64
SEG_MOST = 512
MESH = pl.DeviceIdType.MESH
BF = jnp.bfloat16
F32 = jnp.float32
NEG = -1e30
VMEM_LIMIT = 67043328
MID, GF, FSND, FRCV = 0, 2, 4, 5


def nn(a, b):
    return jnp.dot(a, b, preferred_element_type=F32)


def nt(a, b):
    return lax.dot_general(a, b, (((1,), (1,)), ((), ())), preferred_element_type=F32)


def merge(x):
    return x.reshape(-1, x.shape[-1])


def spin(lo, hi, body):
    def step(i, carry):
        body(i)
        return carry

    lax.fori_loop(lo, hi, step, 0)


def order_table(T):
    return [sorted(range(T), key=lambda b: (abs(b - a), b if a < T / 2 else -b)) for a in range(T)]


def layer_kernel(cf, names, *refs):
    r = SimpleNamespace(**dict(zip(names, refs)))
    T, NQ, TB, D, R, C, HC, DP = cf.T, cf.NQ, cf.TB, cf.D, cf.R, cf.C, cf.HC, cf.DP
    S = NQ // 2
    RW = T * TB
    RC = 32
    heads = C // HD
    table = order_table(T)

    d = lax.axis_index("dp")
    t = lax.axis_index("tensor")
    q = lax.div(d, 2)
    c = d - 2 * q
    oc = 1 - c
    partner = (2 * q + oc, t)

    def perm(x):
        if NQ % 4:
            return x
        m = lax.rem(x, 4)
        return x + lax.div(m, 2) * (1 - 2 * lax.rem(m, 2))

    pos = perm(q)

    def chip_at(x):
        return perm(lax.rem(x + 4 * NQ, NQ))

    nxt = (2 * chip_at(pos + 1) + c, t)
    prv = (2 * chip_at(pos - 1) + c, t)

    def ind(a, b, n):
        x = lax.rem(a - b + n, n)
        return 1 - lax.div(x + n - 1, n)

    def tp(j):
        if isinstance(j, int):
            return sum(table[a][j] * ind(t, a, T) for a in range(T))
        js = [ind(j, b, T) for b in range(T)]
        total = 0
        for a in range(T):
            total = total + ind(t, a, T) * sum(table[a][b] * js[b] for b in range(T))
        return total

    def copy(src, dst, ss, rs, dev):
        return pltpu.make_async_remote_copy(
            src_ref=src, dst_ref=dst, send_sem=ss, recv_sem=rs, device_id=dev, device_id_type=MESH
        )

    def go(cp, op):
        if op == "start":
            cp.start()
        else:
            cp.wait_send()

    def half(kd, ref, h):
        if kd.split:
            return ref.at[h]
        n = kd.rows // 2
        return ref.at[pl.ds(h * n, n)]

    kt = SimpleNamespace(piece=lambda tt, qq: r.X.at[tt], zs=r.t_zs, zr=r.t_zr)
    kq = SimpleNamespace(
        piece=lambda tt, qq: r.Wq.at[2 * qq + c], split=False, rows=R, rs=r.q_rs, rr=r.q_rr,
        gs=r.q_gs, gr=r.q_gr, HB=r.q_HB, FB=r.q_FB,
    )
    ko = SimpleNamespace(
        piece=lambda tt, qq: r.Wo.at[tt, 2 * qq + c], split=False, rows=R, zs=r.o_zs, zr=r.o_zr,
        rs=r.o_rs, rr=r.o_rr, gs=r.o_gs, gr=r.o_gr, HB=r.o_HB, FB=r.o_FB,
        cs=r.o_cs, cr=r.o_cr, ZB=r.o_ZB,
    )
    ku = SimpleNamespace(
        piece=lambda tt, qq: r.Wu.at[tt, qq], split=True, rows=2 * R, zs=r.u_zs, zr=r.u_zr,
        rs=r.u_rs, rr=r.u_rr, gs=r.u_gs, gr=r.u_gr, HB=r.u_HB, FB=r.u_FB,
        cs=r.u_cs, cr=r.u_cr, ZB=r.u_ZB,
    )
    kd_ = SimpleNamespace(
        piece=lambda tt, qq: r.Wd.at[tt, qq], split=True, rows=2 * R, zs=r.d_zs, zr=r.d_zr,
        rs=r.d_rs, rr=r.d_rr, gs=r.d_gs, gr=r.d_gr, HB=r.d_HB, FB=r.d_FB,
        cs=r.d_cs, cr=r.d_cr, ZB=r.d_ZB,
    )
    kg = SimpleNamespace(piece=lambda tt, qq: r.POOL.at[tt], cs=r.g_cs, cr=r.g_cr, ZB=r.g_ZB)

    def z_right(k, tt, op):
        @pl.when((tt <= t) & (t < T - 1))
        def _():
            ref = k.piece(tt, q)
            go(copy(ref, ref, k.zs.at[tt, 0], k.zr.at[tt], (d, t + 1)), op)

    def z_left(k, tt, op):
        @pl.when((tt >= t) & (t > 0))
        def _():
            ref = k.piece(tt, q)
            go(copy(ref, ref, k.zs.at[tt, 1], k.zr.at[tt], (d, t - 1)), op)

    def z_send(k, tt, op="start"):
        z_right(k, tt, op)
        z_left(k, tt, op)

    def z_wait(k, tt):
        ref = k.piece(tt, q)
        copy(ref, ref, k.zs.at[tt, 0], k.zr.at[tt], partner).wait_recv()

    def ring_send(k, tt, s, op="start"):
        a = k.piece(tt, chip_at(pos - s))
        b = k.piece(tt, chip_at(pos + s))
        if s == S - 1:
            a, b = half(k, a, 0), half(k, b, 1)
        go(copy(a, a, k.rs.at[tt, 0, s], k.rr.at[tt, 0, s], nxt), op)
        go(copy(b, b, k.rs.at[tt, 1, s], k.rr.at[tt, 1, s], prv), op)

    def ring_wait(k, tt, s):
        a = k.piece(tt, chip_at(pos - 1 - s))
        b = k.piece(tt, chip_at(pos + 1 + s))
        if s == S - 1:
            a, b = half(k, a, 0), half(k, b, 1)
        copy(a, a, k.rs.at[tt, 0, s], k.rr.at[tt, 0, s], nxt).wait_recv()
        copy(b, b, k.rs.at[tt, 1, s], k.rr.at[tt, 1, s], prv).wait_recv()

    def twin_o(tt, qq):
        ref = r.Wo.at[tt, 2 * qq + c]
        copy(ref, ref, r.tw_s.at[0], r.tw_r.at[0], partner).start()

    def twin_q(tt, qq):
        ref = r.Wq.at[2 * qq + c]
        copy(ref, ref, r.tw_s.at[1], r.tw_r.at[1], partner).start()

    def arrived(k, tt, s, twin):
        ring_wait(k, tt, s)
        if twin is not None:
            twin(tt, chip_at(pos + 1 + s))
            if s < S - 1:
                twin(tt, chip_at(pos - 1 - s))

    def ring_adv(k, tt, twin=None):
        for s in range(1, S):
            arrived(k, tt, s - 1, twin)
            ring_send(k, tt, s)

    def ring_fin(k, tt, twin=None):
        arrived(k, tt, S - 1, twin)

    def add(dst, src):
        dst[...] = (dst[...].astype(F32) + src[...].astype(F32)).astype(BF)

    def rs_send(k, tt, s, op="start"):
        a = k.piece(tt, chip_at(pos + S - s))
        b = k.piece(tt, chip_at(pos - S + s))
        if s == 0:
            a, b = half(k, a, 0), half(k, b, 1)
            da, db = k.HB.at[tt, 0], k.HB.at[tt, 1]
        else:
            da, db = k.FB.at[tt, 0, s - 1], k.FB.at[tt, 1, s - 1]
        go(copy(a, da, k.gs.at[tt, 0, s], k.gr.at[tt, 0, s], nxt), op)
        go(copy(b, db, k.gs.at[tt, 1, s], k.gr.at[tt, 1, s], prv), op)

    def rs_add(k, tt, s):
        a = k.piece(tt, chip_at(pos + S - s - 1))
        b = k.piece(tt, chip_at(pos - S + s + 1))
        if s == 0:
            a, b = half(k, a, 0), half(k, b, 1)
            da, db = k.HB.at[tt, 0], k.HB.at[tt, 1]
        else:
            da, db = k.FB.at[tt, 0, s - 1], k.FB.at[tt, 1, s - 1]
        copy(da, da, k.gs.at[tt, 0, s], k.gr.at[tt, 0, s], nxt).wait_recv()
        add(a, da)
        copy(db, db, k.gs.at[tt, 1, s], k.gr.at[tt, 1, s], prv).wait_recv()
        add(b, db)

    def rs_mid(k, tt):
        for s in range(1, S):
            rs_add(k, tt, s - 1)
            rs_send(k, tt, s)

    def rs_last(k, tt):
        rs_add(k, tt, S - 1)

    def chain_send(k, tt, op="start"):
        ref = k.piece(tt, q)

        @pl.when(tt > t)
        def _():
            go(copy(ref, k.ZB.at[tt], k.cs.at[tt], k.cr.at[tt], (d, t + 1)), op)

        @pl.when(tt < t)
        def _():
            slot = tt + (T - tt) * ind(tt, t - 1, T)
            go(copy(ref, k.ZB.at[slot], k.cs.at[tt], k.cr.at[slot], (d, t - 1)), op)

    def chain_take(k, tt, slot):
        copy(k.ZB.at[slot], k.ZB.at[slot], k.cs.at[tt], k.cr.at[slot], partner).wait_recv()
        add(k.piece(tt, q), k.ZB.at[slot])

    def chain_first(k, tt):
        @pl.when(((tt > t) & (t == 0)) | ((tt < t) & (t == T - 1)))
        def _():
            chain_send(k, tt)

    def chain_on(k, tt):
        @pl.when(((tt > t) & (t > 0)) | ((tt < t) & (t < T - 1)))
        def _():
            chain_take(k, tt, tt)
            chain_send(k, tt)

    def chain_end(k):
        @pl.when(t > 0)
        def _():
            chain_take(k, t, t)

        @pl.when(t < T - 1)
        def _():
            chain_take(k, t, T)

    barrier = pltpu.get_barrier_semaphore()
    peers = [partner]
    peers += [(2 * lax.rem(q + k, NQ) + c, t) for k in range(1, NQ)]
    peers += [(d, lax.rem(t + k, T)) for k in range(1, T)]
    for peer in peers:
        pl.semaphore_signal(barrier, inc=1, device_id=peer, device_id_type=MESH)
    gets = [
        pltpu.make_async_copy(r.tok, r.X.at[t], r.in_s.at[0]),
        pltpu.make_async_copy(r.og, r.out, r.in_s.at[1]),
    ]
    for n in range(3):
        gets.append(
            pltpu.make_async_copy(r.wq.at[n], r.Wq.at[d, :, pl.ds(n * C, C)], r.in_s.at[2 + n])
        )
    for get in gets:
        get.start()
    lo = pl.multiple_of(c * HC, 128)
    ro = pl.multiple_of(oc * HC, 128)

    def flipped(x):
        return x.astype(F32).T.astype(BF)

    r.Wo[t, d] = flipped(r.wo[...])
    r.FSW[0] = r.wu[:, pl.ds(ro, HC)]
    r.FSW[1] = flipped(r.wd[pl.ds(ro, HC), :])
    r.Wu[t, q, c] = r.wu[:, pl.ds(lo, HC)]
    r.Wd[t, q, c] = flipped(r.wd[pl.ds(lo, HC), :])
    r.BU[t] = r.bup[...].astype(F32).reshape(1, 2 * HC)
    for n, name in enumerate(("b_out", "g1", "n1", "b_down", "g2", "n2")):
        r.vecs[n : n + 1, :] = getattr(r, name)[...].astype(F32).reshape(1, D)
    r.segc[...] = jnp.broadcast_to(r.seg[...].astype(F32), (128, RW)).T
    for get in gets:
        get.wait()
    pl.semaphore_wait(barrier, len(peers))

    swap_u = copy(r.FSW.at[0], r.Wu.at[t, q, c], r.sw_s.at[0], r.sw_r.at[0], partner)
    swap_d = copy(r.FSW.at[1], r.Wd.at[t, q, c], r.sw_s.at[1], r.sw_r.at[1], partner)
    swap_u.start()
    z_send(ko, t)
    twin_q(0, q)
    ring_send(kq, 0, 0)
    swap_d.start()
    twin_o(t, q)
    ring_send(ko, t, 0)

    def swapped(n, ref):
        ref = ref.at[t, q, oc]
        copy(ref, ref, r.sw_s.at[n], r.sw_r.at[n], partner).wait_recv()

    swapped(0, r.Wu)
    z_send(ku, t)
    z_send(kt, t)
    ring_send(ku, t, 0)
    swapped(1, r.Wd)

    def weights_z(tt):
        @pl.when(tt == 0)
        def _():
            z_right(kd_, t, "start")

        @pl.when(tt == T - 1)
        def _():
            z_left(kd_, t, "start")

    weights_z(t)
    for k in range(1, T):
        tt = lax.rem(t + k, T)
        copy(r.BU.at[t], r.BU.at[t], r.b_s.at[tt], r.b_r.at[t], (d, tt)).start()
    r.SACC[...] = jnp.zeros_like(r.SACC)
    r.SB[...] = jnp.zeros_like(r.SB)
    r.DK[...] = jnp.zeros_like(r.DK)
    r.DV[...] = jnp.zeros_like(r.DV)
    r.AM[...] = jnp.full_like(r.AM, NEG)
    r.AL[...] = jnp.zeros_like(r.AL)
    r.ACC[...] = jnp.zeros_like(r.ACC)

    def project(tt):
        x = r.X[tt]
        at = pl.ds(pl.multiple_of(tt * TB, TB), TB)
        for part, name in enumerate(("Q", "K", "V")):
            w = merge(r.Wq[:, :, part * C : (part + 1) * C])
            y = nn(x, w)
            if part != 1:
                y = y + r.bqv[part // 2 : part // 2 + 1, :].astype(F32)
            y = y.astype(BF)
            if part == 0:
                r.Q[at, :] = y * jnp.asarray(HD ** (-0.5), BF)
            elif part == 1:
                r.K[at, :] = y
                r.KT[:, at] = y.astype(F32).T.astype(BF)
            else:
                r.V[at, :] = y
                r.VT[:, at] = y.astype(F32).T.astype(BF)

    lane = lax.broadcasted_iota(jnp.int32, (1, 128), 1)
    picks = [(lane < HD).astype(F32).astype(BF), (lane >= HD).astype(F32).astype(BF)]
    reach = (SEG_MOST - 2) // TB + 1

    def rows_at(i):
        return pl.ds(pl.multiple_of(i * TB, TB), TB)

    def seg_row(i):
        return r.seg[:, rows_at(i)].astype(F32)

    def pair_up(i, b):
        bias = jnp.where(r.segc[rows_at(b), 0:1] == seg_row(i), 0.0, NEG)
        pairs = [slice((h // 2) * 128, (h // 2) * 128 + 128) for h in range(heads)]
        owns = [slice(h * HD, (h + 1) * HD) for h in range(heads)]
        before = [r.AM[i, h : h + 1, :] for h in range(heads)]
        sums = [r.AL[i, h : h + 1, :] for h in range(heads)]
        scs = [
            nt(r.K[rows_at(b), pairs[h]], r.Q[rows_at(i), pairs[h]] * picks[h % 2]) + bias
            for h in range(heads)
        ]
        tops = [jnp.maximum(before[h], jnp.max(scs[h], axis=0, keepdims=True)) for h in range(heads)]
        es = [jnp.exp(scs[h] - tops[h]) for h in range(heads)]
        shrinks = [jnp.exp(before[h] - tops[h]) for h in range(heads)]
        news = [nn(r.VT[owns[h], rows_at(b)], es[h].astype(BF)) for h in range(heads)]
        for h in range(heads):
            r.AM[i, h : h + 1, :] = tops[h]
            r.AL[i, h : h + 1, :] = sums[h] * shrinks[h] + jnp.sum(es[h], axis=0, keepdims=True)
            r.ACC[i, owns[h], :] = r.ACC[i, owns[h], :] * shrinks[h] + news[h]

    def attend(j):
        new = tp(j)

        def one(n):
            other = tp(lax.div(n, 2))
            side = lax.rem(n, 2)
            i = other + (new - other) * side
            b = new + (other - new) * side

            @pl.when((i - b <= reach) & (b - i <= reach))
            def _():
                pair_up(i, b)

        spin(0, 2 * j + 1, one)

    def finish_context(j):
        i = lax.rem(t + 1 + j, T)
        for h in range(heads):
            own = slice(h * HD, (h + 1) * HD)
            r.CT[own, :] = r.ACC[i, own, :] / r.AL[i, h : h + 1, :]
        r.AM[i, 0:heads, :] = r.AM[i, 0:heads, :] + jnp.log(r.AL[i, 0:heads, :])
        r.CXR[i] = r.CT[...].T.astype(BF)

        @pl.when(i != t)
        def _():
            copy(r.CXR.at[i], r.CTX.at[t], r.c_s.at[i], r.c_r.at[t], (d, i)).start()

    def bias_for(i):
        r.BIAS[...] = jnp.where(r.segc[:, 0:1] == seg_row(i), 0.0, NEG)

    arrived(kq, 0, 0, twin_q)
    ring_send(kq, 0, 1)
    ring_send(kd_, t, 0)
    def at_distance(k, take):
        @pl.when(t - k >= 0)
        def _():
            take(t - k)

        @pl.when(t + k < T)
        def _():
            take(t + k)

    def take_weights(tt):
        for k in (ko, ku):
            z_wait(k, tt)
            z_send(k, tt)
            ring_send(k, tt, 0)
        twin_o(tt, q)

    def take_tokens(tt):
        z_wait(kt, tt)
        z_send(kt, tt)
        weights_z(tt)

    for j in range(1, T):
        at_distance(j, take_weights)
        ring_adv(ko, tp(j - 1), twin_o)
        ring_adv(ku, tp(j - 1))
        if j == 1:
            for s in range(1, S):
                arrived(kq, 0, s, twin_q)
                if s + 1 < S:
                    ring_send(kq, 0, s + 1)
            copy(r.RQ, r.RQ, r.tw_s.at[1], r.tw_r.at[1], partner).wait_recv()
            project(t)
            attend(0)
        else:
            ring_fin(ko, tp(j - 2), twin_o)
        at_distance(j, take_tokens)
        if j == 1:
            ring_adv(kd_, t)
        project(tp(j))
        attend(j)
    inner = (t > 0) & (t < T - 1)
    edge = (t == 0) | (t == T - 1)

    def take_down(j):
        tt = tp(j)
        z_wait(kd_, tt)
        z_send(kd_, tt)
        ring_send(kd_, tt, 0)

    spin(0, T, finish_context)
    ring_adv(ko, tp(T - 1), twin_o)
    ring_adv(ku, tp(T - 1))
    ring_fin(ko, tp(T - 2), twin_o)
    ring_fin(ko, tp(T - 1), twin_o)
    take_down(1)

    @pl.when(inner)
    def _():
        for j in range(2, T):
            take_down(j)
            if j == 2:
                ring_adv(kd_, tp(1))

    r.CTX[t] = r.CXR[t]
    for k in range(1, T):
        tt = lax.rem(t + k, T)
        copy(r.CTX.at[tt], r.CTX.at[tt], r.c_s.at[tt], r.c_r.at[tt], partner).wait_recv()
    copy(r.RWO, r.RWO, r.tw_s.at[0], r.tw_r.at[0], partner).wait_recv()

    def out_dot(j):
        y = nt(r.CTX[j], merge(r.Wo[j]))

        @pl.when(j == 0)
        def _():
            r.FEED[0] = y

        @pl.when(j > 0)
        def _():
            r.FEED[0] += y

    spin(0, T, out_dot)

    def rows_of(body):
        def step(i):
            body(pl.ds(pl.multiple_of(i * RC, RC), RC))

        spin(0, TB // RC, step)

    def tally(n, x):
        r.SACC[n] += x.reshape(RC // 8, 8, D).sum(axis=0)

    def norm(x):
        mid = x - jnp.mean(x, axis=-1, keepdims=True)
        inverse = lax.rsqrt(jnp.mean(mid * mid, axis=-1, keepdims=True) + 1e-05)
        return mid * inverse, inverse

    def norm_back(up, gain, normed, inverse):
        e = up * gain
        return inverse * (
            e - jnp.mean(e, axis=-1, keepdims=True) - normed * jnp.mean(e * normed, axis=-1, keepdims=True)
        )

    def vec(n):
        return r.vecs[n : n + 1, :]

    def first_norm(at):
        x = r.X[t, at, :].astype(F32) + r.FEED[0, at, :] + vec(0)
        normed, inverse = norm(x)
        h1 = normed * vec(1) + vec(2)
        r.N1[at, :] = normed
        r.IV1[at, :] = inverse
        r.H1[at, :] = h1
        r.POOL[MID + c, at, :] = h1.astype(BF)

    rows_of(first_norm)

    def exchange(n, base, op="start"):
        ref = r.POOL.at[base + c]
        go(copy(ref, ref, r.e_s.at[n], r.e_r.at[n], partner), op)

    def exchanged(n, base):
        ref = r.POOL.at[base + oc]
        copy(ref, ref, r.e_s.at[n], r.e_r.at[n], partner).wait_recv()

    exchange(0, MID)

    @pl.when(edge)
    def _():
        for j in range(2, T):
            take_down(j)
            if j == 2:
                ring_adv(kd_, tp(1))

    for k in range(1, T):
        tt = lax.rem(t + k, T)
        copy(r.BU.at[tt], r.BU.at[tt], r.b_s.at[tt], r.b_r.at[tt], partner).wait_recv()
    exchanged(0, MID)

    def turn(src, dst):
        def step(b):
            y = r.POOL[src + b].astype(F32).T.astype(BF)
            dst[:, pl.ds(pl.multiple_of(b * TB, TB), TB)] = y

        spin(0, 2, step)

    def up(j):
        tt = tp(j)
        ring_fin(ku, tt)
        w = merge(r.Wu[tt])
        bias = r.BU[tt, :, pl.ds(lo, HC)]

        def block(b):
            r.PRE[...] = nn(r.POOL[MID + b], w) + bias

            def piece(i):
                at = pl.ds(pl.multiple_of(i * RC, RC), RC)
                v = r.PRE[at, :]
                cdf = 0.5 * (1.0 + lax.erf(v * 2.0 ** (-0.5)))
                slope = cdf + v * jnp.exp(-0.5 * v * v) * (2.0 * math.pi) ** (-0.5)
                to = pl.ds(pl.multiple_of(b * TB + i * RC, RC), RC)
                r.ACT[tt, to, :] = (v * cdf).astype(BF)
                r.SL[tt, to, :] = slope.astype(BF)

            spin(0, TB // RC, piece)

        spin(0, 2, block)

    for j in range(T):
        ahead = 2 if j == 0 else j + 1 if j >= 2 else T
        if ahead < T:
            ring_adv(kd_, tp(ahead))
        up(j)
    turn(MID, r.MIDT)

    def down(j):
        tt = tp(j)
        ring_fin(kd_, tt)
        w = merge(r.Wd[tt])

        def block(b):
            y = nt(r.ACT[tt, pl.ds(pl.multiple_of(b * TB, TB), TB), :], w)
            if j == 0:
                r.FEED[b] = y
            else:
                r.FEED[b] += y

        spin(0, 2, block)

    for j in range(T):
        down(j)

    def give(n):
        def step(at):
            r.POOL[FSND, at, :] = r.FEED[oc, at, :].astype(BF)

        rows_of(step)
        copy(r.POOL.at[FSND], r.POOL.at[FRCV], r.e_s.at[n], r.e_r.at[n], partner).start()
        copy(r.POOL.at[FRCV], r.POOL.at[FRCV], r.e_s.at[n], r.e_r.at[n], partner).wait_recv()
        copy(r.POOL.at[FSND], r.POOL.at[FRCV], r.e_s.at[n], r.e_r.at[n], partner).wait_send()

    def given(n, at):
        return r.FEED[c, at, :] + r.POOL[FRCV, at, :].astype(F32)

    give(1)

    def second_norm(at):
        x = r.H1[at, :] + given(1, at) + vec(3)
        normed, inverse = norm(x)
        g = r.out[at, :].astype(F32)
        r.out[at, :] = (normed * vec(4) + vec(5)).astype(BF)
        tally(0, g * normed)
        tally(1, g)
        back = norm_back(g, vec(4), normed, inverse)
        r.H1[at, :] = back
        low = back.astype(BF)
        r.POOL[GF + c, at, :] = low
        tally(2, low.astype(F32))

    rows_of(second_norm)
    exchange(2, GF)

    def drain_gather(k):
        def step(tt):
            if hasattr(k, "zs"):
                z_send(k, tt, "drain")
            for s in range(S):
                ring_send(k, tt, s, "drain")

        spin(0, T, step)

    drain_gather(ku)
    drain_gather(kd_)
    swap_u.wait_send()
    swap_d.wait_send()
    exchanged(2, GF)
    turn(GF, r.GFT)

    def slot_back(k):
        tt = tp(T - 1 - k)

        def block(b):
            to = pl.ds(pl.multiple_of(b * TB, TB), TB)
            r.PRE[...] = nn(r.POOL[GF + b], merge(r.Wd[tt]))

            def piece(i):
                at = pl.ds(pl.multiple_of(i * RC, RC), RC)
                tr = pl.ds(pl.multiple_of(b * TB + i * RC, RC), RC)
                gp = (r.PRE[at, :] * r.SL[tt, tr, :].astype(F32)).astype(BF)
                r.SL[tt, tr, :] = gp
                r.SBA[...] += gp.astype(F32).reshape(RC // 8, 8, HC).sum(axis=0)

            spin(0, TB // RC, piece)
            y = nt(r.SL[tt, to, :], merge(r.Wu[tt]))

            @pl.when(k == 0)
            def _():
                r.FEED[b] = y

            @pl.when(k > 0)
            def _():
                r.FEED[b] += y

        r.SBA[...] = jnp.zeros_like(r.SBA)
        spin(0, 2, block)
        r.SB[pl.ds(2 * tt + c, 1)] = r.SBA[...].sum(axis=0, keepdims=True)[None]

    def slot_weights(k):
        tt = tp(T - 1 - k)

        def down_weight(qq):
            at = pl.ds(pl.multiple_of(qq * 2 * R, 2 * R), 2 * R)
            r.Wd[tt, qq] = nn(r.GFT[at, :], r.ACT[tt]).astype(BF).reshape(2, R, HC)

        def up_weight(qq):
            at = pl.ds(pl.multiple_of(qq * 2 * R, 2 * R), 2 * R)
            r.Wu[tt, qq] = nn(r.MIDT[at, :], r.SL[tt]).astype(BF).reshape(2, R, HC)

        spin(0, NQ, down_weight)

        @pl.when(k < T - 1)
        def _():
            rs_send(kd_, tt, 0)

        spin(0, NQ, up_weight)

        @pl.when(k < T - 1)
        def _():
            rs_send(ku, tt, 0)

    H = T // 2
    many = max(2, 256 // R)

    def far(k):
        return tp(T - 1 - k)

    def pair_mid(k):
        rs_mid(kd_, far(k))
        rs_mid(ku, far(k))

    def pair_last(k):
        for w in (kd_, ku):
            rs_last(w, far(k))
            chain_first(w, far(k))

    def pair_on(k):
        chain_on(kd_, far(k))
        chain_on(ku, far(k))

    def part_last(w, k):
        rs_last(w, far(k))
        chain_first(w, far(k))

    def slots(k):
        slot_back(k)

        @pl.when(k == 0)
        def _():
            slot_weights(k)

        @pl.when(k == 1)
        def _():
            rs_mid(kd_, far(0))

        @pl.when(k == 2)
        def _():
            rs_mid(ku, far(0))

    spin(0, T, slots)
    give(3)

    def first_back(at):
        g = r.H1[at, :] + given(3, at)
        normed = r.N1[at, :]
        tally(3, g * normed)
        tally(4, g)
        back = norm_back(g, vec(1), normed, r.IV1[at, :])
        r.H1[at, :] = back
        low = back.astype(BF)
        r.gtok[at, :] = low
        tally(5, low.astype(F32))

    rows_of(first_back)

    def context_back(k):
        tt = tp(T - 1 - k)
        r.CXR[tt] = nn(r.gtok[...], merge(r.Wo[tt])).astype(BF)

        @pl.when(tt != t)
        def _():
            copy(r.CXR.at[tt], r.GC.at[t], r.gc_s.at[tt], r.gc_r.at[t], (d, tt)).start()

        @pl.when(tt == t)
        def _():
            r.GC[t] = r.CXR[t]

    for k in range(1, T):
        tt = lax.rem(t + k, T)
        copy(r.CXR.at[tt], r.CTX.at[t], r.c_s.at[tt], r.c_r.at[t], (d, tt)).wait_send()
    spin(0, T, context_back)
    spin(1, H, slot_weights)
    part_last(kd_, 0)
    for n in range(6):
        r.SV[n : n + 1, :] = r.SACC[n].sum(axis=0, keepdims=True)
    r.SV[6:8, :] = jnp.zeros((2, D), F32)

    def sum_core(n, ref, box, op):
        cp = copy(ref, box, r.a_s.at[0, n], r.a_r.at[0, n], partner)
        if op == "start":
            cp.start()
        else:
            copy(box, box, r.a_s.at[0, n], r.a_r.at[0, n], partner).wait_recv()
            cp.wait_send()
            ref[...] += box[...]

    def sum_group(stage, n, ref, box, me, count, dev, op):
        if op == "start":
            box[me] = ref[...]
        for k in range(1, count):
            other = lax.rem(me + k, count)
            sems = r.ag_s.at[stage, n, other], r.ag_r.at[stage, n, me]
            if op == "start":
                copy(box.at[me], box.at[me], *sems, dev(other)).start()
            else:
                copy(box.at[me], box.at[me], *sems, dev(other)).wait_send()
                copy(
                    box.at[other], box.at[other], r.ag_s.at[stage, n, other],
                    r.ag_r.at[stage, n, other], dev(other),
                ).wait_recv()
        if op != "start":
            total = box[0]
            for k in range(1, count):
                total = total + box[k]
            ref[...] = total

    def chip_dev(other):
        return (2 * other + c, t)

    def row_dev(other):
        return (d, other)

    sum_core(0, r.SV, r.SV1, "start")
    sum_core(1, r.SB, r.SB1, "start")

    outer = ind(t, 0, T) + ind(t, T - 1, T)

    def attend_back(j):
        i = tp(j) + (tp(T - 1 - j) - tp(j)) * outer
        at = pl.ds(pl.multiple_of(i * TB, TB), TB)

        @pl.when(i != t)
        def _():
            copy(r.GC.at[i], r.GC.at[i], r.gc_s.at[i], r.gc_r.at[i], partner).wait_recv()

        bias_for(i)
        for h in range(heads):
            pair = slice((h // 2) * 128, (h // 2) * 128 + 128)
            qh = r.Q[at, pair] * picks[h % 2]
            gh = r.GC[i, :, pair] * picks[h % 2]
            pr = jnp.exp(nt(r.K[:, pair], qh) + r.BIAS[...] - r.AM[i, h : h + 1, :])
            gp = nt(r.V[:, pair], gh)
            r.DV[:, pair] += nn(pr.astype(BF), gh)
            prod = pr * gp
            delta = jnp.sum(prod, axis=0, keepdims=True)
            ds = (prod - pr * delta).astype(BF)
            r.DK[:, pair] += nn(ds, qh)
            r.CT[h * HD : (h + 1) * HD, :] = nn(r.KT[h * HD : (h + 1) * HD, :], ds) * HD ** (-0.5)
        r.DPJ[i, :, 0:C] = r.CT[...].T.astype(BF)

    exchange(0, MID, "drain")
    exchange(2, GF, "drain")

    r.SQ[...] = jnp.zeros_like(r.SQ)

    def input_back(k):
        tt = far(k)
        at = pl.ds(pl.multiple_of(tt * TB, TB), TB)
        r.DPJ[tt, :, C : 2 * C] = r.DK[at, :].astype(BF)
        r.DPJ[tt, :, 2 * C : 3 * C] = r.DV[at, :].astype(BF)
        r.SQ[0:1, :] += r.DPJ[tt, :, 0:C].astype(F32).sum(axis=0, keepdims=True)
        r.SQ[1:2, :] += r.DPJ[tt, :, 2 * C : 3 * C].astype(F32).sum(axis=0, keepdims=True)
        r.POOL[tt] = nt(r.DPJ[tt], merge(r.Wq[...])).astype(BF)

        @pl.when(jnp.int32(k) < 2)
        def _():
            chain_first(kg, tt)

    drain_gather(ko)
    copy(r.RWO, r.RWO, r.tw_s.at[0], r.tw_r.at[0], partner).wait_send()


    def out_back(tt):
        def weight(g):
            at = pl.ds(pl.multiple_of(g * many * R, 128), many * R)
            y = lax.dot_general(
                r.gtok[:, at], r.CTX[tt], (((0,), (0,)), ((), ())), preferred_element_type=F32
            ).astype(BF)
            r.Wo[tt, pl.ds(many * g, many)] = y.reshape(many, R, C)
            for k in range(many // 2):
                qq = g * (many // 2) + k
                copy(r.Wo.at[tt, 2 * qq + oc], r.RWO.at[tt, qq], r.go_s.at[0], r.go_r.at[0], partner).start()

        spin(0, DP // many, weight)

    spin(0, T, out_back)

    def attend_early(j):
        attend_back(j)

        @pl.when(j == 0)
        def _():
            part_last(ku, 0)

    spin(0, H, attend_early)
    copy(r.RWO, r.RWO, r.go_s.at[0], r.go_r.at[0], partner).wait_recv()

    def out_join(k):
        tt = tp(T - 1 - k)

        def step(qq):
            add(r.Wo.at[tt, 2 * qq + c], r.RWO.at[tt, qq])

        spin(0, NQ, step)
        rs_send(ko, tt, 0)

    spin(0, T, out_join)
    for k in range(1, H):
        pair_mid(k)
    spin(H, T - 1, slot_weights)
    sum_core(0, r.SV, r.SV1, "end")
    sum_core(1, r.SB, r.SB1, "end")
    sum_group(0, 0, r.SV, r.SV2, q, NQ, chip_dev, "start")
    sum_group(0, 1, r.SB, r.SB2, q, NQ, chip_dev, "start")

    def attend_late(j):
        attend_back(j)
        if T - 1 > reach:

            @pl.when((j == T - 2) & edge)
            def _():
                input_back(0)

    spin(H, T, attend_late)
    def input_rest(k):
        @pl.when((k > 0) | inner | (T - 1 <= reach))
        def _():
            input_back(k)

    spin(0, T, input_rest)
    spin(T - 1, T, slot_weights)
    for k in range(T):
        rs_mid(ko, far(k))
    sum_core(2, r.SQ, r.SQ1, "start")
    pair_on(0)

    copy(r.RQ, r.RQ, r.tw_s.at[1], r.tw_r.at[1], partner).wait_send()
    for s in range(S):
        ring_send(kq, 0, s, "drain")

    def qkv_weight(g):
        cols = pl.ds(pl.multiple_of(g * many * R, 128), many * R)
        x = merge(r.X[:, :, cols])
        y = lax.dot_general(
            x, merge(r.DPJ[...]), (((0,), (0,)), ((), ())), preferred_element_type=F32
        )
        r.Wq[pl.ds(many * g, many)] = y.astype(BF).reshape(many, R, 3 * C)
        for k in range(many // 2):
            qq = g * (many // 2) + k
            copy(r.Wq.at[2 * qq + oc], r.RQ.at[qq], r.go_s.at[1], r.go_r.at[1], partner).start()

    spin(0, DP // many, qkv_weight)
    sum_core(2, r.SQ, r.SQ1, "end")
    sum_group(0, 2, r.SQ, r.SQ2, q, NQ, chip_dev, "start")
    copy(r.RQ, r.RQ, r.go_s.at[1], r.go_r.at[1], partner).wait_recv()

    def q_join(qq):
        add(r.Wq.at[2 * qq + c], r.RQ.at[qq])

    spin(0, NQ, q_join)
    for k in range(H, T - 1):
        pair_mid(k)
    rs_send(kq, 0, 0)
    rs_send(kd_, t, 0)
    rs_send(ku, t, 0)
    for k in range(T - 1):
        rs_last(ko, far(k))
        chain_first(ko, far(k))
    chain_on(kg, far(0))
    for k in range(1, H):
        pair_last(k)
    for k in range(2, T - 1):
        chain_first(kg, far(k))
    sum_group(0, 0, r.SV, r.SV2, q, NQ, chip_dev, "end")
    sum_group(0, 1, r.SB, r.SB2, q, NQ, chip_dev, "end")
    sum_group(1, 0, r.SV, r.SV3, t, T, row_dev, "start")
    sum_group(1, 1, r.SB, r.SB3, t, T, row_dev, "start")
    for k in range(H, T - 1):
        pair_last(k)
    rs_mid(kq, 0)
    for k in range(H):
        chain_on(ko, far(k))
    order = [2, 1] if T == 4 else list(range(1, T - 1))
    for n, k in enumerate(order):
        pair_on(k)
        chain_on(kg, far(k))
        if n == 0:
            pair_mid(T - 1)
    for k in range(H, T - 1):
        chain_on(ko, far(k))
    rs_last(kd_, t)
    rs_last(ku, t)
    rs_last(ko, t)
    rs_last(kq, 0)
    sum_group(1, 0, r.SV, r.SV3, t, T, row_dev, "end")
    sum_group(1, 1, r.SB, r.SB3, t, T, row_dev, "end")
    sum_group(0, 2, r.SQ, r.SQ2, q, NQ, chip_dev, "end")
    chain_end(kg)

    def finish(at):
        r.gtok[at, :] = (r.H1[at, :] + r.POOL[t, at, :].astype(F32)).astype(BF)

    rows_of(finish)
    chain_end(kd_)
    chain_end(ku)
    chain_end(ko)
    cps = []
    for n, ref in enumerate((r.Wu, r.Wd)):
        cp = copy(ref.at[t, q, oc], r.FSW.at[n], r.fs_s.at[n], r.fs_r.at[n], partner)
        cp.start()
        cps.append(cp)
    for n in range(3):
        r.gwq[n] = r.Wq[d, :, n * C : (n + 1) * C]
    r.gwo[...] = r.Wo[t, d]
    r.sv[...] = r.SV[...]
    r.sbq[...] = r.SQ[...]
    r.sbu[...] = r.SB[pl.ds(2 * t, 2)]
    for n, (ref, o) in enumerate(((r.Wu, r.gwu), (r.Wd, r.gwd))):
        copy(r.FSW.at[n], r.FSW.at[n], r.fs_s.at[n], r.fs_r.at[n], partner).wait_recv()
        o[:, pl.ds(lo, HC)] = ref[t, q, c]
        o[:, pl.ds(ro, HC)] = r.FSW[n]
        cps[n].wait_send()

    def drain(tt):
        z_send(kt, tt, "drain")
        for k in (kd_, ku, ko):
            for s in range(S):
                rs_send(k, tt, s, "drain")
            chain_send(k, tt, "drain")
        chain_send(kg, tt, "drain")

        @pl.when(tt != t)
        def _():
            copy(r.CXR.at[tt], r.GC.at[t], r.gc_s.at[tt], r.gc_r.at[t], (d, tt)).wait_send()
            copy(r.BU.at[t], r.BU.at[t], r.b_s.at[tt], r.b_r.at[t], (d, tt)).wait_send()

    spin(0, T, drain)
    for s in range(S):
        rs_send(kq, 0, s, "drain")
    copy(r.RWO, r.RWO, r.go_s.at[0], r.go_r.at[0], partner).wait_send()
    copy(r.RQ, r.RQ, r.go_s.at[1], r.go_r.at[1], partner).wait_send()


def layer(cf, *args):
    T, NQ, TB, D, R, C, HC, DP = cf.T, cf.NQ, cf.TB, cf.D, cf.R, cf.C, cf.HC, cf.DP
    S = NQ // 2
    RW = T * TB
    Cq = 3 * C
    heads = C // HD
    hp = -(-heads // 8) * 8
    dma = pltpu.SemaphoreType.DMA
    V = pltpu.VMEM
    ins = ["tok", "og", "wq", "wo", "wu", "wd", "bqv", "bup", "b_out", "g1", "n1", "b_down", "g2", "n2", "seg"]
    outs = {
        "out": ((TB, D), BF), "gtok": ((TB, D), BF), "gwq": ((3, R, C), BF), "gwo": ((R, C), BF),
        "gwu": ((R, 2 * HC), BF), "gwd": ((R, 2 * HC), BF), "sv": ((8, D), F32),
        "sbq": ((8, C), F32), "sbu": ((2, 1, HC), F32),
    }
    scratch = {
        "X": V((T, TB, D), BF), "Wq": V((DP, R, Cq), BF), "Wo": V((T, DP, R, C), BF),
        "Wu": V((T, NQ, 2, R, HC), BF), "Wd": V((T, NQ, 2, R, HC), BF), "BU": V((T, 1, 2 * HC), F32), "vecs": V((8, D), F32), "segc": V((RW, 128), F32),
        "Q": V((RW, C), BF), "K": V((RW, C), BF), "V": V((RW, C), BF),
        "KT": V((C, RW), BF), "VT": V((C, RW), BF), "BIAS": V((RW, TB), F32),
        "CT": V((C, TB), F32), "AM": V((T, hp, TB), F32), "AL": V((T, hp, TB), F32), "ACC": V((T, C, TB), F32), "CXR": V((T, TB, C), BF),
        "CTX": V((T, TB, C), BF), "FEED": V((2, TB, D), F32), "N1": V((TB, D), F32),
        "IV1": V((TB, 1), F32), "H1": V((TB, D), F32), "POOL": V((max(6, T), TB, D), BF),
        "MIDT": V((D, 2 * TB), BF), "PRE": V((TB, HC), F32), "ACT": V((T, 2 * TB, HC), BF),
        "SL": V((T, 2 * TB, HC), BF),
        "GFT": V((D, 2 * TB), BF),
        "GC": V((T, TB, C), BF),
        "DK": V((RW, C), F32), "DV": V((RW, C), F32), "DPJ": V((T, TB, Cq), BF),
        "g_ZB": V((T + 1, TB, D), BF), "RWO": V((T, NQ, R, C), BF), "RQ": V((NQ, R, Cq), BF),
        "FSW": V((2, R, HC), BF),
        "q_HB": V((1, 2, R // 2, Cq), BF), "q_FB": V((1, 2, S - 1, R, Cq), BF),
        "o_HB": V((T, 2, R // 2, C), BF), "o_FB": V((T, 2, S - 1, R, C), BF), "o_ZB": V((T + 1, R, C), BF),
        "u_HB": V((T, 2, R, HC), BF), "u_FB": V((T, 2, S - 1, 2, R, HC), BF), "u_ZB": V((T + 1, 2, R, HC), BF),
        "d_HB": V((T, 2, R, HC), BF), "d_FB": V((T, 2, S - 1, 2, R, HC), BF), "d_ZB": V((T + 1, 2, R, HC), BF),
        "SACC": V((6, 8, D), F32), "SBA": V((8, HC), F32),
        "SV": V((8, D), F32), "SV1": V((8, D), F32), "SV2": V((NQ, 8, D), F32), "SV3": V((T, 8, D), F32),
        "SB": V((2 * T, 1, HC), F32), "SB1": V((2 * T, 1, HC), F32), "SB2": V((NQ, 2 * T, 1, HC), F32),
        "SB3": V((T, 2 * T, 1, HC), F32),
        "SQ": V((8, C), F32), "SQ1": V((8, C), F32), "SQ2": V((NQ, 8, C), F32),
        "t_zs": dma((T, 2)), "t_zr": dma((T,)),
        "q_rs": dma((1, 2, S)), "q_rr": dma((1, 2, S)), "q_gs": dma((1, 2, S)), "q_gr": dma((1, 2, S)),
        "tw_s": dma((2,)), "tw_r": dma((2,)), "sw_s": dma((2,)), "sw_r": dma((2,)),
        "b_s": dma((T,)), "b_r": dma((T,)), "c_s": dma((T,)), "c_r": dma((T,)),
        "e_s": dma((4,)), "e_r": dma((4,)), "gc_s": dma((T,)), "gc_r": dma((T,)),
        "go_s": dma((2,)), "go_r": dma((2,)), "g_cs": dma((T,)), "g_cr": dma((T + 1,)),
        "a_s": dma((1, 3)), "a_r": dma((1, 3)),
        "ag_s": dma((2, 3, max(NQ, T))), "ag_r": dma((2, 3, max(NQ, T))),
        "fs_s": dma((2,)), "fs_r": dma((2,)), "in_s": dma((5,)),
    }
    for n in "oud":
        scratch[n + "_zs"] = dma((T, 2))
        scratch[n + "_zr"] = dma((T,))
        for m in ("_rs", "_rr", "_gs", "_gr"):
            scratch[n + m] = dma((T, 2, S))
        scratch[n + "_cs"] = dma((T,))
        scratch[n + "_cr"] = dma((T + 1,))
    names = ins + list(outs) + list(scratch)
    vm = pl.BlockSpec(memory_space=pltpu.VMEM)
    return pl.pallas_call(
        functools.partial(layer_kernel, cf, names),
        out_shape=tuple(jax.ShapeDtypeStruct(s, k) for s, k in outs.values()),
        in_specs=[pl.BlockSpec(memory_space=pl.ANY)] * 3 + [vm] * (len(ins) - 3),
        out_specs=(vm,) * len(outs),
        scratch_shapes=list(scratch.values()),
        compiler_params=pltpu.CompilerParams(
            collective_id=0, has_side_effects=True, vmem_limit_bytes=VMEM_LIMIT
        ),
        name="layer",
    )(*args)


def tail_kernel(cf, *refs):
    src, dst = refs[:9], refs[9:]
    out, gtok, gwq, gwo, gwu, gwd, sv, sbq, sbu = src
    dst[0][...] = out[...]
    dst[1][...] = gtok[...]
    dst[2][...] = gwq[...].astype(F32)
    dst[3][...] = sbq[0:2, :]
    dst[4][...] = gwo[...].astype(F32).T
    for n, row in ((5, 5), (6, 3), (7, 4), (11, 2), (12, 0), (13, 1)):
        dst[n][...] = sv[row : row + 1, :].reshape(cf.D)
    dst[8][...] = gwu[...].astype(F32)
    for n in range(2):
        dst[9][pl.ds(n * cf.HC, cf.HC)] = sbu[n].reshape(cf.HC)
    dst[10][...] = gwd[...].astype(F32).T


def tail(cf, *args):
    R, C, D, HC, TB = cf.R, cf.C, cf.D, cf.HC, cf.TB
    vm = pl.BlockSpec(memory_space=pltpu.VMEM)
    shapes = [
        ((TB, D), BF), ((TB, D), BF), ((3, R, C), F32), ((2, C), F32), ((C, R), F32),
        ((D,), F32), ((D,), F32), ((D,), F32), ((R, 2 * HC), F32), ((2 * HC,), F32),
        ((2 * HC, R), F32), ((D,), F32), ((D,), F32), ((D,), F32),
    ]
    return pl.pallas_call(
        functools.partial(tail_kernel, cf),
        out_shape=tuple(jax.ShapeDtypeStruct(*s) for s in shapes),
        in_specs=[vm] * len(args),
        out_specs=(vm,) * len(shapes),
        name="tail",
    )(*args)


def shards(
    tokens, segment_ids, out_grad, w_qkv, b_qv, w_out, b_out, norm1_gain, norm1_bias,
    w_up, b_up, w_down, b_down, norm2_gain, norm2_bias,
):
    DP, T = lax.axis_size("dp"), lax.axis_size("tensor")
    TB, D = tokens.shape
    R, _, C = w_qkv.shape
    HC = w_up.shape[1] // 2
    cf = SimpleNamespace(T=T, NQ=DP // 2, TB=TB, D=D, R=R, C=C, HC=HC, DP=DP)
    res = layer(
        cf, tokens, out_grad, w_qkv.transpose(1, 0, 2), w_out, w_up, w_down, b_qv, b_up,
        b_out, norm1_gain, norm1_bias, b_down, norm2_gain, norm2_bias, segment_ids,
    )
    res = list(tail(cf, *res))
    res[2] = res[2].transpose(1, 0, 2)
    return tuple(res)


def solution(mesh):
    tok = P(("dp", "tensor"), None)
    in_specs = (
        tok, P("dp", None), tok, P("dp", None, "tensor"), P(None, "tensor"), P("tensor", "dp"),
        P(), P(), P(), P("dp", "tensor"), P("tensor"), P("tensor", "dp"), P(), P(), P(),
    )
    out_specs = (
        tok, tok, P("dp", None, "tensor"), P(None, "tensor"), P("tensor", "dp"),
        P(), P(), P(), P("dp", "tensor"), P("tensor"), P("tensor", "dp"), P(), P(), P(),
    )
    return jax.shard_map(shards, mesh=mesh, in_specs=in_specs, out_specs=out_specs, check_vma=False)
```
